8 devices in a mesh: kv: 2 (over z, y), dup: 4 (over x, core).
Axes of the slice: x: 2, y: 2, z: 1, core: 2. Of those that a mesh axis runs over, the one named last changes fastest.
Arguments:
- queries: bfloat16 [512, 32, 128], P('kv', 'dup'), parts along dimension 0
- key_cache: bfloat16 [512, 2048, 128], P('kv', 'dup'), parts along dimension 0
- value_cache: bfloat16 [512, 2048, 128], P('kv', 'dup'), parts along dimension 0
- lengths: int32 [512], P('kv'), parts along dimension 0
Outputs:
- output: bfloat16 [512, 32, 128], P('kv', 'dup'), parts along dimension 0
There are 2 independent parts. The reference program is written for one: setup_inputs(seed, part) draws one part's arguments, and reference() takes and returns one part's arrays. A program takes and returns all parts, laid end to end along the dimension named above; each array names one.
All inputs are finite; a program needn't handle non-finite values.
Results may differ from the reference program's by a relative error of at most 0.0071394.
Values are sent between devices in bfloat16 or wider.
A program may use at most 1 GiB of HBM per device.

```python
import math
import jax
import jax.numpy as jnp
from jax import lax

BATCH = 256
SEQ = 2048
HEADS = 32
KV_HEADS = 4
HEAD_DIM = 128
DRAFT = 4

GROUP_HEADS = HEADS // KV_HEADS
QUERY_ROWS = GROUP_HEADS * DRAFT


def wave_field(k_freq, k_phase, k_dir, strength):
    spot_frac = jnp.arange(SEQ, dtype=jnp.float32) / SEQ
    freq_row = jax.random.randint(k_freq, (BATCH, 3), 1, 17, jnp.int32).astype(jnp.float32)
    phases = jax.random.uniform(k_phase, (BATCH, 3), jnp.float32) * (2.0 * math.pi)
    directions = jax.random.normal(k_dir, (BATCH, 3, HEAD_DIM), jnp.float32)
    wave_vals = jnp.cos(2.0 * math.pi * freq_row[:, None, :] * spot_frac[None, :, None] + phases[:, None, :])
    return strength * jnp.einsum("bsk,bkd->bsd", wave_vals, directions)


def setup_inputs(seed: int = 0, part: int = 0) -> dict:
    part_key = jax.random.fold_in(jax.random.key(seed), part)
    key_list = jax.random.split(part_key, 11)
    queries = jax.random.normal(key_list[0], (BATCH, QUERY_ROWS, HEAD_DIM), jnp.float32)
    k_noise = jax.random.normal(key_list[1], (BATCH, SEQ, HEAD_DIM), jnp.float32)
    key_cache = k_noise + wave_field(key_list[2], key_list[3], key_list[4], 1.5)
    v_noise = jax.random.normal(key_list[5], (BATCH, SEQ, HEAD_DIM), jnp.float32)
    value_cache = v_noise + wave_field(key_list[6], key_list[7], key_list[8], 1.0)
    low_len = max(DRAFT, SEQ // 8)
    lengths = jax.random.randint(key_list[9], (BATCH,), low_len, SEQ + 1, jnp.int32)
    full_row = jax.random.randint(key_list[10], (), 0, BATCH, jnp.int32)
    lengths = jnp.where(jnp.arange(BATCH) == full_row, SEQ, lengths).astype(jnp.int32)
    return {"queries": queries.astype(jnp.bfloat16), "key_cache": key_cache.astype(jnp.bfloat16), "value_cache": value_cache.astype(jnp.bfloat16), "lengths": lengths}


def reference(queries, key_cache, value_cache, lengths):
    score_scale = 1.0 / math.sqrt(HEAD_DIM)
    draft_pos = jnp.arange(QUERY_ROWS) % DRAFT
    seq_pos = jnp.arange(SEQ)

    def one_sequence(operands):
        q_rows, k_rows, v_rows, length = operands
        scores = jnp.dot(q_rows, k_rows.T, preferred_element_type=jnp.float32) * score_scale
        last_pos = length - DRAFT + draft_pos
        allowed = seq_pos[None, :] <= last_pos[:, None]
        scores = jnp.where(allowed, scores, -jnp.inf)
        row_peak = jnp.max(scores, axis=1, keepdims=True)
        prob_vals = jnp.exp(scores - row_peak)
        row_mass = jnp.sum(prob_vals, axis=1, keepdims=True)
        weighted = jnp.dot(prob_vals.astype(jnp.bfloat16), v_rows, preferred_element_type=jnp.float32)
        return (weighted / row_mass).astype(jnp.bfloat16)

    return lax.map(one_sequence, (queries, key_cache, value_cache, lengths))
```

```python
import functools
import math

import jax
import jax.numpy as jnp
from jax import lax
from jax.experimental import pallas as pl
from jax.experimental.pallas import tpu as pltpu
from jax.sharding import PartitionSpec as P

DRAFT = 4
CHUNK = 16
RING = 6
AHEAD = 2
FINAL_LAG = 10
ROWS = 8
MESH = pl.DeviceIdType.MESH
LOWEST = -3.0e38
FLOOR = -2.0e38


def kernel(
    num_chunks,
    scale,
    len_ref,
    q_hbm,
    k_hbm,
    v_hbm,
    out_hbm,
    kbuf,
    vbuf,
    qbuf,
    sbuf,
    part,
    stat,
    peer_part,
    peer_stat,
    send_out,
    send_lse,
    recv_out,
    recv_lse,
    own_lse,
    out_buf,
    k_sem,
    v_sem,
    q_local,
    q_chip_send,
    q_chip_recv,
    q_sib_send,
    q_sib_recv,
    q_fwd_send,
    q_fwd_recv,
    part_send,
    part_recv,
    stat_send,
    stat_recv,
    o_send,
    o_recv,
    l_send,
    l_recv,
    out_sem,
):
    me = lax.axis_index("dup")
    chip, core = me // 2, lax.rem(me, 2)
    sib = 2 * chip + (1 - core)
    far = 2 * (1 - chip) + core
    far_sib = 2 * (1 - chip) + (1 - core)
    span = kbuf.shape[2]
    pairs = CHUNK // 2

    def load_k(step, slot):
        return pltpu.make_async_copy(k_hbm.at[pl.ds(step * CHUNK, CHUNK)], kbuf.at[slot], k_sem.at[slot])

    def load_v(step, slot):
        return pltpu.make_async_copy(v_hbm.at[pl.ds(step * CHUNK, CHUNK)], vbuf.at[slot], v_sem.at[slot])

    def q_rows(step, owner):
        return qbuf.at[pl.ds(step * CHUNK, CHUNK), pl.ds(pl.multiple_of(owner * ROWS, ROWS), ROWS)]

    def q_mine(step):
        return q_hbm.at[pl.ds(step * CHUNK, CHUNK)]

    def keep_q(step):
        return pltpu.make_async_copy(q_mine(step), q_rows(step, me), q_local.at[step])

    def remote(src, dst, send, recv, dev):
        return pltpu.make_async_remote_copy(
            src_ref=src, dst_ref=dst, send_sem=send, recv_sem=recv, device_id={"dup": dev}, device_id_type=MESH
        )

    def q_to_far(step, owner):
        return remote(q_mine(step), q_rows(step, owner), q_chip_send.at[step], q_chip_recv.at[step], far)

    def q_to_sib(step, owner):
        return remote(q_mine(step), q_rows(step, owner), q_sib_send.at[step], q_sib_recv.at[step], sib)

    def q_forward(step, owner):
        return remote(q_rows(step, owner), q_rows(step, owner), q_fwd_send.at[step], q_fwd_recv.at[step], sib)

    def give_part(step):
        return remote(part.at[step, 1 - core], peer_part.at[step], part_send.at[step], part_recv.at[step], sib)

    def give_stat(step):
        return remote(stat.at[step], peer_stat.at[step], stat_send.at[step], stat_recv.at[step], sib)

    def give_out(step):
        return remote(send_out.at[step], recv_out.at[step], o_send.at[step], o_recv.at[step], far)

    def give_lse(step):
        return remote(send_lse.at[step], recv_lse.at[step], l_send.at[step], l_recv.at[step], far)

    def store_out(step):
        return pltpu.make_async_copy(
            out_buf.at[step], out_hbm.at[pl.ds(step * CHUNK * ROWS, CHUNK * ROWS)], out_sem.at[step]
        )

    for step in range(RING):
        load_k(step, step).start()
        load_v(step, step).start()

    barrier = pltpu.get_barrier_semaphore()
    for dev in (sib, far):
        pl.semaphore_signal(barrier, inc=1, device_id={"dup": dev}, device_id_type=MESH)
    pl.semaphore_wait(barrier, 2)

    @pl.loop(0, num_chunks)
    def _(step):
        q_to_far(step, me).start()
        q_to_sib(step, me).start()
        keep_q(step).start()

    def forward_q(step):
        q_to_far(step, far).wait_recv()
        q_forward(step, far).start()

    def await_q(step):
        keep_q(step).wait()
        q_to_sib(step, sib).wait_recv()
        q_forward(step, far_sib).wait_recv()

    lane = lax.broadcasted_iota(jnp.int32, (ROWS, 128), 1)
    draft_of_row = lax.rem(lax.broadcasted_iota(jnp.int32, (ROWS, span), 0), DRAFT)
    reach = lax.broadcasted_iota(jnp.int32, (ROWS, span), 1) - draft_of_row + (me * span + DRAFT)
    log2e = 1.0 / math.log(2.0)
    rate = scale * log2e

    def score_pair(step, slot, at, i):
        b = step * CHUNK + 2 * i
        q_a, q_b = qbuf[b], qbuf[b + 1]
        none = jnp.zeros_like(q_a)
        left = jnp.concatenate([jnp.concatenate([q_a, none], 1), jnp.concatenate([none, q_b], 1)], 0)
        right = jnp.concatenate([kbuf[slot, 2 * i], kbuf[slot, 2 * i + 1]], 1)
        sbuf[at, i] = lax.dot_general(left, right, (((1,), (1,)), ((), ())), preferred_element_type=jnp.float32)

    def attend_pair(step, slot, at, i, peaks, masses):
        probs = []
        for h in range(2):
            allowed = reach <= len_ref[step * CHUNK + 2 * i + h]
            for d in range(4):
                s = sbuf[at, i, pl.ds(32 * h + 8 * d, 8), :]
                s = jnp.where(allowed, s, LOWEST)
                peak = jnp.maximum(jnp.max(s, axis=1, keepdims=True), FLOOR)
                p = jnp.exp2((s - peak) * rate)
                mass = jnp.sum(p, axis=1, keepdims=True)
                here = lane == (CHUNK * d + 2 * i + h)
                peaks = jnp.where(here, peak, peaks)
                masses = jnp.where(here, mass, masses)
                probs.append(p)
        p = jnp.concatenate(probs, 0).astype(jnp.bfloat16)
        v = jnp.concatenate([vbuf[slot, 2 * i], vbuf[slot, 2 * i + 1]], 1)
        o = lax.dot_general(p, v, (((1,), (0,)), ((), ())), preferred_element_type=jnp.float32)
        for h in range(2):
            for d in range(4):
                part[step, d % 2, d // 2, 2 * i + h] = o[32 * h + 8 * d : 32 * h + 8 * d + 8, 128 * h : 128 * h + 128]
        return peaks, masses

    def to_front(tile, owner):
        return pltpu.roll(tile, lax.rem(128 - owner * CHUNK, 128), 1)

    def merge_chip(step):
        m_a, l_a, m_b, l_b = stat[step, 0], stat[step, 1], peer_stat[step, 0], peer_stat[step, 1]
        top = jnp.maximum(m_a, m_b)
        w_a, w_b = jnp.exp2((m_a - top) * rate), jnp.exp2((m_b - top) * rate)
        total = w_a * l_a + w_b * l_b
        some = total > 0.0
        safe = jnp.where(some, total, 1.0)
        inverse = jnp.where(some, 1.0 / safe, 0.0)
        w_a, w_b = w_a * inverse, w_b * inverse
        lse = jnp.where(some, top * rate + jnp.log2(safe), LOWEST)
        own_lse[step] = to_front(lse, me)
        send_lse[step] = to_front(lse, far)
        w_a_own, w_b_own = to_front(w_a, me), to_front(w_b, me)
        w_a_far, w_b_far = to_front(w_a, far), to_front(w_b, far)
        for i in range(pairs):
            far_out = []
            for h in range(2):
                b = 2 * i + h
                part[step, core, chip, b] = (
                    w_a_own[:, b : b + 1] * part[step, core, chip, b] + w_b_own[:, b : b + 1] * peer_part[step, chip, b]
                )
                far_out.append(
                    w_a_far[:, b : b + 1] * part[step, core, 1 - chip, b]
                    + w_b_far[:, b : b + 1] * peer_part[step, 1 - chip, b]
                )
            send_out[step, pl.ds(16 * i, 16), :] = jnp.concatenate(far_out, 0).astype(jnp.bfloat16)

    def merge_final(step):
        mine, theirs = own_lse[step], recv_lse[step]
        top = jnp.maximum(mine, theirs)
        w_a, w_b = jnp.exp2(mine - top), jnp.exp2(theirs - top)
        inverse = 1.0 / (w_a + w_b)
        w_a, w_b = w_a * inverse, w_b * inverse
        for i in range(pairs):
            other = recv_out[step, pl.ds(16 * i, 16), :].astype(jnp.float32)
            outs = []
            for h in range(2):
                b = 2 * i + h
                outs.append(
                    w_a[:, b : b + 1] * part[step, core, chip, b] + w_b[:, b : b + 1] * other[8 * h : 8 * h + 8]
                )
            out_buf[step, pl.ds(16 * i, 16), :] = jnp.concatenate(outs, 0).astype(jnp.bfloat16)

    def chip_stage(step):
        give_part(step).wait_recv()
        give_stat(step).wait_recv()
        merge_chip(step)
        give_out(step).start()
        give_lse(step).start()

    def final_stage(step):
        give_out(step).wait_recv()
        give_lse(step).wait_recv()
        merge_final(step)
        store_out(step).start()

    def attend(step, with_next):
        slot, at = lax.rem(step, RING), lax.rem(step, 2)
        next_slot, next_at = lax.rem(step + 1, RING), 1 - at
        peaks = jnp.zeros((ROWS, 128), jnp.float32)
        masses = jnp.zeros((ROWS, 128), jnp.float32)
        for i in range(pairs):
            if with_next:
                score_pair(step + 1, next_slot, next_at, i)
            peaks, masses = attend_pair(step, slot, at, i, peaks, masses)
        stat[step, 0] = peaks
        stat[step, 1] = masses

    last = num_chunks - 1
    for step in range(AHEAD):
        forward_q(step)
    await_q(0)
    load_k(0, 0).wait()
    for i in range(pairs):
        score_pair(0, 0, 0, i)
    load_k(RING, 0).start()

    @pl.loop(0, last)
    def _(step):
        @pl.when(step + AHEAD < num_chunks)
        def _():
            forward_q(step + AHEAD)

        await_q(step + 1)
        load_k(step + 1, lax.rem(step + 1, RING)).wait()
        load_v(step, lax.rem(step, RING)).wait()
        attend(step, True)

        @pl.when(step + 1 + RING < num_chunks)
        def _():
            load_k(step + 1 + RING, lax.rem(step + 1, RING)).start()

        @pl.when(step + RING < num_chunks)
        def _():
            load_v(step + RING, lax.rem(step, RING)).start()

        give_part(step).start()
        give_stat(step).start()

        @pl.when(step >= 2)
        def _():
            chip_stage(step - 2)

        @pl.when(step >= FINAL_LAG)
        def _():
            final_stage(step - FINAL_LAG)

    load_v(last, lax.rem(last, RING)).wait()
    attend(last, False)
    give_part(last).start()
    give_stat(last).start()

    @pl.loop(last - 2, num_chunks)
    def _(step):
        chip_stage(step)

    @pl.loop(last - FINAL_LAG, num_chunks)
    def _(step):
        final_stage(step)

    @pl.loop(0, num_chunks)
    def _(step):
        q_to_far(step, me).wait_send()
        q_to_sib(step, me).wait_send()
        q_forward(step, far).wait_send()
        give_part(step).wait_send()
        give_stat(step).wait_send()
        give_out(step).wait_send()
        give_lse(step).wait_send()
        store_out(step).wait()


def solution(mesh):
    def group_step(q_local, k_span, v_span, len_local):
        num_batch, span, dim = k_span.shape
        n = num_batch // CHUNK
        f32, bf16 = jnp.float32, jnp.bfloat16
        dma = lambda *shape: pltpu.SemaphoreType.DMA(shape)
        hbm = pl.BlockSpec(memory_space=pltpu.HBM)
        out = pl.pallas_call(
            functools.partial(kernel, n, dim**-0.5),
            out_shape=jax.ShapeDtypeStruct((num_batch * ROWS, dim), bf16),
            in_specs=[pl.BlockSpec(memory_space=pltpu.SMEM), hbm, hbm, hbm],
            out_specs=hbm,
            scratch_shapes=[
                pltpu.VMEM((RING, CHUNK, span, dim), bf16),
                pltpu.VMEM((RING, CHUNK, span, dim), bf16),
                pltpu.VMEM((num_batch, 4 * ROWS, dim), bf16),
                pltpu.VMEM((2, CHUNK // 2, 64, span), f32),
                pltpu.VMEM((n, 2, 2, CHUNK, ROWS, dim), f32),
                pltpu.VMEM((n, 2, ROWS, dim), f32),
                pltpu.VMEM((n, 2, CHUNK, ROWS, dim), f32),
                pltpu.VMEM((n, 2, ROWS, dim), f32),
                pltpu.VMEM((n, CHUNK * ROWS, dim), bf16),
                pltpu.VMEM((n, ROWS, dim), f32),
                pltpu.VMEM((n, CHUNK * ROWS, dim), bf16),
                pltpu.VMEM((n, ROWS, dim), f32),
                pltpu.VMEM((n, ROWS, dim), f32),
                pltpu.VMEM((n, CHUNK * ROWS, dim), bf16),
                dma(RING),
                dma(RING),
            ]
            + [dma(n)] * 16,
            compiler_params=pltpu.CompilerParams(
                collective_id=0, has_side_effects=True, vmem_limit_bytes=60 * 1024 * 1024
            ),
        )(len_local, q_local, k_span, v_span)
        return out.reshape(num_batch, ROWS, dim)

    return jax.shard_map(
        group_step,
        mesh=mesh,
        in_specs=(P("kv", "dup", None), P("kv", "dup", None), P("kv", "dup", None), P("kv")),
        out_specs=P("kv", "dup", None),
        check_vma=False,
    )
```

```python
import functools
import math

import jax
import jax.numpy as jnp
from jax import lax
from jax.experimental import pallas as pl
from jax.experimental.pallas import tpu as pltpu
from jax.sharding import PartitionSpec as P

DRAFT = 4
CHUNK = 16
RING = 6
AHEAD = 2
FINAL_LAG = 10
ROWS = 8
MESH = pl.DeviceIdType.MESH
LOWEST = -3.0e38
FLOOR = -2.0e38


def kernel(
    num_chunks,
    scale,
    len_ref,
    q_hbm,
    k_hbm,
    v_hbm,
    out_hbm,
    kbuf,
    vbuf,
    qbuf,
    sbuf,
    pbuf,
    part,
    stat,
    peer_part,
    peer_stat,
    send_out,
    send_lse,
    recv_out,
    recv_lse,
    own_lse,
    out_buf,
    k_sem,
    v_sem,
    q_local,
    q_chip_send,
    q_chip_recv,
    q_sib_send,
    q_sib_recv,
    q_fwd_send,
    q_fwd_recv,
    part_send,
    part_recv,
    stat_send,
    stat_recv,
    o_send,
    o_recv,
    l_send,
    l_recv,
    out_sem,
):
    me = lax.axis_index("dup")
    chip, core = me // 2, lax.rem(me, 2)
    sib = 2 * chip + (1 - core)
    far = 2 * (1 - chip) + core
    far_sib = 2 * (1 - chip) + (1 - core)
    span = kbuf.shape[2]
    pairs = CHUNK // 2

    def load_k(step, slot):
        return pltpu.make_async_copy(k_hbm.at[pl.ds(step * CHUNK, CHUNK)], kbuf.at[slot], k_sem.at[slot])

    def load_v(step, slot):
        return pltpu.make_async_copy(v_hbm.at[pl.ds(step * CHUNK, CHUNK)], vbuf.at[slot], v_sem.at[slot])

    def q_rows(step, owner):
        return qbuf.at[pl.ds(step * CHUNK, CHUNK), pl.ds(pl.multiple_of(owner * ROWS, ROWS), ROWS)]

    def q_mine(step):
        return q_hbm.at[pl.ds(step * CHUNK, CHUNK)]

    def keep_q(step):
        return pltpu.make_async_copy(q_mine(step), q_rows(step, me), q_local.at[step])

    def remote(src, dst, send, recv, dev):
        return pltpu.make_async_remote_copy(
            src_ref=src, dst_ref=dst, send_sem=send, recv_sem=recv, device_id={"dup": dev}, device_id_type=MESH
        )

    def q_to_far(step, owner):
        return remote(q_mine(step), q_rows(step, owner), q_chip_send.at[step], q_chip_recv.at[step], far)

    def q_to_sib(step, owner):
        return remote(q_mine(step), q_rows(step, owner), q_sib_send.at[step], q_sib_recv.at[step], sib)

    def q_forward(step, owner):
        return remote(q_rows(step, owner), q_rows(step, owner), q_fwd_send.at[step], q_fwd_recv.at[step], sib)

    def give_part(step):
        return remote(part.at[step, 1 - core], peer_part.at[step], part_send.at[step], part_recv.at[step], sib)

    def give_stat(step):
        return remote(stat.at[step], peer_stat.at[step], stat_send.at[step], stat_recv.at[step], sib)

    def give_out(step):
        return remote(send_out.at[step], recv_out.at[step], o_send.at[step], o_recv.at[step], far)

    def give_lse(step):
        return remote(send_lse.at[step], recv_lse.at[step], l_send.at[step], l_recv.at[step], far)

    def store_out(step):
        return pltpu.make_async_copy(
            out_buf.at[step], out_hbm.at[pl.ds(step * CHUNK * ROWS, CHUNK * ROWS)], out_sem.at[step]
        )

    for step in range(RING):
        load_k(step, step).start()
        load_v(step, step).start()

    barrier = pltpu.get_barrier_semaphore()
    for dev in (sib, far):
        pl.semaphore_signal(barrier, inc=1, device_id={"dup": dev}, device_id_type=MESH)
    pl.semaphore_wait(barrier, 2)

    @pl.loop(0, num_chunks)
    def _(step):
        q_to_far(step, me).start()
        q_to_sib(step, me).start()
        keep_q(step).start()

    def forward_q(step):
        q_to_far(step, far).wait_recv()
        q_forward(step, far).start()

    def await_q(step):
        keep_q(step).wait()
        q_to_sib(step, sib).wait_recv()
        q_forward(step, far_sib).wait_recv()

    lane = lax.broadcasted_iota(jnp.int32, (ROWS, 128), 1)
    draft_of_row = lax.rem(lax.broadcasted_iota(jnp.int32, (ROWS, span), 0), DRAFT)
    reach = lax.broadcasted_iota(jnp.int32, (ROWS, span), 1) - draft_of_row + (me * span + DRAFT)
    log2e = 1.0 / math.log(2.0)
    rate = scale * log2e

    def score_pair(step, slot, i):
        b = step * CHUNK + 2 * i
        q_a, q_b = qbuf[b], qbuf[b + 1]
        none = jnp.zeros_like(q_a)
        left = jnp.concatenate([jnp.concatenate([q_a, none], 1), jnp.concatenate([none, q_b], 1)], 0)
        right = jnp.concatenate([kbuf[slot, 2 * i], kbuf[slot, 2 * i + 1]], 1)
        return lax.dot_general(left, right, (((1,), (1,)), ((), ())), preferred_element_type=jnp.float32)

    def mask_pair(step, i, scores):
        for h in range(2):
            allowed = reach <= len_ref[step * CHUNK + 2 * i + h]
            for d in range(4):
                row = 32 * h + 8 * d
                s = jnp.where(allowed, scores[row : row + 8], LOWEST)
                sbuf[i, pl.ds(row, 8), :] = s
                peak = jnp.maximum(jnp.max(s, axis=1, keepdims=True), FLOOR)
                pbuf[i, pl.ds(row, 8), :] = jnp.broadcast_to(peak, (ROWS, 128))

    def attend_pair(step, slot, i, peaks, masses):
        probs = []
        for h in range(2):
            for d in range(4):
                row = 32 * h + 8 * d
                peak = pbuf[i, pl.ds(row, 8), :]
                s = sbuf[i, pl.ds(row, 8), :]
                p = jnp.exp2((s - jnp.concatenate([peak] * (span // 128), 1)) * rate)
                mass = jnp.sum(p, axis=1, keepdims=True)
                here = lane == (CHUNK * d + 2 * i + h)
                peaks = jnp.where(here, peak, peaks)
                masses = jnp.where(here, mass, masses)
                probs.append(p)
        p = jnp.concatenate(
            [jnp.concatenate(probs[j : j + 2], 0).astype(jnp.bfloat16) for j in range(0, 8, 2)], 0
        )
        v = jnp.concatenate([vbuf[slot, 2 * i], vbuf[slot, 2 * i + 1]], 1)
        o = lax.dot_general(p, v, (((1,), (0,)), ((), ())), preferred_element_type=jnp.float32)
        for h in range(2):
            for d in range(4):
                part[step, d % 2, d // 2, 2 * i + h] = o[32 * h + 8 * d : 32 * h + 8 * d + 8, 128 * h : 128 * h + 128]
        return peaks, masses

    def to_front(tile, owner):
        return pltpu.roll(tile, lax.rem(128 - owner * CHUNK, 128), 1)

    def merge_chip(step):
        m_a, l_a, m_b, l_b = stat[step, 0], stat[step, 1], peer_stat[step, 0], peer_stat[step, 1]
        top = jnp.maximum(m_a, m_b)
        w_a, w_b = jnp.exp2((m_a - top) * rate), jnp.exp2((m_b - top) * rate)
        total = w_a * l_a + w_b * l_b
        some = total > 0.0
        safe = jnp.where(some, total, 1.0)
        inverse = jnp.where(some, 1.0 / safe, 0.0)
        w_a, w_b = w_a * inverse, w_b * inverse
        lse = jnp.where(some, top * rate + jnp.log2(safe), LOWEST)
        own_lse[step] = to_front(lse, me)
        send_lse[step] = to_front(lse, far)
        w_a_own, w_b_own = to_front(w_a, me), to_front(w_b, me)
        w_a_far, w_b_far = to_front(w_a, far), to_front(w_b, far)
        for i in range(pairs):
            far_out = []
            for h in range(2):
                b = 2 * i + h
                part[step, core, chip, b] = (
                    w_a_own[:, b : b + 1] * part[step, core, chip, b] + w_b_own[:, b : b + 1] * peer_part[step, chip, b]
                )
                far_out.append(
                    w_a_far[:, b : b + 1] * part[step, core, 1 - chip, b]
                    + w_b_far[:, b : b + 1] * peer_part[step, 1 - chip, b]
                )
            send_out[step, pl.ds(16 * i, 16), :] = jnp.concatenate(far_out, 0).astype(jnp.bfloat16)

    def merge_final(step):
        mine, theirs = own_lse[step], recv_lse[step]
        top = jnp.maximum(mine, theirs)
        w_a, w_b = jnp.exp2(mine - top), jnp.exp2(theirs - top)
        inverse = 1.0 / (w_a + w_b)
        w_a, w_b = w_a * inverse, w_b * inverse
        for i in range(pairs):
            other = recv_out[step, pl.ds(16 * i, 16), :].astype(jnp.float32)
            outs = []
            for h in range(2):
                b = 2 * i + h
                outs.append(
                    w_a[:, b : b + 1] * part[step, core, chip, b] + w_b[:, b : b + 1] * other[8 * h : 8 * h + 8]
                )
            out_buf[step, pl.ds(16 * i, 16), :] = jnp.concatenate(outs, 0).astype(jnp.bfloat16)

    def chip_stage(step):
        give_part(step).wait_recv()
        give_stat(step).wait_recv()
        merge_chip(step)
        give_out(step).start()
        give_lse(step).start()

    def final_stage(step):
        give_out(step).wait_recv()
        give_lse(step).wait_recv()
        merge_final(step)
        store_out(step).start()

    def attend(step, with_next):
        slot, next_slot = lax.rem(step, RING), lax.rem(step + 1, RING)
        peaks = jnp.zeros((ROWS, 128), jnp.float32)
        masses = jnp.zeros((ROWS, 128), jnp.float32)
        for i in range(pairs):
            if with_next:
                scores = score_pair(step + 1, next_slot, i)
            peaks, masses = attend_pair(step, slot, i, peaks, masses)
            if with_next:
                mask_pair(step + 1, i, scores)
        stat[step, 0] = peaks
        stat[step, 1] = masses

    last = num_chunks - 1
    for step in range(AHEAD):
        forward_q(step)
    await_q(0)
    load_k(0, 0).wait()
    for i in range(pairs):
        mask_pair(0, i, score_pair(0, 0, i))
    load_k(RING, 0).start()

    @pl.loop(0, last)
    def _(step):
        @pl.when(step + AHEAD < num_chunks)
        def _():
            forward_q(step + AHEAD)

        await_q(step + 1)
        load_k(step + 1, lax.rem(step + 1, RING)).wait()
        load_v(step, lax.rem(step, RING)).wait()
        attend(step, True)

        @pl.when(step + 1 + RING < num_chunks)
        def _():
            load_k(step + 1 + RING, lax.rem(step + 1, RING)).start()

        @pl.when(step + RING < num_chunks)
        def _():
            load_v(step + RING, lax.rem(step, RING)).start()

        give_part(step).start()
        give_stat(step).start()

        @pl.when(step >= 2)
        def _():
            chip_stage(step - 2)

        @pl.when(step >= FINAL_LAG)
        def _():
            final_stage(step - FINAL_LAG)

    load_v(last, lax.rem(last, RING)).wait()
    attend(last, False)
    give_part(last).start()
    give_stat(last).start()

    @pl.loop(last - 2, num_chunks)
    def _(step):
        chip_stage(step)

    @pl.loop(last - FINAL_LAG, num_chunks)
    def _(step):
        final_stage(step)

    @pl.loop(0, num_chunks)
    def _(step):
        q_to_far(step, me).wait_send()
        q_to_sib(step, me).wait_send()
        q_forward(step, far).wait_send()
        give_part(step).wait_send()
        give_stat(step).wait_send()
        give_out(step).wait_send()
        give_lse(step).wait_send()
        store_out(step).wait()


def solution(mesh):
    def group_step(q_local, k_span, v_span, len_local):
        num_batch, span, dim = k_span.shape
        n = num_batch // CHUNK
        f32, bf16 = jnp.float32, jnp.bfloat16
        dma = lambda *shape: pltpu.SemaphoreType.DMA(shape)
        hbm = pl.BlockSpec(memory_space=pltpu.HBM)
        out = pl.pallas_call(
            functools.partial(kernel, n, dim**-0.5),
            out_shape=jax.ShapeDtypeStruct((num_batch * ROWS, dim), bf16),
            in_specs=[pl.BlockSpec(memory_space=pltpu.SMEM), hbm, hbm, hbm],
            out_specs=hbm,
            scratch_shapes=[
                pltpu.VMEM((RING, CHUNK, span, dim), bf16),
                pltpu.VMEM((RING, CHUNK, span, dim), bf16),
                pltpu.VMEM((num_batch, 4 * ROWS, dim), bf16),
                pltpu.VMEM((CHUNK // 2, 64, span), f32),
                pltpu.VMEM((CHUNK // 2, 64, 128), f32),
                pltpu.VMEM((n, 2, 2, CHUNK, ROWS, dim), f32),
                pltpu.VMEM((n, 2, ROWS, dim), f32),
                pltpu.VMEM((n, 2, CHUNK, ROWS, dim), f32),
                pltpu.VMEM((n, 2, ROWS, dim), f32),
                pltpu.VMEM((n, CHUNK * ROWS, dim), bf16),
                pltpu.VMEM((n, ROWS, dim), f32),
                pltpu.VMEM((n, CHUNK * ROWS, dim), bf16),
                pltpu.VMEM((n, ROWS, dim), f32),
                pltpu.VMEM((n, ROWS, dim), f32),
                pltpu.VMEM((n, CHUNK * ROWS, dim), bf16),
                dma(RING),
                dma(RING),
            ]
            + [dma(n)] * 16,
            compiler_params=pltpu.CompilerParams(
                collective_id=0, has_side_effects=True, vmem_limit_bytes=60 * 1024 * 1024
            ),
        )(len_local, q_local, k_span, v_span)
        return out.reshape(num_batch, ROWS, dim)

    return jax.shard_map(
        group_step,
        mesh=mesh,
        in_specs=(P("kv", "dup", None), P("kv", "dup", None), P("kv", "dup", None), P("kv")),
        out_specs=P("kv", "dup", None),
        check_vma=False,
    )
```

```python
import functools
import math

import jax
import jax.numpy as jnp
from jax import lax
from jax.experimental import pallas as pl
from jax.experimental.pallas import tpu as pltpu
from jax.sharding import PartitionSpec as P

DRAFT = 4
CHUNK = 16
RING = 6
AHEAD = 2
EARLY_FINALS = 8
ROWS = 8
OWN, FAR, SIB, FAR_SIB = range(4)
MESH = pl.DeviceIdType.MESH
LOWEST = -3.0e38
FLOOR = -2.0e38


def kernel(
    num_chunks,
    scale,
    len_ref,
    q_hbm,
    k_hbm,
    v_hbm,
    out_hbm,
    kbuf,
    vbuf,
    qbuf,
    sbuf,
    pbuf,
    keep,
    give,
    peer,
    stat,
    peer_stat,
    own_out,
    send_out,
    send_lse,
    recv_out,
    recv_lse,
    own_lse,
    out_buf,
    k_sem,
    v_sem,
    q_local,
    q_chip_send,
    q_chip_recv,
    q_sib_send,
    q_sib_recv,
    q_fwd_send,
    q_fwd_recv,
    part_send,
    part_recv,
    stat_send,
    stat_recv,
    o_send,
    o_recv,
    l_send,
    l_recv,
    out_sem,
):
    me = lax.axis_index("dup")
    chip, core = me // 2, lax.rem(me, 2)
    sib = 2 * chip + (1 - core)
    far = 2 * (1 - chip) + core
    span = kbuf.shape[2]
    pairs = CHUNK // 2
    n = num_chunks

    def load_k(step, slot):
        return pltpu.make_async_copy(k_hbm.at[pl.ds(step * CHUNK, CHUNK)], kbuf.at[slot], k_sem.at[slot])

    def load_v(step, slot):
        return pltpu.make_async_copy(v_hbm.at[pl.ds(step * CHUNK, CHUNK)], vbuf.at[slot], v_sem.at[slot])

    def q_rows(step, role):
        return qbuf.at[pl.ds(step * CHUNK, CHUNK), pl.ds(role * ROWS, ROWS)]

    def q_mine(step):
        return q_hbm.at[pl.ds(step * CHUNK, CHUNK)]

    def keep_q(step):
        return pltpu.make_async_copy(q_mine(step), q_rows(step, OWN), q_local.at[step])

    def remote(src, dst, send, recv, dev):
        return pltpu.make_async_remote_copy(
            src_ref=src, dst_ref=dst, send_sem=send, recv_sem=recv, device_id={"dup": dev}, device_id_type=MESH
        )

    def q_to_far(step):
        return remote(q_mine(step), q_rows(step, FAR), q_chip_send.at[step], q_chip_recv.at[step], far)

    def q_to_sib(step):
        return remote(q_mine(step), q_rows(step, SIB), q_sib_send.at[step], q_sib_recv.at[step], sib)

    def q_forward(step):
        return remote(q_rows(step, FAR), q_rows(step, FAR_SIB), q_fwd_send.at[step], q_fwd_recv.at[step], sib)

    def give_part(step):
        return remote(give.at[step], peer.at[step], part_send.at[step], part_recv.at[step], sib)

    def give_stat(step):
        return remote(stat.at[step], peer_stat.at[step], stat_send.at[step], stat_recv.at[step], sib)

    def give_out(step):
        return remote(send_out.at[step], recv_out.at[step], o_send.at[step], o_recv.at[step], far)

    def give_lse(step):
        return remote(send_lse.at[step], recv_lse.at[step], l_send.at[step], l_recv.at[step], far)

    def store_out(step):
        return pltpu.make_async_copy(
            out_buf.at[step], out_hbm.at[pl.ds(step * CHUNK * ROWS, CHUNK * ROWS)], out_sem.at[step]
        )

    for step in range(RING):
        load_k(step, step).start()
        load_v(step, step).start()

    barrier = pltpu.get_barrier_semaphore()
    for dev in (sib, far):
        pl.semaphore_signal(barrier, inc=1, device_id={"dup": dev}, device_id_type=MESH)
    pl.semaphore_wait(barrier, 2)

    @pl.loop(0, n)
    def _(step):
        q_to_far(step).start()
        q_to_sib(step).start()
        keep_q(step).start()

    def forward_q(step):
        q_to_far(step).wait_recv()
        q_forward(step).start()

    def await_q(step):
        keep_q(step).wait()
        q_to_sib(step).wait_recv()
        q_forward(step).wait_recv()

    lane = lax.broadcasted_iota(jnp.int32, (ROWS, 128), 1)
    draft_of_row = lax.rem(lax.broadcasted_iota(jnp.int32, (ROWS, span), 0), DRAFT)
    reach = lax.broadcasted_iota(jnp.int32, (ROWS, span), 1) - draft_of_row + (me * span + DRAFT)
    rate = scale / math.log(2.0)

    def score_pair(step, slot, i):
        b = step * CHUNK + 2 * i
        q_a, q_b = qbuf[b], qbuf[b + 1]
        none = jnp.zeros_like(q_a)
        left = jnp.concatenate([jnp.concatenate([q_a, none], 1), jnp.concatenate([none, q_b], 1)], 0)
        right = jnp.concatenate([kbuf[slot, 2 * i], kbuf[slot, 2 * i + 1]], 1)
        return lax.dot_general(left, right, (((1,), (1,)), ((), ())), preferred_element_type=jnp.float32)

    def mask_pair(step, i, scores):
        for h in range(2):
            allowed = reach <= len_ref[step * CHUNK + 2 * i + h]
            for d in range(4):
                row = 32 * h + 8 * d
                s = jnp.where(allowed, scores[row : row + 8], LOWEST)
                sbuf[i, pl.ds(row, 8), :] = s
                peak = jnp.maximum(jnp.max(s, axis=1, keepdims=True), FLOOR)
                pbuf[i, pl.ds(row, 8), :] = jnp.broadcast_to(peak, (ROWS, 128))

    def attend_pair(step, slot, i, peaks, masses):
        probs = []
        for h in range(2):
            for d in range(4):
                row = 32 * h + 8 * d
                peak = pbuf[i, pl.ds(row, 8), :]
                s = sbuf[i, pl.ds(row, 8), :]
                p = jnp.exp2((s - jnp.concatenate([peak] * (span // 128), 1)) * rate)
                mass = jnp.sum(p, axis=1, keepdims=True)
                here = lane == (CHUNK * d + 2 * i + h)
                peaks = jnp.where(here, peak, peaks)
                masses = jnp.where(here, mass, masses)
                probs.append(p)
        p = jnp.concatenate(
            [jnp.concatenate(probs[j : j + 2], 0).astype(jnp.bfloat16) for j in range(0, 8, 2)], 0
        )
        v = jnp.concatenate([vbuf[slot, 2 * i], vbuf[slot, 2 * i + 1]], 1)
        o = lax.dot_general(p, v, (((1,), (0,)), ((), ())), preferred_element_type=jnp.float32)
        for h in range(2):
            for d in range(4):
                home = keep if d in (OWN, FAR) else give
                home[step, d % 2, 2 * i + h] = o[32 * h + 8 * d : 32 * h + 8 * d + 8, 128 * h : 128 * h + 128]
        return peaks, masses

    def merge_chip(step):
        m_a, l_a = stat[step, 0], stat[step, 1]
        m_b, l_b = (pltpu.roll(peer_stat[step, j], 128 - SIB * CHUNK, 1) for j in range(2))
        top = jnp.maximum(m_a, m_b)
        w_a, w_b = jnp.exp2((m_a - top) * rate), jnp.exp2((m_b - top) * rate)
        total = w_a * l_a + w_b * l_b
        some = total > 0.0
        safe = jnp.where(some, total, 1.0)
        inverse = jnp.where(some, 1.0 / safe, 0.0)
        w_a, w_b = w_a * inverse, w_b * inverse
        lse = jnp.where(some, top * rate + jnp.log2(safe), LOWEST)
        own_lse[step] = lse
        send_lse[step] = pltpu.roll(lse, 128 - FAR * CHUNK, 1)

        def both(role, b):
            c = role * CHUNK + b
            return w_a[:, c : c + 1] * keep[step, role, b] + w_b[:, c : c + 1] * peer[step, role, b]

        for i in range(pairs):
            for b in (2 * i, 2 * i + 1):
                own_out[step, b] = both(OWN, b)
            far_out = [both(FAR, b) for b in (2 * i, 2 * i + 1)]
            send_out[step, pl.ds(16 * i, 16), :] = jnp.concatenate(far_out, 0).astype(jnp.bfloat16)

    def merge_final(step):
        mine, theirs = own_lse[step], recv_lse[step]
        top = jnp.maximum(mine, theirs)
        w_a, w_b = jnp.exp2(mine - top), jnp.exp2(theirs - top)
        inverse = 1.0 / (w_a + w_b)
        w_a, w_b = w_a * inverse, w_b * inverse
        for i in range(pairs):
            other = recv_out[step, pl.ds(16 * i, 16), :].astype(jnp.float32)
            outs = []
            for h in range(2):
                b = 2 * i + h
                outs.append(w_a[:, b : b + 1] * own_out[step, b] + w_b[:, b : b + 1] * other[8 * h : 8 * h + 8])
            out_buf[step, pl.ds(16 * i, 16), :] = jnp.concatenate(outs, 0).astype(jnp.bfloat16)

    def await_peer(step):
        give_part(step).wait_recv()
        give_stat(step).wait_recv()

    def send_far(step):
        give_out(step).start()
        give_lse(step).start()

    def final_stage(step):
        give_out(step).wait_recv()
        give_lse(step).wait_recv()
        merge_final(step)
        store_out(step).start()

    def attend(step, with_next):
        slot, next_slot = lax.rem(step, RING), lax.rem(step + 1, RING)
        peaks = jnp.zeros((ROWS, 128), jnp.float32)
        masses = jnp.zeros((ROWS, 128), jnp.float32)
        for i in range(pairs):
            if with_next:
                scores = score_pair(step + 1, next_slot, i)
            peaks, masses = attend_pair(step, slot, i, peaks, masses)
            if with_next:
                mask_pair(step + 1, i, scores)
        stat[step, 0] = peaks
        stat[step, 1] = masses

    last = n - 1
    for step in range(AHEAD):
        forward_q(step)
    await_q(0)
    load_k(0, 0).wait()
    for i in range(pairs):
        mask_pair(0, i, score_pair(0, 0, i))
    load_k(RING, 0).start()

    @pl.loop(0, last)
    def _(step):
        @pl.when(step + AHEAD < n)
        def _():
            forward_q(step + AHEAD)

        await_q(step + 1)
        load_k(step + 1, lax.rem(step + 1, RING)).wait()
        load_v(step, lax.rem(step, RING)).wait()

        @pl.when(step >= 2)
        def _():
            await_peer(step - 2)

        ready = (step + n - 2) // n
        merge_chip(ready * (step - 2) + (1 - ready) * n)
        attend(step, True)

        @pl.when(step >= 2)
        def _():
            send_far(step - 2)

        @pl.when(step + 1 + RING < n)
        def _():
            load_k(step + 1 + RING, lax.rem(step + 1, RING)).start()

        @pl.when(step + RING < n)
        def _():
            load_v(step + RING, lax.rem(step, RING)).start()

        give_part(step).start()
        give_stat(step).start()

    load_v(last, lax.rem(last, RING)).wait()
    await_peer(last - 2)
    merge_chip(last - 2)
    attend(last, False)
    send_far(last - 2)
    give_part(last).start()
    give_stat(last).start()
    await_peer(last - 1)
    merge_chip(last - 1)
    send_far(last - 1)

    @pl.loop(0, EARLY_FINALS)
    def _(step):
        final_stage(step)

    await_peer(last)
    merge_chip(last)
    send_far(last)

    @pl.loop(EARLY_FINALS, n)
    def _(step):
        final_stage(step)

    @pl.loop(0, n)
    def _(step):
        q_to_far(step).wait_send()
        q_to_sib(step).wait_send()
        q_forward(step).wait_send()
        give_part(step).wait_send()
        give_stat(step).wait_send()
        give_out(step).wait_send()
        give_lse(step).wait_send()
        store_out(step).wait()


def solution(mesh):
    def group_step(q_local, k_span, v_span, len_local):
        num_batch, span, dim = k_span.shape
        n = num_batch // CHUNK
        f32, bf16 = jnp.float32, jnp.bfloat16
        dma = lambda *shape: pltpu.SemaphoreType.DMA(shape)
        hbm = pl.BlockSpec(memory_space=pltpu.HBM)
        out = pl.pallas_call(
            functools.partial(kernel, n, dim**-0.5),
            out_shape=jax.ShapeDtypeStruct((num_batch * ROWS, dim), bf16),
            in_specs=[pl.BlockSpec(memory_space=pltpu.SMEM), hbm, hbm, hbm],
            out_specs=hbm,
            scratch_shapes=[
                pltpu.VMEM((RING, CHUNK, span, dim), bf16),
                pltpu.VMEM((RING, CHUNK, span, dim), bf16),
                pltpu.VMEM((num_batch, 4 * ROWS, dim), bf16),
                pltpu.VMEM((CHUNK // 2, 64, span), f32),
                pltpu.VMEM((CHUNK // 2, 64, 128), f32),
                pltpu.VMEM((n + 1, 2, CHUNK, ROWS, dim), f32),
                pltpu.VMEM((n, 2, CHUNK, ROWS, dim), f32),
                pltpu.VMEM((n + 1, 2, CHUNK, ROWS, dim), f32),
                pltpu.VMEM((n + 1, 2, ROWS, dim), f32),
                pltpu.VMEM((n + 1, 2, ROWS, dim), f32),
                pltpu.VMEM((n + 1, CHUNK, ROWS, dim), f32),
                pltpu.VMEM((n + 1, CHUNK * ROWS, dim), bf16),
                pltpu.VMEM((n + 1, ROWS, dim), f32),
                pltpu.VMEM((n, CHUNK * ROWS, dim), bf16),
                pltpu.VMEM((n, ROWS, dim), f32),
                pltpu.VMEM((n + 1, ROWS, dim), f32),
                pltpu.VMEM((n, CHUNK * ROWS, dim), bf16),
                dma(RING),
                dma(RING),
            ]
            + [dma(n)] * 16,
            compiler_params=pltpu.CompilerParams(
                collective_id=0, has_side_effects=True, vmem_limit_bytes=60 * 1024 * 1024
            ),
        )(len_local, q_local, k_span, v_span)
        return out.reshape(num_batch, ROWS, dim)

    return jax.shard_map(
        group_step,
        mesh=mesh,
        in_specs=(P("kv", "dup", None), P("kv", "dup", None), P("kv", "dup", None), P("kv")),
        out_specs=P("kv", "dup", None),
        check_vma=False,
    )
```

```python
import functools
import math

import jax
import jax.numpy as jnp
from jax import lax
from jax.experimental import pallas as pl
from jax.experimental.pallas import tpu as pltpu
from jax.sharding import PartitionSpec as P

DRAFT = 4
CHUNK = 16
RING = 6
AHEAD = 2
EARLY_FINALS = 8
ROWS = 8
OWN, FAR, SIB, FAR_SIB = range(4)
MESH = pl.DeviceIdType.MESH
LOWEST = -3.0e38
FLOOR = -2.0e38


def kernel(
    num_chunks,
    scale,
    len_ref,
    q_hbm,
    k_hbm,
    v_hbm,
    out_hbm,
    kbuf,
    vbuf,
    qbuf,
    sbuf,
    pbuf,
    keep,
    give,
    peer,
    stat,
    peer_stat,
    own_out,
    send_out,
    send_lse,
    recv_out,
    recv_lse,
    own_lse,
    out_buf,
    k_sem,
    v_sem,
    q_local,
    q_chip_send,
    q_chip_recv,
    q_sib_send,
    q_sib_recv,
    q_fwd_send,
    q_fwd_recv,
    part_send,
    part_recv,
    stat_send,
    stat_recv,
    o_send,
    o_recv,
    l_send,
    l_recv,
    out_sem,
):
    me = lax.axis_index("dup")
    chip, core = me // 2, lax.rem(me, 2)
    sib = 2 * chip + (1 - core)
    far = 2 * (1 - chip) + core
    span = kbuf.shape[2]
    pairs = CHUNK // 2
    n = num_chunks

    def load_k(step, slot):
        return pltpu.make_async_copy(k_hbm.at[pl.ds(step * CHUNK, CHUNK)], kbuf.at[slot], k_sem.at[slot])

    def load_v(step, slot):
        return pltpu.make_async_copy(v_hbm.at[pl.ds(step * CHUNK, CHUNK)], vbuf.at[slot], v_sem.at[slot])

    def q_rows(step, role):
        return qbuf.at[role, pl.ds(step * CHUNK * ROWS, CHUNK * ROWS)]

    def q_mine(step):
        return q_hbm.at[pl.ds(step * CHUNK * ROWS, CHUNK * ROWS)]

    def keep_q(step):
        return pltpu.make_async_copy(q_mine(step), q_rows(step, OWN), q_local.at[step])

    def remote(src, dst, send, recv, dev):
        return pltpu.make_async_remote_copy(
            src_ref=src, dst_ref=dst, send_sem=send, recv_sem=recv, device_id={"dup": dev}, device_id_type=MESH
        )

    def q_to_far(step):
        return remote(q_mine(step), q_rows(step, FAR), q_chip_send.at[step], q_chip_recv.at[step], far)

    def q_to_sib(step):
        return remote(q_mine(step), q_rows(step, SIB), q_sib_send.at[step], q_sib_recv.at[step], sib)

    def q_forward(step):
        return remote(q_rows(step, FAR), q_rows(step, FAR_SIB), q_fwd_send.at[step], q_fwd_recv.at[step], sib)

    def give_part(step):
        return remote(give.at[step], peer.at[step], part_send.at[step], part_recv.at[step], sib)

    def give_stat(step):
        return remote(stat.at[step], peer_stat.at[step], stat_send.at[step], stat_recv.at[step], sib)

    def give_out(step):
        return remote(send_out.at[step], recv_out.at[step], o_send.at[step], o_recv.at[step], far)

    def give_lse(step):
        return remote(send_lse.at[step], recv_lse.at[step], l_send.at[step], l_recv.at[step], far)

    def store_out(step):
        return pltpu.make_async_copy(
            out_buf.at[step], out_hbm.at[pl.ds(step * CHUNK * ROWS, CHUNK * ROWS)], out_sem.at[step]
        )

    for step in range(RING):
        load_k(step, step).start()
        load_v(step, step).start()

    barrier = pltpu.get_barrier_semaphore()
    for dev in (sib, far):
        pl.semaphore_signal(barrier, inc=1, device_id={"dup": dev}, device_id_type=MESH)
    pl.semaphore_wait(barrier, 2)

    @pl.loop(0, n)
    def _(step):
        q_to_far(step).start()
        q_to_sib(step).start()
        keep_q(step).start()

    def forward_q(step):
        q_to_far(step).wait_recv()
        q_forward(step).start()

    def await_q(step):
        keep_q(step).wait()
        q_to_sib(step).wait_recv()
        q_forward(step).wait_recv()

    lane = lax.broadcasted_iota(jnp.int32, (ROWS, 128), 1)
    draft_of_row = lax.rem(lax.broadcasted_iota(jnp.int32, (ROWS, span), 0), DRAFT)
    reach = lax.broadcasted_iota(jnp.int32, (ROWS, span), 1) - draft_of_row + (me * span + DRAFT)
    rate = scale / math.log(2.0)

    first = lax.rem(lax.broadcasted_iota(jnp.int32, (16, 128), 0), 16) < ROWS
    of_first = jnp.where(first, 1.0, 0.0).astype(jnp.bfloat16)
    of_second = jnp.where(first, 0.0, 1.0).astype(jnp.bfloat16)

    def score_pair(step, slot, i):
        start = pl.multiple_of(step * CHUNK * ROWS, 16) + 16 * i
        q = [qbuf[role, pl.ds(start, 16), :] for role in range(4)]
        left = jnp.concatenate([jnp.concatenate([x * of_first, x * of_second], 1) for x in q], 0)
        right = jnp.concatenate([kbuf[slot, 2 * i], kbuf[slot, 2 * i + 1]], 1)
        return lax.dot_general(left, right, (((1,), (1,)), ((), ())), preferred_element_type=jnp.float32)

    def mask_pair(step, i, scores):
        for h in range(2):
            allowed = reach <= len_ref[step * CHUNK + 2 * i + h]
            for d in range(4):
                row = 16 * d + 8 * h
                s = jnp.where(allowed, scores[row : row + 8], LOWEST)
                sbuf[i, pl.ds(row, 8), :] = s
                peak = jnp.maximum(jnp.max(s, axis=1, keepdims=True), FLOOR)
                pbuf[i, pl.ds(row, 8), :] = jnp.broadcast_to(peak, (ROWS, 128))

    def attend_pair(step, slot, i, peaks, masses):
        probs = []
        for d in range(4):
            for h in range(2):
                row = 16 * d + 8 * h
                peak = pbuf[i, pl.ds(row, 8), :]
                s = sbuf[i, pl.ds(row, 8), :]
                p = jnp.exp2((s - jnp.concatenate([peak] * (span // 128), 1)) * rate)
                mass = jnp.sum(p, axis=1, keepdims=True)
                here = lane == (CHUNK * d + 2 * i + h)
                peaks = jnp.where(here, peak, peaks)
                masses = jnp.where(here, mass, masses)
                probs.append(p)
        p = jnp.concatenate(
            [jnp.concatenate(probs[j : j + 2], 0).astype(jnp.bfloat16) for j in range(0, 8, 2)], 0
        )
        v = jnp.concatenate([vbuf[slot, 2 * i], vbuf[slot, 2 * i + 1]], 1)
        o = lax.dot_general(p, v, (((1,), (0,)), ((), ())), preferred_element_type=jnp.float32)
        for h in range(2):
            for d in range(4):
                home = keep if d in (OWN, FAR) else give
                home[step, d % 2, 2 * i + h] = o[16 * d + 8 * h : 16 * d + 8 * h + 8, 128 * h : 128 * h + 128]
        return peaks, masses

    def merge_chip(step):
        m_a, l_a = stat[step, 0], stat[step, 1]
        m_b, l_b = (pltpu.roll(peer_stat[step, j], 128 - SIB * CHUNK, 1) for j in range(2))
        top = jnp.maximum(m_a, m_b)
        w_a, w_b = jnp.exp2((m_a - top) * rate), jnp.exp2((m_b - top) * rate)
        total = w_a * l_a + w_b * l_b
        some = total > 0.0
        safe = jnp.where(some, total, 1.0)
        inverse = jnp.where(some, 1.0 / safe, 0.0)
        w_a, w_b = w_a * inverse, w_b * inverse
        lse = jnp.where(some, top * rate + jnp.log2(safe), LOWEST)
        own_lse[step] = lse
        send_lse[step] = pltpu.roll(lse, 128 - FAR * CHUNK, 1)

        def both(role, b):
            c = role * CHUNK + b
            return w_a[:, c : c + 1] * keep[step, role, b] + w_b[:, c : c + 1] * peer[step, role, b]

        for i in range(pairs):
            for b in (2 * i, 2 * i + 1):
                own_out[step, b] = both(OWN, b)
            far_out = [both(FAR, b) for b in (2 * i, 2 * i + 1)]
            send_out[step, pl.ds(16 * i, 16), :] = jnp.concatenate(far_out, 0).astype(jnp.bfloat16)

    def merge_final(step):
        mine, theirs = own_lse[step], recv_lse[step]
        top = jnp.maximum(mine, theirs)
        w_a, w_b = jnp.exp2(mine - top), jnp.exp2(theirs - top)
        inverse = 1.0 / (w_a + w_b)
        w_a, w_b = w_a * inverse, w_b * inverse
        for i in range(pairs):
            other = recv_out[step, pl.ds(16 * i, 16), :].astype(jnp.float32)
            outs = []
            for h in range(2):
                b = 2 * i + h
                outs.append(w_a[:, b : b + 1] * own_out[step, b] + w_b[:, b : b + 1] * other[8 * h : 8 * h + 8])
            out_buf[step, pl.ds(16 * i, 16), :] = jnp.concatenate(outs, 0).astype(jnp.bfloat16)

    def await_peer(step):
        give_part(step).wait_recv()
        give_stat(step).wait_recv()

    def send_far(step):
        give_out(step).start()
        give_lse(step).start()

    def final_stage(step):
        give_out(step).wait_recv()
        give_lse(step).wait_recv()
        merge_final(step)
        store_out(step).start()

    def attend(step, with_next):
        slot, next_slot = lax.rem(step, RING), lax.rem(step + 1, RING)
        peaks = jnp.zeros((ROWS, 128), jnp.float32)
        masses = jnp.zeros((ROWS, 128), jnp.float32)
        for i in range(pairs):
            if with_next:
                scores = score_pair(step + 1, next_slot, i)
            peaks, masses = attend_pair(step, slot, i, peaks, masses)
            if with_next:
                mask_pair(step + 1, i, scores)
        stat[step, 0] = peaks
        stat[step, 1] = masses

    last = n - 1
    for step in range(AHEAD):
        forward_q(step)
    await_q(0)
    load_k(0, 0).wait()
    for i in range(pairs):
        mask_pair(0, i, score_pair(0, 0, i))
    load_k(RING, 0).start()

    @pl.loop(0, last)
    def _(step):
        @pl.when(step + AHEAD < n)
        def _():
            forward_q(step + AHEAD)

        await_q(step + 1)
        load_k(step + 1, lax.rem(step + 1, RING)).wait()
        load_v(step, lax.rem(step, RING)).wait()

        @pl.when(step >= 2)
        def _():
            await_peer(step - 2)

        ready = (step + n - 2) // n
        merge_chip(ready * (step - 2) + (1 - ready) * n)
        attend(step, True)

        @pl.when(step >= 2)
        def _():
            send_far(step - 2)

        @pl.when(step + 1 + RING < n)
        def _():
            load_k(step + 1 + RING, lax.rem(step + 1, RING)).start()

        @pl.when(step + RING < n)
        def _():
            load_v(step + RING, lax.rem(step, RING)).start()

        give_part(step).start()
        give_stat(step).start()

    load_v(last, lax.rem(last, RING)).wait()
    await_peer(last - 2)
    merge_chip(last - 2)
    attend(last, False)
    send_far(last - 2)
    give_part(last).start()
    give_stat(last).start()
    await_peer(last - 1)
    merge_chip(last - 1)
    send_far(last - 1)

    @pl.loop(0, EARLY_FINALS)
    def _(step):
        final_stage(step)

    await_peer(last)
    merge_chip(last)
    send_far(last)

    @pl.loop(EARLY_FINALS, n)
    def _(step):
        final_stage(step)

    @pl.loop(0, n)
    def _(step):
        q_to_far(step).wait_send()
        q_to_sib(step).wait_send()
        q_forward(step).wait_send()
        give_part(step).wait_send()
        give_stat(step).wait_send()
        give_out(step).wait_send()
        give_lse(step).wait_send()
        store_out(step).wait()


def solution(mesh):
    def group_step(q_local, k_span, v_span, len_local):
        num_batch, span, dim = k_span.shape
        n = num_batch // CHUNK
        f32, bf16 = jnp.float32, jnp.bfloat16
        dma = lambda *shape: pltpu.SemaphoreType.DMA(shape)
        hbm = pl.BlockSpec(memory_space=pltpu.HBM)
        out = pl.pallas_call(
            functools.partial(kernel, n, dim**-0.5),
            out_shape=jax.ShapeDtypeStruct((num_batch * ROWS, dim), bf16),
            in_specs=[pl.BlockSpec(memory_space=pltpu.SMEM), hbm, hbm, hbm],
            out_specs=hbm,
            scratch_shapes=[
                pltpu.VMEM((RING, CHUNK, span, dim), bf16),
                pltpu.VMEM((RING, CHUNK, span, dim), bf16),
                pltpu.VMEM((4, num_batch * ROWS, dim), bf16),
                pltpu.VMEM((CHUNK // 2, 64, span), f32),
                pltpu.VMEM((CHUNK // 2, 64, 128), f32),
                pltpu.VMEM((n + 1, 2, CHUNK, ROWS, dim), f32),
                pltpu.VMEM((n, 2, CHUNK, ROWS, dim), f32),
                pltpu.VMEM((n + 1, 2, CHUNK, ROWS, dim), f32),
                pltpu.VMEM((n + 1, 2, ROWS, dim), f32),
                pltpu.VMEM((n + 1, 2, ROWS, dim), f32),
                pltpu.VMEM((n + 1, CHUNK, ROWS, dim), f32),
                pltpu.VMEM((n + 1, CHUNK * ROWS, dim), bf16),
                pltpu.VMEM((n + 1, ROWS, dim), f32),
                pltpu.VMEM((n, CHUNK * ROWS, dim), bf16),
                pltpu.VMEM((n, ROWS, dim), f32),
                pltpu.VMEM((n + 1, ROWS, dim), f32),
                pltpu.VMEM((n, CHUNK * ROWS, dim), bf16),
                dma(RING),
                dma(RING),
            ]
            + [dma(n)] * 16,
            compiler_params=pltpu.CompilerParams(
                collective_id=0, has_side_effects=True, vmem_limit_bytes=60 * 1024 * 1024
            ),
        )(len_local, q_local.reshape(num_batch * ROWS, dim), k_span, v_span)
        return out.reshape(num_batch, ROWS, dim)

    return jax.shard_map(
        group_step,
        mesh=mesh,
        in_specs=(P("kv", "dup", None), P("kv", "dup", None), P("kv", "dup", None), P("kv")),
        out_specs=P("kv", "dup", None),
        check_vma=False,
    )
```

```python
import functools
import math

import jax
import jax.numpy as jnp
from jax import lax
from jax.experimental import pallas as pl
from jax.experimental.pallas import tpu as pltpu
from jax.sharding import PartitionSpec as P

DRAFT = 4
CHUNK = 16
RING = 6
AHEAD = 2
EARLY_FINALS = 8
ROWS = 8
OWN, FAR, SIB, FAR_SIB = range(4)
MESH = pl.DeviceIdType.MESH
LOWEST = -3.0e38
FLOOR = -2.0e38


def kernel(
    num_chunks,
    scale,
    len_ref,
    q_hbm,
    k_hbm,
    v_hbm,
    out_hbm,
    kbuf,
    vbuf,
    qbuf,
    sbuf,
    pbuf,
    keep,
    give,
    peer,
    stat,
    peer_stat,
    own_out,
    send_out,
    send_lse,
    recv_out,
    recv_lse,
    own_lse,
    out_buf,
    k_sem,
    v_sem,
    q_local,
    q_chip_send,
    q_chip_recv,
    q_sib_send,
    q_sib_recv,
    q_fwd_send,
    q_fwd_recv,
    part_send,
    part_recv,
    stat_send,
    stat_recv,
    o_send,
    o_recv,
    l_send,
    l_recv,
    out_sem,
):
    me = lax.axis_index("dup")
    chip, core = me // 2, lax.rem(me, 2)
    sib = 2 * chip + (1 - core)
    far = 2 * (1 - chip) + core
    span = kbuf.shape[2]
    pairs = CHUNK // 2
    n = num_chunks

    def load_k(step, slot):
        return pltpu.make_async_copy(k_hbm.at[pl.ds(step * CHUNK, CHUNK)], kbuf.at[slot], k_sem.at[slot])

    def load_v(step, slot):
        return pltpu.make_async_copy(v_hbm.at[pl.ds(step * CHUNK, CHUNK)], vbuf.at[slot], v_sem.at[slot])

    def q_rows(step, role):
        return qbuf.at[role, pl.ds(step * CHUNK * ROWS, CHUNK * ROWS)]

    def q_mine(step):
        return q_rows(step, OWN)

    def remote(src, dst, send, recv, dev):
        return pltpu.make_async_remote_copy(
            src_ref=src, dst_ref=dst, send_sem=send, recv_sem=recv, device_id={"dup": dev}, device_id_type=MESH
        )

    def q_to_far(step):
        return remote(q_mine(step), q_rows(step, FAR), q_chip_send.at[step], q_chip_recv.at[step], far)

    def q_to_sib(step):
        return remote(q_mine(step), q_rows(step, SIB), q_sib_send.at[step], q_sib_recv.at[step], sib)

    def q_forward(step):
        return remote(q_rows(step, FAR), q_rows(step, FAR_SIB), q_fwd_send.at[step], q_fwd_recv.at[step], sib)

    def give_part(step):
        return remote(give.at[step], peer.at[step], part_send.at[step], part_recv.at[step], sib)

    def give_stat(step):
        return remote(stat.at[step], peer_stat.at[step], stat_send.at[step], stat_recv.at[step], sib)

    def give_out(step):
        return remote(send_out.at[step], recv_out.at[step], o_send.at[step], o_recv.at[step], far)

    def give_lse(step):
        return remote(send_lse.at[step], recv_lse.at[step], l_send.at[step], l_recv.at[step], far)

    def store_out(step):
        return pltpu.make_async_copy(
            out_buf.at[step], out_hbm.at[pl.ds(step * CHUNK * ROWS, CHUNK * ROWS)], out_sem.at[step]
        )

    whole_q = pltpu.make_async_copy(q_hbm, qbuf.at[OWN], q_local.at[0])
    whole_q.start()
    for step in range(RING):
        load_k(step, step).start()
        load_v(step, step).start()

    barrier = pltpu.get_barrier_semaphore()
    for dev in (sib, far):
        pl.semaphore_signal(barrier, inc=1, device_id={"dup": dev}, device_id_type=MESH)
    pl.semaphore_wait(barrier, 2)
    whole_q.wait()
    q_to_far(0).start()
    q_to_far(1).start()

    @pl.loop(0, n)
    def _(step):
        q_to_sib(step).start()

    def forward_q(step):
        q_to_far(step).wait_recv()
        q_forward(step).start()

    def await_q(step):
        q_to_sib(step).wait_recv()
        q_forward(step).wait_recv()

    lane = lax.broadcasted_iota(jnp.int32, (ROWS, 128), 1)
    draft_of_row = lax.rem(lax.broadcasted_iota(jnp.int32, (ROWS, span), 0), DRAFT)
    reach = lax.broadcasted_iota(jnp.int32, (ROWS, span), 1) - draft_of_row + (me * span + DRAFT)
    rate = scale / math.log(2.0)

    first = lax.rem(lax.broadcasted_iota(jnp.int32, (16, 128), 0), 16) < ROWS
    of_first = jnp.where(first, 1.0, 0.0).astype(jnp.bfloat16)
    of_second = jnp.where(first, 0.0, 1.0).astype(jnp.bfloat16)

    def score_pair(step, slot, i):
        start = pl.multiple_of(step * CHUNK * ROWS, 16) + 16 * i
        q = [qbuf[role, pl.ds(start, 16), :] for role in range(4)]
        left = jnp.concatenate([jnp.concatenate([x * of_first, x * of_second], 1) for x in q], 0)
        right = jnp.concatenate([kbuf[slot, 2 * i], kbuf[slot, 2 * i + 1]], 1)
        return lax.dot_general(left, right, (((1,), (1,)), ((), ())), preferred_element_type=jnp.float32)

    def mask_pair(step, i, scores):
        for h in range(2):
            allowed = reach <= len_ref[step * CHUNK + 2 * i + h]
            for d in range(4):
                row = 16 * d + 8 * h
                s = jnp.where(allowed, scores[row : row + 8], LOWEST)
                sbuf[i, pl.ds(row, 8), :] = s
                peak = jnp.maximum(jnp.max(s, axis=1, keepdims=True), FLOOR)
                pbuf[i, pl.ds(row, 8), :] = jnp.broadcast_to(peak, (ROWS, 128))

    def attend_pair(step, slot, i, peaks, masses):
        probs = []
        for d in range(4):
            for h in range(2):
                row = 16 * d + 8 * h
                peak = pbuf[i, pl.ds(row, 8), :]
                s = sbuf[i, pl.ds(row, 8), :]
                p = jnp.exp2((s - jnp.concatenate([peak] * (span // 128), 1)) * rate)
                mass = jnp.sum(p, axis=1, keepdims=True)
                here = lane == (CHUNK * d + 2 * i + h)
                peaks = jnp.where(here, peak, peaks)
                masses = jnp.where(here, mass, masses)
                probs.append(p)
        p = jnp.concatenate(
            [jnp.concatenate(probs[j : j + 2], 0).astype(jnp.bfloat16) for j in range(0, 8, 2)], 0
        )
        v = jnp.concatenate([vbuf[slot, 2 * i], vbuf[slot, 2 * i + 1]], 1)
        o = lax.dot_general(p, v, (((1,), (0,)), ((), ())), preferred_element_type=jnp.float32)
        for h in range(2):
            for d in range(4):
                home = keep if d in (OWN, FAR) else give
                home[step, d % 2, 2 * i + h] = o[16 * d + 8 * h : 16 * d + 8 * h + 8, 128 * h : 128 * h + 128]
        return peaks, masses

    def merge_chip(step):
        m_a, l_a = stat[step, 0], stat[step, 1]
        m_b, l_b = (pltpu.roll(peer_stat[step, j], 128 - SIB * CHUNK, 1) for j in range(2))
        top = jnp.maximum(m_a, m_b)
        w_a, w_b = jnp.exp2((m_a - top) * rate), jnp.exp2((m_b - top) * rate)
        total = w_a * l_a + w_b * l_b
        some = total > 0.0
        safe = jnp.where(some, total, 1.0)
        inverse = jnp.where(some, 1.0 / safe, 0.0)
        w_a, w_b = w_a * inverse, w_b * inverse
        lse = jnp.where(some, top * rate + jnp.log2(safe), LOWEST)
        own_lse[step] = lse
        send_lse[step] = pltpu.roll(lse, 128 - FAR * CHUNK, 1)

        def both(role, b):
            c = role * CHUNK + b
            return w_a[:, c : c + 1] * keep[step, role, b] + w_b[:, c : c + 1] * peer[step, role, b]

        for i in range(pairs):
            for b in (2 * i, 2 * i + 1):
                own_out[step, b] = both(OWN, b)
            far_out = [both(FAR, b) for b in (2 * i, 2 * i + 1)]
            send_out[step, pl.ds(16 * i, 16), :] = jnp.concatenate(far_out, 0).astype(jnp.bfloat16)

    def merge_final(step):
        mine, theirs = own_lse[step], recv_lse[step]
        top = jnp.maximum(mine, theirs)
        w_a, w_b = jnp.exp2(mine - top), jnp.exp2(theirs - top)
        inverse = 1.0 / (w_a + w_b)
        w_a, w_b = w_a * inverse, w_b * inverse
        for i in range(pairs):
            other = recv_out[step, pl.ds(16 * i, 16), :].astype(jnp.float32)
            outs = []
            for h in range(2):
                b = 2 * i + h
                outs.append(w_a[:, b : b + 1] * own_out[step, b] + w_b[:, b : b + 1] * other[8 * h : 8 * h + 8])
            out_buf[step, pl.ds(16 * i, 16), :] = jnp.concatenate(outs, 0).astype(jnp.bfloat16)

    def await_peer(step):
        give_part(step).wait_recv()
        give_stat(step).wait_recv()

    def send_far(step):
        give_out(step).start()
        give_lse(step).start()

    def final_stage(step):
        give_out(step).wait_recv()
        give_lse(step).wait_recv()
        merge_final(step)
        store_out(step).start()

    def attend(step, with_next):
        slot, next_slot = lax.rem(step, RING), lax.rem(step + 1, RING)
        peaks = jnp.zeros((ROWS, 128), jnp.float32)
        masses = jnp.zeros((ROWS, 128), jnp.float32)
        for i in range(pairs):
            if with_next:
                scores = score_pair(step + 1, next_slot, i)
            peaks, masses = attend_pair(step, slot, i, peaks, masses)
            if with_next:
                mask_pair(step + 1, i, scores)
        stat[step, 0] = peaks
        stat[step, 1] = masses

    last = n - 1
    forward_q(0)
    q_to_far(2).start()
    forward_q(1)
    q_to_far(3).start()
    q_to_far(4).start()
    await_q(0)
    load_k(0, 0).wait()
    for i in range(pairs):
        mask_pair(0, i, score_pair(0, 0, i))
    load_k(RING, 0).start()

    @pl.loop(0, last)
    def _(step):
        @pl.when(step + 5 < n)
        def _():
            q_to_far(step + 5).start()

        @pl.when(step + AHEAD < n)
        def _():
            forward_q(step + AHEAD)

        await_q(step + 1)
        load_k(step + 1, lax.rem(step + 1, RING)).wait()
        load_v(step, lax.rem(step, RING)).wait()

        @pl.when(step >= 2)
        def _():
            await_peer(step - 2)

        ready = (step + n - 2) // n
        merge_chip(ready * (step - 2) + (1 - ready) * n)
        attend(step, True)

        @pl.when(step >= 2)
        def _():
            send_far(step - 2)

        @pl.when(step + 1 + RING < n)
        def _():
            load_k(step + 1 + RING, lax.rem(step + 1, RING)).start()

        @pl.when(step + RING < n)
        def _():
            load_v(step + RING, lax.rem(step, RING)).start()

        give_part(step).start()
        give_stat(step).start()

    load_v(last, lax.rem(last, RING)).wait()
    await_peer(last - 2)
    merge_chip(last - 2)
    attend(last, False)
    send_far(last - 2)
    give_part(last).start()
    give_stat(last).start()
    await_peer(last - 1)
    merge_chip(last - 1)
    send_far(last - 1)

    @pl.loop(0, EARLY_FINALS)
    def _(step):
        final_stage(step)

    await_peer(last)
    merge_chip(last)
    send_far(last)

    @pl.loop(EARLY_FINALS, n)
    def _(step):
        final_stage(step)

    @pl.loop(0, n)
    def _(step):
        q_to_far(step).wait_send()
        q_to_sib(step).wait_send()
        q_forward(step).wait_send()
        give_part(step).wait_send()
        give_stat(step).wait_send()
        give_out(step).wait_send()
        give_lse(step).wait_send()
        store_out(step).wait()


def solution(mesh):
    def group_step(q_local, k_span, v_span, len_local):
        num_batch, span, dim = k_span.shape
        n = num_batch // CHUNK
        f32, bf16 = jnp.float32, jnp.bfloat16
        dma = lambda *shape: pltpu.SemaphoreType.DMA(shape)
        hbm = pl.BlockSpec(memory_space=pltpu.HBM)
        out = pl.pallas_call(
            functools.partial(kernel, n, dim**-0.5),
            out_shape=jax.ShapeDtypeStruct((num_batch * ROWS, dim), bf16),
            in_specs=[pl.BlockSpec(memory_space=pltpu.SMEM), hbm, hbm, hbm],
            out_specs=hbm,
            scratch_shapes=[
                pltpu.VMEM((RING, CHUNK, span, dim), bf16),
                pltpu.VMEM((RING, CHUNK, span, dim), bf16),
                pltpu.VMEM((4, num_batch * ROWS, dim), bf16),
                pltpu.VMEM((CHUNK // 2, 64, span), f32),
                pltpu.VMEM((CHUNK // 2, 64, 128), f32),
                pltpu.VMEM((n + 1, 2, CHUNK, ROWS, dim), f32),
                pltpu.VMEM((n, 2, CHUNK, ROWS, dim), f32),
                pltpu.VMEM((n + 1, 2, CHUNK, ROWS, dim), f32),
                pltpu.VMEM((n + 1, 2, ROWS, dim), f32),
                pltpu.VMEM((n + 1, 2, ROWS, dim), f32),
                pltpu.VMEM((n + 1, CHUNK, ROWS, dim), f32),
                pltpu.VMEM((n + 1, CHUNK * ROWS, dim), bf16),
                pltpu.VMEM((n + 1, ROWS, dim), f32),
                pltpu.VMEM((n, CHUNK * ROWS, dim), bf16),
                pltpu.VMEM((n, ROWS, dim), f32),
                pltpu.VMEM((n + 1, ROWS, dim), f32),
                pltpu.VMEM((n, CHUNK * ROWS, dim), bf16),
                dma(RING),
                dma(RING),
                dma(1),
            ]
            + [dma(n)] * 15,
            compiler_params=pltpu.CompilerParams(
                collective_id=0, has_side_effects=True, vmem_limit_bytes=60 * 1024 * 1024
            ),
        )(len_local, q_local.reshape(num_batch * ROWS, dim), k_span, v_span)
        return out.reshape(num_batch, ROWS, dim)

    return jax.shard_map(
        group_step,
        mesh=mesh,
        in_specs=(P("kv", "dup", None), P("kv", "dup", None), P("kv", "dup", None), P("kv")),
        out_specs=P("kv", "dup", None),
        check_vma=False,
    )
```

```python
import functools
import math

import jax
import jax.numpy as jnp
from jax import lax
from jax.experimental import pallas as pl
from jax.experimental.pallas import tpu as pltpu
from jax.sharding import PartitionSpec as P

DRAFT = 4
CHUNK = 16
RING = 3
AHEAD = 2
EARLY_FINALS = 8
ROWS = 8
OWN, FAR, SIB, FAR_SIB = range(4)
MESH = pl.DeviceIdType.MESH
LOWEST = -3.0e38
FLOOR = -2.0e38


def kernel(
    num_chunks,
    scale,
    len_ref,
    q_hbm,
    k_hbm,
    v_hbm,
    out_hbm,
    kbuf,
    vbuf,
    qbuf,
    sbuf,
    pbuf,
    keep,
    give,
    peer,
    stat,
    peer_stat,
    own_out,
    send_out,
    send_lse,
    recv_out,
    recv_lse,
    own_lse,
    out_buf,
    k_sem,
    v_sem,
    q_local,
    q_chip_send,
    q_chip_recv,
    q_sib_send,
    q_sib_recv,
    q_fwd_send,
    q_fwd_recv,
    part_send,
    part_recv,
    stat_send,
    stat_recv,
    o_send,
    o_recv,
    l_send,
    l_recv,
    out_sem,
):
    me = lax.axis_index("dup")
    chip, core = me // 2, lax.rem(me, 2)
    sib = 2 * chip + (1 - core)
    far = 2 * (1 - chip) + core
    span = kbuf.shape[2]
    pairs = CHUNK // 2
    n = num_chunks

    def load_k(step, slot):
        return pltpu.make_async_copy(k_hbm.at[pl.ds(step * CHUNK, CHUNK)], kbuf.at[slot], k_sem.at[slot])

    def load_v(step, slot):
        return pltpu.make_async_copy(v_hbm.at[pl.ds(step * CHUNK, CHUNK)], vbuf.at[slot], v_sem.at[slot])

    def q_rows(step, role):
        return qbuf.at[role, pl.ds(step * CHUNK * ROWS, CHUNK * ROWS)]

    def q_mine(step):
        return q_rows(step, OWN)

    def remote(src, dst, send, recv, dev):
        return pltpu.make_async_remote_copy(
            src_ref=src, dst_ref=dst, send_sem=send, recv_sem=recv, device_id={"dup": dev}, device_id_type=MESH
        )

    def q_to_far(step):
        return remote(q_mine(step), q_rows(step, FAR), q_chip_send.at[step], q_chip_recv.at[step], far)

    def q_to_sib(step):
        return remote(q_mine(step), q_rows(step, SIB), q_sib_send.at[step], q_sib_recv.at[step], sib)

    def q_forward(step):
        return remote(q_rows(step, FAR), q_rows(step, FAR_SIB), q_fwd_send.at[step], q_fwd_recv.at[step], sib)

    def give_part(step):
        return remote(give.at[step], peer.at[step], part_send.at[step], part_recv.at[step], sib)

    def give_stat(step):
        return remote(stat.at[step], peer_stat.at[step], stat_send.at[step], stat_recv.at[step], sib)

    def give_out(step):
        return remote(send_out.at[step], recv_out.at[step], o_send.at[step], o_recv.at[step], far)

    def give_lse(step):
        return remote(send_lse.at[step], recv_lse.at[step], l_send.at[step], l_recv.at[step], far)

    def store_out(step):
        return pltpu.make_async_copy(
            out_buf.at[step], out_hbm.at[pl.ds(step * CHUNK * ROWS, CHUNK * ROWS)], out_sem.at[step]
        )

    whole_q = pltpu.make_async_copy(q_hbm, qbuf.at[OWN], q_local.at[0])
    whole_q.start()
    for step in range(RING):
        load_k(step, step).start()
        load_v(step, step).start()

    barrier = pltpu.get_barrier_semaphore()
    for dev in (sib, far):
        pl.semaphore_signal(barrier, inc=1, device_id={"dup": dev}, device_id_type=MESH)
    pl.semaphore_wait(barrier, 2)
    whole_q.wait()
    q_to_far(0).start()
    q_to_far(1).start()

    @pl.loop(0, n)
    def _(step):
        q_to_sib(step).start()

    def forward_q(step):
        q_to_far(step).wait_recv()
        q_forward(step).start()

    def await_q(step):
        q_to_sib(step).wait_recv()
        q_forward(step).wait_recv()

    lane = lax.broadcasted_iota(jnp.int32, (ROWS, 128), 1)
    draft_of_row = lax.rem(lax.broadcasted_iota(jnp.int32, (ROWS, span), 0), DRAFT)
    reach = lax.broadcasted_iota(jnp.int32, (ROWS, span), 1) - draft_of_row + (me * span + DRAFT)
    rate = scale / math.log(2.0)

    first = lax.rem(lax.broadcasted_iota(jnp.int32, (16, 128), 0), 16) < ROWS
    of_first = jnp.where(first, 1.0, 0.0).astype(jnp.bfloat16)
    of_second = jnp.where(first, 0.0, 1.0).astype(jnp.bfloat16)

    def score_pair(step, slot, i):
        start = pl.multiple_of(step * CHUNK * ROWS, 16) + 16 * i
        q = [qbuf[role, pl.ds(start, 16), :] for role in range(4)]
        left = jnp.concatenate([jnp.concatenate([x * of_first, x * of_second], 1) for x in q], 0)
        right = jnp.concatenate([kbuf[slot, 2 * i], kbuf[slot, 2 * i + 1]], 1)
        return lax.dot_general(left, right, (((1,), (1,)), ((), ())), preferred_element_type=jnp.float32)

    def mask_pair(step, i, scores):
        for h in range(2):
            allowed = reach <= len_ref[step * CHUNK + 2 * i + h]
            for d in range(4):
                row = 16 * d + 8 * h
                s = jnp.where(allowed, scores[row : row + 8], LOWEST)
                sbuf[i, pl.ds(row, 8), :] = s
                peak = jnp.maximum(jnp.max(s, axis=1, keepdims=True), FLOOR)
                pbuf[i, pl.ds(row, 8), :] = jnp.broadcast_to(peak, (ROWS, 128))

    def attend_pair(step, slot, i, peaks, masses):
        probs = []
        for d in range(4):
            for h in range(2):
                row = 16 * d + 8 * h
                peak = pbuf[i, pl.ds(row, 8), :]
                s = sbuf[i, pl.ds(row, 8), :]
                p = jnp.exp2((s - jnp.concatenate([peak] * (span // 128), 1)) * rate)
                mass = jnp.sum(p, axis=1, keepdims=True)
                here = lane == (CHUNK * d + 2 * i + h)
                peaks = jnp.where(here, peak, peaks)
                masses = jnp.where(here, mass, masses)
                probs.append(p)
        p = jnp.concatenate(
            [jnp.concatenate(probs[j : j + 2], 0).astype(jnp.bfloat16) for j in range(0, 8, 2)], 0
        )
        v = jnp.concatenate([vbuf[slot, 2 * i], vbuf[slot, 2 * i + 1]], 1)
        o = lax.dot_general(p, v, (((1,), (0,)), ((), ())), preferred_element_type=jnp.float32)
        for h in range(2):
            for d in range(4):
                home = keep if d in (OWN, FAR) else give
                home[step, d % 2, 2 * i + h] = o[16 * d + 8 * h : 16 * d + 8 * h + 8, 128 * h : 128 * h + 128]
        return peaks, masses

    def merge_chip(step):
        m_a, l_a = stat[step, 0], stat[step, 1]
        m_b, l_b = (pltpu.roll(peer_stat[step, j], 128 - SIB * CHUNK, 1) for j in range(2))
        top = jnp.maximum(m_a, m_b)
        w_a, w_b = jnp.exp2((m_a - top) * rate), jnp.exp2((m_b - top) * rate)
        total = w_a * l_a + w_b * l_b
        some = total > 0.0
        safe = jnp.where(some, total, 1.0)
        inverse = jnp.where(some, 1.0 / safe, 0.0)
        w_a, w_b = w_a * inverse, w_b * inverse
        lse = jnp.where(some, top * rate + jnp.log2(safe), LOWEST)
        own_lse[step] = lse
        send_lse[step] = pltpu.roll(lse, 128 - FAR * CHUNK, 1)

        def both(role, b):
            c = role * CHUNK + b
            return w_a[:, c : c + 1] * keep[step, role, b] + w_b[:, c : c + 1] * peer[step, role, b]

        for i in range(pairs):
            for b in (2 * i, 2 * i + 1):
                own_out[step, b] = both(OWN, b)
            far_out = [both(FAR, b) for b in (2 * i, 2 * i + 1)]
            send_out[step, pl.ds(16 * i, 16), :] = jnp.concatenate(far_out, 0).astype(jnp.bfloat16)

    def merge_final(step):
        mine, theirs = own_lse[step], recv_lse[step]
        top = jnp.maximum(mine, theirs)
        w_a, w_b = jnp.exp2(mine - top), jnp.exp2(theirs - top)
        inverse = 1.0 / (w_a + w_b)
        w_a, w_b = w_a * inverse, w_b * inverse
        for i in range(pairs):
            other = recv_out[step, pl.ds(16 * i, 16), :].astype(jnp.float32)
            outs = []
            for h in range(2):
                b = 2 * i + h
                outs.append(w_a[:, b : b + 1] * own_out[step, b] + w_b[:, b : b + 1] * other[8 * h : 8 * h + 8])
            out_buf[step, pl.ds(16 * i, 16), :] = jnp.concatenate(outs, 0).astype(jnp.bfloat16)

    def await_peer(step):
        give_part(step).wait_recv()
        give_stat(step).wait_recv()

    def send_far(step):
        give_out(step).start()
        give_lse(step).start()

    def final_stage(step):
        give_out(step).wait_recv()
        give_lse(step).wait_recv()
        merge_final(step)
        store_out(step).start()

    def attend(step, with_next):
        slot, next_slot = lax.rem(step, RING), lax.rem(step + 1, RING)
        peaks = jnp.zeros((ROWS, 128), jnp.float32)
        masses = jnp.zeros((ROWS, 128), jnp.float32)
        for i in range(pairs):
            if with_next:
                scores = score_pair(step + 1, next_slot, i)
            peaks, masses = attend_pair(step, slot, i, peaks, masses)
            if with_next:
                mask_pair(step + 1, i, scores)
        stat[step, 0] = peaks
        stat[step, 1] = masses

    last = n - 1
    forward_q(0)
    q_to_far(2).start()
    forward_q(1)
    q_to_far(3).start()
    q_to_far(4).start()
    await_q(0)
    load_k(0, 0).wait()
    for i in range(pairs):
        mask_pair(0, i, score_pair(0, 0, i))
    load_k(RING, 0).start()

    @pl.loop(0, last)
    def _(step):
        @pl.when(step + 5 < n)
        def _():
            q_to_far(step + 5).start()

        @pl.when(step + AHEAD < n)
        def _():
            forward_q(step + AHEAD)

        await_q(step + 1)
        load_k(step + 1, lax.rem(step + 1, RING)).wait()
        load_v(step, lax.rem(step, RING)).wait()

        @pl.when(step >= 2)
        def _():
            await_peer(step - 2)

        ready = (step + n - 2) // n
        merge_chip(ready * (step - 2) + (1 - ready) * n)
        attend(step, True)

        @pl.when(step >= 2)
        def _():
            send_far(step - 2)

        @pl.when(step + 1 + RING < n)
        def _():
            load_k(step + 1 + RING, lax.rem(step + 1, RING)).start()

        @pl.when(step + RING < n)
        def _():
            load_v(step + RING, lax.rem(step, RING)).start()

        give_part(step).start()
        give_stat(step).start()

    load_v(last, lax.rem(last, RING)).wait()
    await_peer(last - 2)
    merge_chip(last - 2)
    attend(last, False)
    send_far(last - 2)
    give_part(last).start()
    give_stat(last).start()
    await_peer(last - 1)
    merge_chip(last - 1)
    send_far(last - 1)

    @pl.loop(0, EARLY_FINALS)
    def _(step):
        final_stage(step)

    await_peer(last)
    merge_chip(last)
    send_far(last)

    @pl.loop(EARLY_FINALS, n)
    def _(step):
        final_stage(step)

    @pl.loop(0, n)
    def _(step):
        q_to_far(step).wait_send()
        q_to_sib(step).wait_send()
        q_forward(step).wait_send()
        give_part(step).wait_send()
        give_stat(step).wait_send()
        give_out(step).wait_send()
        give_lse(step).wait_send()
        store_out(step).wait()


def solution(mesh):
    def group_step(q_local, k_span, v_span, len_local):
        num_batch, span, dim = k_span.shape
        n = num_batch // CHUNK
        f32, bf16 = jnp.float32, jnp.bfloat16
        dma = lambda *shape: pltpu.SemaphoreType.DMA(shape)
        hbm = pl.BlockSpec(memory_space=pltpu.HBM)
        out = pl.pallas_call(
            functools.partial(kernel, n, dim**-0.5),
            out_shape=jax.ShapeDtypeStruct((num_batch * ROWS, dim), bf16),
            in_specs=[pl.BlockSpec(memory_space=pltpu.SMEM), hbm, hbm, hbm],
            out_specs=hbm,
            scratch_shapes=[
                pltpu.VMEM((RING, CHUNK, span, dim), bf16),
                pltpu.VMEM((RING, CHUNK, span, dim), bf16),
                pltpu.VMEM((4, num_batch * ROWS, dim), bf16),
                pltpu.VMEM((CHUNK // 2, 64, span), f32),
                pltpu.VMEM((CHUNK // 2, 64, 128), f32),
                pltpu.VMEM((n + 1, 2, CHUNK, ROWS, dim), f32),
                pltpu.VMEM((n, 2, CHUNK, ROWS, dim), f32),
                pltpu.VMEM((n + 1, 2, CHUNK, ROWS, dim), f32),
                pltpu.VMEM((n + 1, 2, ROWS, dim), f32),
                pltpu.VMEM((n + 1, 2, ROWS, dim), f32),
                pltpu.VMEM((n + 1, CHUNK, ROWS, dim), f32),
                pltpu.VMEM((n + 1, CHUNK * ROWS, dim), bf16),
                pltpu.VMEM((n + 1, ROWS, dim), f32),
                pltpu.VMEM((n, CHUNK * ROWS, dim), bf16),
                pltpu.VMEM((n, ROWS, dim), f32),
                pltpu.VMEM((n + 1, ROWS, dim), f32),
                pltpu.VMEM((n, CHUNK * ROWS, dim), bf16),
                dma(RING),
                dma(RING),
                dma(1),
            ]
            + [dma(n)] * 15,
            compiler_params=pltpu.CompilerParams(
                collective_id=0, has_side_effects=True, vmem_limit_bytes=60 * 1024 * 1024
            ),
        )(len_local, q_local.reshape(num_batch * ROWS, dim), k_span, v_span)
        return out.reshape(num_batch, ROWS, dim)

    return jax.shard_map(
        group_step,
        mesh=mesh,
        in_specs=(P("kv", "dup", None), P("kv", "dup", None), P("kv", "dup", None), P("kv")),
        out_specs=P("kv", "dup", None),
        check_vma=False,
    )
```

```python
import functools
import math

import jax
import jax.numpy as jnp
from jax import lax
from jax.experimental import pallas as pl
from jax.experimental.pallas import tpu as pltpu
from jax.sharding import PartitionSpec as P

DRAFT = 4
CHUNK = 16
RING = 6
AHEAD = 2
EARLY_FINALS = 8
ROWS = 8
OWN, FAR, SIB, FAR_SIB = range(4)
MESH = pl.DeviceIdType.MESH
LOWEST = -3.0e38
FLOOR = -2.0e38


def kernel(
    num_chunks,
    scale,
    len_ref,
    q_hbm,
    k_hbm,
    v_hbm,
    out_hbm,
    kbuf,
    vbuf,
    qbuf,
    sbuf,
    pbuf,
    keep,
    give,
    peer,
    stat,
    peer_stat,
    own_out,
    send_out,
    send_lse,
    recv_out,
    recv_lse,
    own_lse,
    out_buf,
    k_sem,
    v_sem,
    q_local,
    q_chip_send,
    q_chip_recv,
    q_sib_send,
    q_sib_recv,
    q_fwd_send,
    q_fwd_recv,
    part_send,
    part_recv,
    stat_send,
    stat_recv,
    o_send,
    o_recv,
    l_send,
    l_recv,
    out_sem,
):
    me = lax.axis_index("dup")
    chip, core = me // 2, lax.rem(me, 2)
    sib = 2 * chip + (1 - core)
    far = 2 * (1 - chip) + core
    span = kbuf.shape[2]
    pairs = CHUNK // 2
    n = num_chunks

    def load_k(step, slot):
        return pltpu.make_async_copy(k_hbm.at[pl.ds(step * CHUNK, CHUNK)], kbuf.at[slot], k_sem.at[slot])

    def load_v(step, slot):
        return pltpu.make_async_copy(v_hbm.at[pl.ds(step * CHUNK, CHUNK)], vbuf.at[slot], v_sem.at[slot])

    def q_rows(step, role):
        return qbuf.at[role, pl.ds(step * CHUNK * ROWS, CHUNK * ROWS)]

    def q_mine(step):
        return q_rows(step, OWN)

    def remote(src, dst, send, recv, dev):
        return pltpu.make_async_remote_copy(
            src_ref=src, dst_ref=dst, send_sem=send, recv_sem=recv, device_id={"dup": dev}, device_id_type=MESH
        )

    def q_to_far(step):
        return remote(q_mine(step), q_rows(step, FAR), q_chip_send.at[step], q_chip_recv.at[step], far)

    def q_to_sib(step):
        return remote(q_mine(step), q_rows(step, SIB), q_sib_send.at[step], q_sib_recv.at[step], sib)

    def q_forward(step):
        return remote(q_rows(step, FAR), q_rows(step, FAR_SIB), q_fwd_send.at[step], q_fwd_recv.at[step], sib)

    def give_part(step):
        return remote(give.at[step], peer.at[step], part_send.at[step], part_recv.at[step], sib)

    def give_stat(step):
        return remote(stat.at[step], peer_stat.at[step], stat_send.at[step], stat_recv.at[step], sib)

    def give_out(step):
        return remote(send_out.at[step], recv_out.at[step], o_send.at[step], o_recv.at[step], far)

    def give_lse(step):
        return remote(send_lse.at[step], recv_lse.at[step], l_send.at[step], l_recv.at[step], far)

    def store_out(step):
        return pltpu.make_async_copy(
            out_buf.at[step], out_hbm.at[pl.ds(step * CHUNK * ROWS, CHUNK * ROWS)], out_sem.at[step]
        )

    whole_q = pltpu.make_async_copy(q_hbm, qbuf.at[OWN], q_local.at[0])
    whole_q.start()
    load_k(0, 0).start()

    barrier = pltpu.get_barrier_semaphore()
    for dev in (sib, far):
        pl.semaphore_signal(barrier, inc=1, device_id={"dup": dev}, device_id_type=MESH)
    pl.semaphore_wait(barrier, 2)
    whole_q.wait()
    for step in range(4):
        q_to_far(step).start()

    @pl.loop(0, n)
    def _(step):
        q_to_sib(step).start()

    load_v(0, 0).start()
    for step in range(1, RING):
        load_k(step, step).start()
        load_v(step, step).start()

    def forward_q(step):
        q_to_far(step).wait_recv()
        q_forward(step).start()

    def await_q(step):
        q_to_sib(step).wait_recv()
        q_forward(step).wait_recv()

    lane = lax.broadcasted_iota(jnp.int32, (ROWS, 128), 1)
    draft_of_row = lax.rem(lax.broadcasted_iota(jnp.int32, (ROWS, span), 0), DRAFT)
    reach = lax.broadcasted_iota(jnp.int32, (ROWS, span), 1) - draft_of_row + (me * span + DRAFT)
    rate = scale / math.log(2.0)

    first = lax.rem(lax.broadcasted_iota(jnp.int32, (16, 128), 0), 16) < ROWS
    of_first = jnp.where(first, 1.0, 0.0).astype(jnp.bfloat16)
    of_second = jnp.where(first, 0.0, 1.0).astype(jnp.bfloat16)

    def score_pair(step, slot, i):
        start = pl.multiple_of(step * CHUNK * ROWS, 16) + 16 * i
        q = [qbuf[role, pl.ds(start, 16), :] for role in range(4)]
        left = jnp.concatenate([jnp.concatenate([x * of_first, x * of_second], 1) for x in q], 0)
        right = jnp.concatenate([kbuf[slot, 2 * i], kbuf[slot, 2 * i + 1]], 1)
        return lax.dot_general(left, right, (((1,), (1,)), ((), ())), preferred_element_type=jnp.float32)

    def mask_pair(step, i, scores):
        for h in range(2):
            allowed = reach <= len_ref[step * CHUNK + 2 * i + h]
            for d in range(4):
                row = 16 * d + 8 * h
                s = jnp.where(allowed, scores[row : row + 8], LOWEST)
                sbuf[i, pl.ds(row, 8), :] = s
                peak = jnp.maximum(jnp.max(s, axis=1, keepdims=True), FLOOR)
                pbuf[i, pl.ds(row, 8), :] = jnp.broadcast_to(peak, (ROWS, 128))

    def attend_pair(step, slot, i, peaks, masses):
        probs = []
        for d in range(4):
            for h in range(2):
                row = 16 * d + 8 * h
                peak = pbuf[i, pl.ds(row, 8), :]
                s = sbuf[i, pl.ds(row, 8), :]
                p = jnp.exp2((s - jnp.concatenate([peak] * (span // 128), 1)) * rate)
                mass = jnp.sum(p, axis=1, keepdims=True)
                here = lane == (CHUNK * d + 2 * i + h)
                peaks = jnp.where(here, peak, peaks)
                masses = jnp.where(here, mass, masses)
                probs.append(p)
        p = jnp.concatenate(
            [jnp.concatenate(probs[j : j + 2], 0).astype(jnp.bfloat16) for j in range(0, 8, 2)], 0
        )
        v = jnp.concatenate([vbuf[slot, 2 * i], vbuf[slot, 2 * i + 1]], 1)
        o = lax.dot_general(p, v, (((1,), (0,)), ((), ())), preferred_element_type=jnp.float32)
        for h in range(2):
            for d in range(4):
                home = keep if d in (OWN, FAR) else give
                home[step, d % 2, 2 * i + h] = o[16 * d + 8 * h : 16 * d + 8 * h + 8, 128 * h : 128 * h + 128]
        return peaks, masses

    def merge_chip(step):
        m_a, l_a = stat[step, 0], stat[step, 1]
        m_b, l_b = (pltpu.roll(peer_stat[step, j], 128 - SIB * CHUNK, 1) for j in range(2))
        top = jnp.maximum(m_a, m_b)
        w_a, w_b = jnp.exp2((m_a - top) * rate), jnp.exp2((m_b - top) * rate)
        total = w_a * l_a + w_b * l_b
        some = total > 0.0
        safe = jnp.where(some, total, 1.0)
        inverse = jnp.where(some, 1.0 / safe, 0.0)
        w_a, w_b = w_a * inverse, w_b * inverse
        lse = jnp.where(some, top * rate + jnp.log2(safe), LOWEST)
        own_lse[step] = lse
        send_lse[step] = pltpu.roll(lse, 128 - FAR * CHUNK, 1)

        def both(role, b):
            c = role * CHUNK + b
            return w_a[:, c : c + 1] * keep[step, role, b] + w_b[:, c : c + 1] * peer[step, role, b]

        for i in range(pairs):
            for b in (2 * i, 2 * i + 1):
                own_out[step, b] = both(OWN, b)
            far_out = [both(FAR, b) for b in (2 * i, 2 * i + 1)]
            send_out[step, pl.ds(16 * i, 16), :] = jnp.concatenate(far_out, 0).astype(jnp.bfloat16)

    def merge_final(step):
        mine, theirs = own_lse[step], recv_lse[step]
        top = jnp.maximum(mine, theirs)
        w_a, w_b = jnp.exp2(mine - top), jnp.exp2(theirs - top)
        inverse = 1.0 / (w_a + w_b)
        w_a, w_b = w_a * inverse, w_b * inverse
        for i in range(pairs):
            other = recv_out[step, pl.ds(16 * i, 16), :].astype(jnp.float32)
            outs = []
            for h in range(2):
                b = 2 * i + h
                outs.append(w_a[:, b : b + 1] * own_out[step, b] + w_b[:, b : b + 1] * other[8 * h : 8 * h + 8])
            out_buf[step, pl.ds(16 * i, 16), :] = jnp.concatenate(outs, 0).astype(jnp.bfloat16)

    def await_peer(step):
        give_part(step).wait_recv()
        give_stat(step).wait_recv()

    def send_far(step):
        give_out(step).start()
        give_lse(step).start()

    def final_stage(step):
        give_out(step).wait_recv()
        give_lse(step).wait_recv()
        merge_final(step)
        store_out(step).start()

    def attend(step, with_next):
        slot, next_slot = lax.rem(step, RING), lax.rem(step + 1, RING)
        peaks = jnp.zeros((ROWS, 128), jnp.float32)
        masses = jnp.zeros((ROWS, 128), jnp.float32)
        for i in range(pairs):
            if with_next:
                scores = score_pair(step + 1, next_slot, i)
            peaks, masses = attend_pair(step, slot, i, peaks, masses)
            if with_next:
                mask_pair(step + 1, i, scores)
        stat[step, 0] = peaks
        stat[step, 1] = masses

    last = n - 1
    for step in range(AHEAD):
        forward_q(step)
        q_to_far(2 * step + 4).start()
        q_to_far(2 * step + 5).start()
    await_q(0)
    load_k(0, 0).wait()
    for i in range(pairs):
        mask_pair(0, i, score_pair(0, 0, i))
    load_k(RING, 0).start()

    @pl.loop(0, last)
    def _(step):
        @pl.when(2 * step + 2 * AHEAD + 4 < n)
        def _():
            q_to_far(2 * step + 2 * AHEAD + 4).start()
            q_to_far(2 * step + 2 * AHEAD + 5).start()

        @pl.when(step + AHEAD < n)
        def _():
            forward_q(step + AHEAD)

        await_q(step + 1)
        load_k(step + 1, lax.rem(step + 1, RING)).wait()
        load_v(step, lax.rem(step, RING)).wait()

        @pl.when(step >= 2)
        def _():
            await_peer(step - 2)

        ready = (step + n - 2) // n
        merge_chip(ready * (step - 2) + (1 - ready) * n)
        attend(step, True)

        @pl.when(step >= 2)
        def _():
            send_far(step - 2)

        @pl.when(step + 1 + RING < n)
        def _():
            load_k(step + 1 + RING, lax.rem(step + 1, RING)).start()

        @pl.when(step + RING < n)
        def _():
            load_v(step + RING, lax.rem(step, RING)).start()

        give_part(step).start()
        give_stat(step).start()

    load_v(last, lax.rem(last, RING)).wait()
    await_peer(last - 2)
    merge_chip(last - 2)
    attend(last, False)
    send_far(last - 2)
    give_part(last).start()
    give_stat(last).start()
    await_peer(last - 1)
    merge_chip(last - 1)
    send_far(last - 1)

    @pl.loop(0, EARLY_FINALS)
    def _(step):
        final_stage(step)

    await_peer(last)
    merge_chip(last)
    send_far(last)

    @pl.loop(EARLY_FINALS, n)
    def _(step):
        final_stage(step)

    @pl.loop(0, n)
    def _(step):
        q_to_far(step).wait_send()
        q_to_sib(step).wait_send()
        q_forward(step).wait_send()
        give_part(step).wait_send()
        give_stat(step).wait_send()
        give_out(step).wait_send()
        give_lse(step).wait_send()
        store_out(step).wait()


def solution(mesh):
    def group_step(q_local, k_span, v_span, len_local):
        num_batch, span, dim = k_span.shape
        n = num_batch // CHUNK
        f32, bf16 = jnp.float32, jnp.bfloat16
        dma = lambda *shape: pltpu.SemaphoreType.DMA(shape)
        hbm = pl.BlockSpec(memory_space=pltpu.HBM)
        out = pl.pallas_call(
            functools.partial(kernel, n, dim**-0.5),
            out_shape=jax.ShapeDtypeStruct((num_batch * ROWS, dim), bf16),
            in_specs=[pl.BlockSpec(memory_space=pltpu.SMEM), hbm, hbm, hbm],
            out_specs=hbm,
            scratch_shapes=[
                pltpu.VMEM((RING, CHUNK, span, dim), bf16),
                pltpu.VMEM((RING, CHUNK, span, dim), bf16),
                pltpu.VMEM((4, num_batch * ROWS, dim), bf16),
                pltpu.VMEM((CHUNK // 2, 64, span), f32),
                pltpu.VMEM((CHUNK // 2, 64, 128), f32),
                pltpu.VMEM((n + 1, 2, CHUNK, ROWS, dim), f32),
                pltpu.VMEM((n, 2, CHUNK, ROWS, dim), f32),
                pltpu.VMEM((n + 1, 2, CHUNK, ROWS, dim), f32),
                pltpu.VMEM((n + 1, 2, ROWS, dim), f32),
                pltpu.VMEM((n + 1, 2, ROWS, dim), f32),
                pltpu.VMEM((n + 1, CHUNK, ROWS, dim), f32),
                pltpu.VMEM((n + 1, CHUNK * ROWS, dim), bf16),
                pltpu.VMEM((n + 1, ROWS, dim), f32),
                pltpu.VMEM((n, CHUNK * ROWS, dim), bf16),
                pltpu.VMEM((n, ROWS, dim), f32),
                pltpu.VMEM((n + 1, ROWS, dim), f32),
                pltpu.VMEM((n, CHUNK * ROWS, dim), bf16),
                dma(RING),
                dma(RING),
                dma(1),
            ]
            + [dma(n)] * 15,
            compiler_params=pltpu.CompilerParams(
                collective_id=0, has_side_effects=True, vmem_limit_bytes=60 * 1024 * 1024
            ),
        )(len_local, q_local.reshape(num_batch * ROWS, dim), k_span, v_span)
        return out.reshape(num_batch, ROWS, dim)

    return jax.shard_map(
        group_step,
        mesh=mesh,
        in_specs=(P("kv", "dup", None), P("kv", "dup", None), P("kv", "dup", None), P("kv")),
        out_specs=P("kv", "dup", None),
        check_vma=False,
    )
```

```python
import functools
import math

import jax
import jax.numpy as jnp
from jax import lax
from jax.experimental import pallas as pl
from jax.experimental.pallas import tpu as pltpu
from jax.sharding import PartitionSpec as P

DRAFT = 4
CHUNK = 16
RING = 2
AHEAD = 3
EARLY_FINALS = 8
ROWS = 8
OWN, FAR, SIB, FAR_SIB = range(4)
MESH = pl.DeviceIdType.MESH
LOWEST = -3.0e38
FLOOR = -2.0e38


def kernel(
    num_chunks,
    scale,
    len_ref,
    q_hbm,
    k_hbm,
    v_hbm,
    out_hbm,
    kbuf,
    vbuf,
    qbuf,
    sbuf,
    pbuf,
    keep,
    give,
    peer,
    stat,
    peer_stat,
    own_out,
    send_out,
    send_lse,
    recv_out,
    recv_lse,
    own_lse,
    out_buf,
    k_sem,
    v_sem,
    q_local,
    q_chip_send,
    q_chip_recv,
    q_sib_send,
    q_sib_recv,
    q_fwd_send,
    q_fwd_recv,
    part_send,
    part_recv,
    stat_send,
    stat_recv,
    o_send,
    o_recv,
    l_send,
    l_recv,
    out_sem,
):
    me = lax.axis_index("dup")
    chip, core = me // 2, lax.rem(me, 2)
    sib = 2 * chip + (1 - core)
    far = 2 * (1 - chip) + core
    span = kbuf.shape[2]
    pairs = CHUNK // 2
    n = num_chunks

    def load_k(step, slot):
        return pltpu.make_async_copy(k_hbm.at[pl.ds(step * CHUNK, CHUNK)], kbuf.at[slot], k_sem.at[slot])

    def load_v(step, slot):
        return pltpu.make_async_copy(v_hbm.at[pl.ds(step * CHUNK, CHUNK)], vbuf.at[slot], v_sem.at[slot])

    def q_rows(step, role):
        return qbuf.at[role, pl.ds(step * CHUNK * ROWS, CHUNK * ROWS)]

    def q_mine(step):
        return q_rows(step, OWN)

    def remote(src, dst, send, recv, dev):
        return pltpu.make_async_remote_copy(
            src_ref=src, dst_ref=dst, send_sem=send, recv_sem=recv, device_id={"dup": dev}, device_id_type=MESH
        )

    def q_to_far(step):
        return remote(q_mine(step), q_rows(step, FAR), q_chip_send.at[step], q_chip_recv.at[step], far)

    def q_to_sib(step):
        return remote(q_mine(step), q_rows(step, SIB), q_sib_send.at[step], q_sib_recv.at[step], sib)

    def q_forward(step):
        return remote(q_rows(step, FAR), q_rows(step, FAR_SIB), q_fwd_send.at[step], q_fwd_recv.at[step], sib)

    def give_part(step):
        return remote(give.at[step], peer.at[step], part_send.at[step], part_recv.at[step], sib)

    def give_stat(step):
        return remote(stat.at[step], peer_stat.at[step], stat_send.at[step], stat_recv.at[step], sib)

    def give_out(step):
        return remote(send_out.at[step], recv_out.at[step], o_send.at[step], o_recv.at[step], far)

    def give_lse(step):
        return remote(send_lse.at[step], recv_lse.at[step], l_send.at[step], l_recv.at[step], far)

    def store_out(step):
        return pltpu.make_async_copy(
            out_buf.at[step], out_hbm.at[pl.ds(step * CHUNK * ROWS, CHUNK * ROWS)], out_sem.at[step]
        )

    whole_q = pltpu.make_async_copy(q_hbm, qbuf.at[OWN], q_local.at[0])
    whole_q.start()
    load_k(0, 0).start()

    barrier = pltpu.get_barrier_semaphore()
    for dev in (sib, far):
        pl.semaphore_signal(barrier, inc=1, device_id={"dup": dev}, device_id_type=MESH)
    pl.semaphore_wait(barrier, 2)
    whole_q.wait()
    for step in range(4):
        q_to_far(step).start()

    @pl.loop(0, n)
    def _(step):
        q_to_sib(step).start()

    load_v(0, 0).start()
    for step in range(1, RING):
        load_k(step, step).start()
        load_v(step, step).start()

    def forward_q(step):
        q_to_far(step).wait_recv()
        q_forward(step).start()

    def await_q(step):
        q_to_sib(step).wait_recv()
        q_forward(step).wait_recv()

    lane = lax.broadcasted_iota(jnp.int32, (ROWS, 128), 1)
    draft_of_row = lax.rem(lax.broadcasted_iota(jnp.int32, (ROWS, span), 0), DRAFT)
    reach = lax.broadcasted_iota(jnp.int32, (ROWS, span), 1) - draft_of_row + (me * span + DRAFT)
    rate = scale / math.log(2.0)

    first = lax.rem(lax.broadcasted_iota(jnp.int32, (16, 128), 0), 16) < ROWS
    of_first = jnp.where(first, 1.0, 0.0).astype(jnp.bfloat16)
    of_second = jnp.where(first, 0.0, 1.0).astype(jnp.bfloat16)

    def score_pair(step, slot, i):
        start = pl.multiple_of(step * CHUNK * ROWS, 16) + 16 * i
        q = [qbuf[role, pl.ds(start, 16), :] for role in range(4)]
        left = jnp.concatenate([jnp.concatenate([x * of_first, x * of_second], 1) for x in q], 0)
        right = jnp.concatenate([kbuf[slot, 2 * i], kbuf[slot, 2 * i + 1]], 1)
        return lax.dot_general(left, right, (((1,), (1,)), ((), ())), preferred_element_type=jnp.float32)

    def mask_pair(step, i, scores):
        for h in range(2):
            allowed = reach <= len_ref[step * CHUNK + 2 * i + h]
            for d in range(4):
                row = 16 * d + 8 * h
                s = jnp.where(allowed, scores[row : row + 8], LOWEST)
                sbuf[i, pl.ds(row, 8), :] = s
                peak = jnp.maximum(jnp.max(s, axis=1, keepdims=True), FLOOR)
                pbuf[i, pl.ds(row, 8), :] = jnp.broadcast_to(peak, (ROWS, 128))

    def attend_pair(step, slot, i, peaks, masses):
        probs = []
        for d in range(4):
            for h in range(2):
                row = 16 * d + 8 * h
                peak = pbuf[i, pl.ds(row, 8), :]
                s = sbuf[i, pl.ds(row, 8), :]
                p = jnp.exp2((s - jnp.concatenate([peak] * (span // 128), 1)) * rate)
                mass = jnp.sum(p, axis=1, keepdims=True)
                here = lane == (CHUNK * d + 2 * i + h)
                peaks = jnp.where(here, peak, peaks)
                masses = jnp.where(here, mass, masses)
                probs.append(p)
        p = jnp.concatenate(
            [jnp.concatenate(probs[j : j + 2], 0).astype(jnp.bfloat16) for j in range(0, 8, 2)], 0
        )
        v = jnp.concatenate([vbuf[slot, 2 * i], vbuf[slot, 2 * i + 1]], 1)
        o = lax.dot_general(p, v, (((1,), (0,)), ((), ())), preferred_element_type=jnp.float32)
        for h in range(2):
            for d in range(4):
                home = keep if d in (OWN, FAR) else give
                home[step, d % 2, 2 * i + h] = o[16 * d + 8 * h : 16 * d + 8 * h + 8, 128 * h : 128 * h + 128]
        return peaks, masses

    def merge_chip(step):
        m_a, l_a = stat[step, 0], stat[step, 1]
        m_b, l_b = (pltpu.roll(peer_stat[step, j], 128 - SIB * CHUNK, 1) for j in range(2))
        top = jnp.maximum(m_a, m_b)
        w_a, w_b = jnp.exp2((m_a - top) * rate), jnp.exp2((m_b - top) * rate)
        total = w_a * l_a + w_b * l_b
        some = total > 0.0
        safe = jnp.where(some, total, 1.0)
        inverse = jnp.where(some, 1.0 / safe, 0.0)
        w_a, w_b = w_a * inverse, w_b * inverse
        lse = jnp.where(some, top * rate + jnp.log2(safe), LOWEST)
        own_lse[step] = lse
        send_lse[step] = pltpu.roll(lse, 128 - FAR * CHUNK, 1)

        def both(role, b):
            c = role * CHUNK + b
            return w_a[:, c : c + 1] * keep[step, role, b] + w_b[:, c : c + 1] * peer[step, role, b]

        for i in range(pairs):
            for b in (2 * i, 2 * i + 1):
                own_out[step, b] = both(OWN, b)
            far_out = [both(FAR, b) for b in (2 * i, 2 * i + 1)]
            send_out[step, pl.ds(16 * i, 16), :] = jnp.concatenate(far_out, 0).astype(jnp.bfloat16)

    def merge_final(step):
        mine, theirs = own_lse[step], recv_lse[step]
        top = jnp.maximum(mine, theirs)
        w_a, w_b = jnp.exp2(mine - top), jnp.exp2(theirs - top)
        inverse = 1.0 / (w_a + w_b)
        w_a, w_b = w_a * inverse, w_b * inverse
        for i in range(pairs):
            other = recv_out[step, pl.ds(16 * i, 16), :].astype(jnp.float32)
            outs = []
            for h in range(2):
                b = 2 * i + h
                outs.append(w_a[:, b : b + 1] * own_out[step, b] + w_b[:, b : b + 1] * other[8 * h : 8 * h + 8])
            out_buf[step, pl.ds(16 * i, 16), :] = jnp.concatenate(outs, 0).astype(jnp.bfloat16)

    def await_peer(step):
        give_part(step).wait_recv()
        give_stat(step).wait_recv()

    def send_far(step):
        give_out(step).start()
        give_lse(step).start()

    def final_stage(step):
        give_out(step).wait_recv()
        give_lse(step).wait_recv()
        merge_final(step)
        store_out(step).start()

    def attend(step, with_next):
        slot, next_slot = lax.rem(step, RING), lax.rem(step + 1, RING)
        peaks = jnp.zeros((ROWS, 128), jnp.float32)
        masses = jnp.zeros((ROWS, 128), jnp.float32)
        for i in range(pairs):
            if with_next:
                scores = score_pair(step + 1, next_slot, i)
            peaks, masses = attend_pair(step, slot, i, peaks, masses)
            if with_next:
                mask_pair(step + 1, i, scores)
        stat[step, 0] = peaks
        stat[step, 1] = masses

    last = n - 1
    for step in range(AHEAD):
        forward_q(step)
        q_to_far(2 * step + 4).start()
        q_to_far(2 * step + 5).start()
    await_q(0)
    load_k(0, 0).wait()
    for i in range(pairs):
        mask_pair(0, i, score_pair(0, 0, i))
    load_k(RING, 0).start()

    @pl.loop(0, last)
    def _(step):
        @pl.when(2 * step + 2 * AHEAD + 4 < n)
        def _():
            q_to_far(2 * step + 2 * AHEAD + 4).start()
            q_to_far(2 * step + 2 * AHEAD + 5).start()

        @pl.when(step + AHEAD < n)
        def _():
            forward_q(step + AHEAD)

        await_q(step + 1)
        load_k(step + 1, lax.rem(step + 1, RING)).wait()
        load_v(step, lax.rem(step, RING)).wait()

        @pl.when(step >= 2)
        def _():
            await_peer(step - 2)

        ready = (step + n - 2) // n
        merge_chip(ready * (step - 2) + (1 - ready) * n)
        attend(step, True)

        @pl.when(step >= 2)
        def _():
            send_far(step - 2)

        @pl.when(step + 1 + RING < n)
        def _():
            load_k(step + 1 + RING, lax.rem(step + 1, RING)).start()

        @pl.when(step + RING < n)
        def _():
            load_v(step + RING, lax.rem(step, RING)).start()

        give_part(step).start()
        give_stat(step).start()

    load_v(last, lax.rem(last, RING)).wait()
    await_peer(last - 2)
    merge_chip(last - 2)
    attend(last, False)
    send_far(last - 2)
    give_part(last).start()
    give_stat(last).start()
    await_peer(last - 1)
    merge_chip(last - 1)
    send_far(last - 1)

    @pl.loop(0, EARLY_FINALS)
    def _(step):
        final_stage(step)

    await_peer(last)
    merge_chip(last)
    send_far(last)

    @pl.loop(EARLY_FINALS, n)
    def _(step):
        final_stage(step)

    @pl.loop(0, n)
    def _(step):
        q_to_far(step).wait_send()
        q_to_sib(step).wait_send()
        q_forward(step).wait_send()
        give_part(step).wait_send()
        give_stat(step).wait_send()
        give_out(step).wait_send()
        give_lse(step).wait_send()
        store_out(step).wait()


def solution(mesh):
    def group_step(q_local, k_span, v_span, len_local):
        num_batch, span, dim = k_span.shape
        n = num_batch // CHUNK
        f32, bf16 = jnp.float32, jnp.bfloat16
        dma = lambda *shape: pltpu.SemaphoreType.DMA(shape)
        hbm = pl.BlockSpec(memory_space=pltpu.HBM)
        out = pl.pallas_call(
            functools.partial(kernel, n, dim**-0.5),
            out_shape=jax.ShapeDtypeStruct((num_batch * ROWS, dim), bf16),
            in_specs=[pl.BlockSpec(memory_space=pltpu.SMEM), hbm, hbm, hbm],
            out_specs=hbm,
            scratch_shapes=[
                pltpu.VMEM((RING, CHUNK, span, dim), bf16),
                pltpu.VMEM((RING, CHUNK, span, dim), bf16),
                pltpu.VMEM((4, num_batch * ROWS, dim), bf16),
                pltpu.VMEM((CHUNK // 2, 64, span), f32),
                pltpu.VMEM((CHUNK // 2, 64, 128), f32),
                pltpu.VMEM((n + 1, 2, CHUNK, ROWS, dim), f32),
                pltpu.VMEM((n, 2, CHUNK, ROWS, dim), f32),
                pltpu.VMEM((n + 1, 2, CHUNK, ROWS, dim), f32),
                pltpu.VMEM((n + 1, 2, ROWS, dim), f32),
                pltpu.VMEM((n + 1, 2, ROWS, dim), f32),
                pltpu.VMEM((n + 1, CHUNK, ROWS, dim), f32),
                pltpu.VMEM((n + 1, CHUNK * ROWS, dim), bf16),
                pltpu.VMEM((n + 1, ROWS, dim), f32),
                pltpu.VMEM((n, CHUNK * ROWS, dim), bf16),
                pltpu.VMEM((n, ROWS, dim), f32),
                pltpu.VMEM((n + 1, ROWS, dim), f32),
                pltpu.VMEM((n, CHUNK * ROWS, dim), bf16),
                dma(RING),
                dma(RING),
                dma(1),
            ]
            + [dma(n)] * 15,
            compiler_params=pltpu.CompilerParams(
                collective_id=0, has_side_effects=True, vmem_limit_bytes=60 * 1024 * 1024
            ),
        )(len_local, q_local.reshape(num_batch * ROWS, dim), k_span, v_span)
        return out.reshape(num_batch, ROWS, dim)

    return jax.shard_map(
        group_step,
        mesh=mesh,
        in_specs=(P("kv", "dup", None), P("kv", "dup", None), P("kv", "dup", None), P("kv")),
        out_specs=P("kv", "dup", None),
        check_vma=False,
    )
```

```python
import functools
import math

import jax
import jax.numpy as jnp
from jax import lax
from jax.experimental import pallas as pl
from jax.experimental.pallas import tpu as pltpu
from jax.sharding import PartitionSpec as P

DRAFT = 4
CHUNK = 16
RING = 6
AHEAD = 2
LAG = 3
EARLY_FINALS = 8
ROWS = 8
OWN, FAR, SIB, FAR_SIB = range(4)
MESH = pl.DeviceIdType.MESH
LOWEST = -3.0e38
FLOOR = -2.0e38


def kernel(
    num_chunks,
    scale,
    len_ref,
    q_hbm,
    k_hbm,
    v_hbm,
    out_hbm,
    kbuf,
    vbuf,
    qbuf,
    sbuf,
    pbuf,
    keep,
    give,
    peer,
    stat,
    peer_stat,
    own_out,
    send_out,
    send_lse,
    recv_out,
    recv_lse,
    own_lse,
    out_buf,
    k_sem,
    v_sem,
    q_local,
    q_chip_send,
    q_chip_recv,
    q_sib_send,
    q_sib_recv,
    q_fwd_send,
    q_fwd_recv,
    part_send,
    part_recv,
    stat_send,
    stat_recv,
    o_send,
    o_recv,
    l_send,
    l_recv,
    out_sem,
):
    me = lax.axis_index("dup")
    chip, core = me // 2, lax.rem(me, 2)
    sib = 2 * chip + (1 - core)
    far = 2 * (1 - chip) + core
    span = kbuf.shape[2]
    pairs = CHUNK // 2
    n = num_chunks

    def load_k(step, slot):
        return pltpu.make_async_copy(k_hbm.at[pl.ds(step * CHUNK, CHUNK)], kbuf.at[slot], k_sem.at[slot])

    def load_v(step, slot):
        return pltpu.make_async_copy(v_hbm.at[pl.ds(step * CHUNK, CHUNK)], vbuf.at[slot], v_sem.at[slot])

    def q_rows(step, role):
        return qbuf.at[role, pl.ds(step * CHUNK * ROWS, CHUNK * ROWS)]

    def q_mine(step):
        return q_rows(step, OWN)

    def remote(src, dst, send, recv, dev):
        return pltpu.make_async_remote_copy(
            src_ref=src, dst_ref=dst, send_sem=send, recv_sem=recv, device_id={"dup": dev}, device_id_type=MESH
        )

    def q_to_far(step):
        return remote(q_mine(step), q_rows(step, FAR), q_chip_send.at[step], q_chip_recv.at[step], far)

    def q_to_sib(step):
        return remote(q_mine(step), q_rows(step, SIB), q_sib_send.at[step], q_sib_recv.at[step], sib)

    def q_forward(step):
        return remote(q_rows(step, FAR), q_rows(step, FAR_SIB), q_fwd_send.at[step], q_fwd_recv.at[step], sib)

    def give_part(step):
        return remote(give.at[step], peer.at[step], part_send.at[step], part_recv.at[step], sib)

    def give_stat(step):
        return remote(stat.at[step], peer_stat.at[step], stat_send.at[step], stat_recv.at[step], sib)

    def give_out(step):
        return remote(send_out.at[step], recv_out.at[step], o_send.at[step], o_recv.at[step], far)

    def give_lse(step):
        return remote(send_lse.at[step], recv_lse.at[step], l_send.at[step], l_recv.at[step], far)

    def store_out(step):
        return pltpu.make_async_copy(
            out_buf.at[step], out_hbm.at[pl.ds(step * CHUNK * ROWS, CHUNK * ROWS)], out_sem.at[step]
        )

    whole_q = pltpu.make_async_copy(q_hbm, qbuf.at[OWN], q_local.at[0])
    whole_q.start()
    load_k(0, 0).start()

    barrier = pltpu.get_barrier_semaphore()
    for dev in (sib, far):
        pl.semaphore_signal(barrier, inc=1, device_id={"dup": dev}, device_id_type=MESH)
    pl.semaphore_wait(barrier, 2)
    whole_q.wait()
    for step in range(4):
        q_to_far(step).start()

    @pl.loop(0, n)
    def _(step):
        q_to_sib(step).start()

    load_v(0, 0).start()
    for step in range(1, RING):
        load_k(step, step).start()
        load_v(step, step).start()

    def forward_q(step):
        q_to_far(step).wait_recv()
        q_forward(step).start()

    def await_q(step):
        q_to_sib(step).wait_recv()
        q_forward(step).wait_recv()

    lane = lax.broadcasted_iota(jnp.int32, (ROWS, 128), 1)
    draft_of_row = lax.rem(lax.broadcasted_iota(jnp.int32, (ROWS, span), 0), DRAFT)
    reach = lax.broadcasted_iota(jnp.int32, (ROWS, span), 1) - draft_of_row + (me * span + DRAFT)
    rate = scale / math.log(2.0)

    first = lax.rem(lax.broadcasted_iota(jnp.int32, (16, 128), 0), 16) < ROWS
    of_first = jnp.where(first, 1.0, 0.0).astype(jnp.bfloat16)
    of_second = jnp.where(first, 0.0, 1.0).astype(jnp.bfloat16)

    def score_pair(step, slot, i):
        start = pl.multiple_of(step * CHUNK * ROWS, 16) + 16 * i
        q = [qbuf[role, pl.ds(start, 16), :] for role in range(4)]
        left = jnp.concatenate([jnp.concatenate([x * of_first, x * of_second], 1) for x in q], 0)
        right = jnp.concatenate([kbuf[slot, 2 * i], kbuf[slot, 2 * i + 1]], 1)
        return lax.dot_general(left, right, (((1,), (1,)), ((), ())), preferred_element_type=jnp.float32)

    def mask_pair(step, i, scores):
        for h in range(2):
            allowed = reach <= len_ref[step * CHUNK + 2 * i + h]
            for d in range(4):
                row = 16 * d + 8 * h
                s = jnp.where(allowed, scores[row : row + 8], LOWEST)
                sbuf[i, pl.ds(row, 8), :] = s
                peak = jnp.maximum(jnp.max(s, axis=1, keepdims=True), FLOOR)
                pbuf[i, pl.ds(row, 8), :] = jnp.broadcast_to(peak, (ROWS, 128))

    def attend_pair(step, slot, i, peaks, masses):
        probs = []
        for d in range(4):
            for h in range(2):
                row = 16 * d + 8 * h
                peak = pbuf[i, pl.ds(row, 8), :]
                s = sbuf[i, pl.ds(row, 8), :]
                p = jnp.exp2((s - jnp.concatenate([peak] * (span // 128), 1)) * rate)
                mass = jnp.sum(p, axis=1, keepdims=True)
                here = lane == (CHUNK * d + 2 * i + h)
                peaks = jnp.where(here, peak, peaks)
                masses = jnp.where(here, mass, masses)
                probs.append(p)
        p = jnp.concatenate(
            [jnp.concatenate(probs[j : j + 2], 0).astype(jnp.bfloat16) for j in range(0, 8, 2)], 0
        )
        v = jnp.concatenate([vbuf[slot, 2 * i], vbuf[slot, 2 * i + 1]], 1)
        o = lax.dot_general(p, v, (((1,), (0,)), ((), ())), preferred_element_type=jnp.float32)
        for h in range(2):
            for d in range(4):
                home = keep if d in (OWN, FAR) else give
                home[step, d % 2, 2 * i + h] = o[16 * d + 8 * h : 16 * d + 8 * h + 8, 128 * h : 128 * h + 128]
        return peaks, masses

    def merge_chip(step):
        m_a, l_a = stat[step, 0], stat[step, 1]
        m_b, l_b = (pltpu.roll(peer_stat[step, j], 128 - SIB * CHUNK, 1) for j in range(2))
        top = jnp.maximum(m_a, m_b)
        w_a, w_b = jnp.exp2((m_a - top) * rate), jnp.exp2((m_b - top) * rate)
        total = w_a * l_a + w_b * l_b
        some = total > 0.0
        safe = jnp.where(some, total, 1.0)
        inverse = jnp.where(some, 1.0 / safe, 0.0)
        w_a, w_b = w_a * inverse, w_b * inverse
        lse = jnp.where(some, top * rate + jnp.log2(safe), LOWEST)
        own_lse[step] = lse
        send_lse[step] = pltpu.roll(lse, 128 - FAR * CHUNK, 1)

        def both(role, b):
            c = role * CHUNK + b
            return w_a[:, c : c + 1] * keep[step, role, b] + w_b[:, c : c + 1] * peer[step, role, b]

        for i in range(pairs):
            for b in (2 * i, 2 * i + 1):
                own_out[step, b] = both(OWN, b)
            far_out = [both(FAR, b) for b in (2 * i, 2 * i + 1)]
            send_out[step, pl.ds(16 * i, 16), :] = jnp.concatenate(far_out, 0).astype(jnp.bfloat16)

    def merge_final(step):
        mine, theirs = own_lse[step], recv_lse[step]
        top = jnp.maximum(mine, theirs)
        w_a, w_b = jnp.exp2(mine - top), jnp.exp2(theirs - top)
        inverse = 1.0 / (w_a + w_b)
        w_a, w_b = w_a * inverse, w_b * inverse
        for i in range(pairs):
            other = recv_out[step, pl.ds(16 * i, 16), :].astype(jnp.float32)
            outs = []
            for h in range(2):
                b = 2 * i + h
                outs.append(w_a[:, b : b + 1] * own_out[step, b] + w_b[:, b : b + 1] * other[8 * h : 8 * h + 8])
            out_buf[step, pl.ds(16 * i, 16), :] = jnp.concatenate(outs, 0).astype(jnp.bfloat16)

    def await_peer(step):
        give_part(step).wait_recv()
        give_stat(step).wait_recv()

    def send_far(step):
        give_out(step).start()
        give_lse(step).start()

    def final_stage(step):
        give_out(step).wait_recv()
        give_lse(step).wait_recv()
        merge_final(step)
        store_out(step).start()

    def attend(step, with_next):
        slot, next_slot = lax.rem(step, RING), lax.rem(step + 1, RING)
        peaks = jnp.zeros((ROWS, 128), jnp.float32)
        masses = jnp.zeros((ROWS, 128), jnp.float32)
        for i in range(pairs):
            if with_next:
                scores = score_pair(step + 1, next_slot, i)
            peaks, masses = attend_pair(step, slot, i, peaks, masses)
            if with_next:
                mask_pair(step + 1, i, scores)
        stat[step, 0] = peaks
        stat[step, 1] = masses

    last = n - 1
    for step in range(AHEAD):
        forward_q(step)
        q_to_far(2 * step + 4).start()
        q_to_far(2 * step + 5).start()
    await_q(0)
    load_k(0, 0).wait()
    for i in range(pairs):
        mask_pair(0, i, score_pair(0, 0, i))
    load_k(RING, 0).start()

    @pl.loop(0, last)
    def _(step):
        @pl.when(2 * step + 2 * AHEAD + 4 < n)
        def _():
            q_to_far(2 * step + 2 * AHEAD + 4).start()
            q_to_far(2 * step + 2 * AHEAD + 5).start()

        @pl.when(step + AHEAD < n)
        def _():
            forward_q(step + AHEAD)

        await_q(step + 1)
        load_k(step + 1, lax.rem(step + 1, RING)).wait()
        load_v(step, lax.rem(step, RING)).wait()

        @pl.when(step >= LAG)
        def _():
            await_peer(step - LAG)

        ready = (step + n - LAG) // n
        merge_chip(ready * (step - LAG) + (1 - ready) * n)
        attend(step, True)
        give_part(step).start()
        give_stat(step).start()

        @pl.when(step >= LAG)
        def _():
            send_far(step - LAG)

        @pl.when(step + 1 + RING < n)
        def _():
            load_k(step + 1 + RING, lax.rem(step + 1, RING)).start()

        @pl.when(step + RING < n)
        def _():
            load_v(step + RING, lax.rem(step, RING)).start()

    load_v(last, lax.rem(last, RING)).wait()
    await_peer(last - LAG)
    merge_chip(last - LAG)
    attend(last, False)
    give_part(last).start()
    give_stat(last).start()
    send_far(last - LAG)

    @pl.loop(last - LAG + 1, last)
    def _(step):
        await_peer(step)
        merge_chip(step)
        send_far(step)

    @pl.loop(0, EARLY_FINALS)
    def _(step):
        final_stage(step)

    await_peer(last)
    merge_chip(last)
    send_far(last)

    @pl.loop(EARLY_FINALS, n)
    def _(step):
        final_stage(step)

    @pl.loop(0, n)
    def _(step):
        q_to_far(step).wait_send()
        q_to_sib(step).wait_send()
        q_forward(step).wait_send()
        give_part(step).wait_send()
        give_stat(step).wait_send()
        give_out(step).wait_send()
        give_lse(step).wait_send()
        store_out(step).wait()


def solution(mesh):
    def group_step(q_local, k_span, v_span, len_local):
        num_batch, span, dim = k_span.shape
        n = num_batch // CHUNK
        f32, bf16 = jnp.float32, jnp.bfloat16
        dma = lambda *shape: pltpu.SemaphoreType.DMA(shape)
        hbm = pl.BlockSpec(memory_space=pltpu.HBM)
        out = pl.pallas_call(
            functools.partial(kernel, n, dim**-0.5),
            out_shape=jax.ShapeDtypeStruct((num_batch * ROWS, dim), bf16),
            in_specs=[pl.BlockSpec(memory_space=pltpu.SMEM), hbm, hbm, hbm],
            out_specs=hbm,
            scratch_shapes=[
                pltpu.VMEM((RING, CHUNK, span, dim), bf16),
                pltpu.VMEM((RING, CHUNK, span, dim), bf16),
                pltpu.VMEM((4, num_batch * ROWS, dim), bf16),
                pltpu.VMEM((CHUNK // 2, 64, span), f32),
                pltpu.VMEM((CHUNK // 2, 64, 128), f32),
                pltpu.VMEM((n + 1, 2, CHUNK, ROWS, dim), f32),
                pltpu.VMEM((n, 2, CHUNK, ROWS, dim), f32),
                pltpu.VMEM((n + 1, 2, CHUNK, ROWS, dim), f32),
                pltpu.VMEM((n + 1, 2, ROWS, dim), f32),
                pltpu.VMEM((n + 1, 2, ROWS, dim), f32),
                pltpu.VMEM((n + 1, CHUNK, ROWS, dim), f32),
                pltpu.VMEM((n + 1, CHUNK * ROWS, dim), bf16),
                pltpu.VMEM((n + 1, ROWS, dim), f32),
                pltpu.VMEM((n, CHUNK * ROWS, dim), bf16),
                pltpu.VMEM((n, ROWS, dim), f32),
                pltpu.VMEM((n + 1, ROWS, dim), f32),
                pltpu.VMEM((n, CHUNK * ROWS, dim), bf16),
                dma(RING),
                dma(RING),
                dma(1),
            ]
            + [dma(n)] * 15,
            compiler_params=pltpu.CompilerParams(
                collective_id=0, has_side_effects=True, vmem_limit_bytes=60 * 1024 * 1024
            ),
        )(len_local, q_local.reshape(num_batch * ROWS, dim), k_span, v_span)
        return out.reshape(num_batch, ROWS, dim)

    return jax.shard_map(
        group_step,
        mesh=mesh,
        in_specs=(P("kv", "dup", None), P("kv", "dup", None), P("kv", "dup", None), P("kv")),
        out_specs=P("kv", "dup", None),
        check_vma=False,
    )
```

```python
import functools
import math

import jax
import jax.numpy as jnp
from jax import lax
from jax.experimental import pallas as pl
from jax.experimental.pallas import tpu as pltpu
from jax.sharding import PartitionSpec as P

DRAFT = 4
CHUNK = 16
RING = 6
AHEAD = 2
LAG = 2
FINAL_LAG = 8
EARLY_FINALS = 4
PV_LAG = 2
ROWS = 8
OWN, FAR, SIB, FAR_SIB = range(4)
MESH = pl.DeviceIdType.MESH
LOWEST = -3.0e38
FLOOR = -2.0e38


def kernel(
    num_chunks,
    scale,
    len_ref,
    q_hbm,
    k_hbm,
    v_hbm,
    out_hbm,
    kbuf,
    vbuf,
    qbuf,
    sbuf,
    pbuf,
    ebuf,
    keep,
    give,
    peer,
    stat,
    peer_stat,
    own_out,
    send_out,
    send_lse,
    recv_out,
    recv_lse,
    own_lse,
    out_buf,
    k_sem,
    v_sem,
    q_local,
    q_chip_send,
    q_chip_recv,
    q_sib_send,
    q_sib_recv,
    q_fwd_send,
    q_fwd_recv,
    part_send,
    part_recv,
    stat_send,
    stat_recv,
    o_send,
    o_recv,
    l_send,
    l_recv,
    out_sem,
):
    me = lax.axis_index("dup")
    chip, core = me // 2, lax.rem(me, 2)
    sib = 2 * chip + (1 - core)
    far = 2 * (1 - chip) + core
    span = kbuf.shape[2]
    pairs = CHUNK // 2
    n = num_chunks

    def load_k(step, slot):
        return pltpu.make_async_copy(k_hbm.at[pl.ds(step * CHUNK, CHUNK)], kbuf.at[slot], k_sem.at[slot])

    def load_v(step, slot):
        return pltpu.make_async_copy(v_hbm.at[pl.ds(step * CHUNK, CHUNK)], vbuf.at[slot], v_sem.at[slot])

    def q_rows(step, role):
        return qbuf.at[role, pl.ds(step * CHUNK * ROWS, CHUNK * ROWS)]

    def q_mine(step):
        return q_rows(step, OWN)

    def remote(src, dst, send, recv, dev):
        return pltpu.make_async_remote_copy(
            src_ref=src, dst_ref=dst, send_sem=send, recv_sem=recv, device_id={"dup": dev}, device_id_type=MESH
        )

    def q_to_far(step):
        return remote(q_mine(step), q_rows(step, FAR), q_chip_send.at[step], q_chip_recv.at[step], far)

    def q_to_sib(step):
        return remote(q_mine(step), q_rows(step, SIB), q_sib_send.at[step], q_sib_recv.at[step], sib)

    def q_forward(step):
        return remote(q_rows(step, FAR), q_rows(step, FAR_SIB), q_fwd_send.at[step], q_fwd_recv.at[step], sib)

    def give_part(step):
        return remote(give.at[step], peer.at[step], part_send.at[step], part_recv.at[step], sib)

    def give_stat(step):
        return remote(stat.at[step], peer_stat.at[step], stat_send.at[step], stat_recv.at[step], sib)

    def give_out(step):
        return remote(send_out.at[step], recv_out.at[step], o_send.at[step], o_recv.at[step], far)

    def give_lse(step):
        return remote(send_lse.at[step], recv_lse.at[step], l_send.at[step], l_recv.at[step], far)

    def store_out(step):
        return pltpu.make_async_copy(
            out_buf.at[step], out_hbm.at[pl.ds(step * CHUNK * ROWS, CHUNK * ROWS)], out_sem.at[step]
        )

    whole_q = pltpu.make_async_copy(q_hbm, qbuf.at[OWN], q_local.at[0])
    whole_q.start()
    load_k(0, 0).start()

    barrier = pltpu.get_barrier_semaphore()
    for dev in (sib, far):
        pl.semaphore_signal(barrier, inc=1, device_id={"dup": dev}, device_id_type=MESH)
    pl.semaphore_wait(barrier, 2)
    whole_q.wait()
    for step in range(4):
        q_to_far(step).start()

    @pl.loop(0, n)
    def _(step):
        q_to_sib(step).start()

    load_v(0, 0).start()
    for step in range(1, RING):
        load_k(step, step).start()
        load_v(step, step).start()

    def forward_q(step):
        q_to_far(step).wait_recv()
        q_forward(step).start()

    def await_q(step):
        q_to_sib(step).wait_recv()
        q_forward(step).wait_recv()

    lane = lax.broadcasted_iota(jnp.int32, (ROWS, 128), 1)
    draft_of_row = lax.rem(lax.broadcasted_iota(jnp.int32, (ROWS, span), 0), DRAFT)
    reach = lax.broadcasted_iota(jnp.int32, (ROWS, span), 1) - draft_of_row + (me * span + DRAFT)
    rate = scale / math.log(2.0)

    first = lax.rem(lax.broadcasted_iota(jnp.int32, (16, 128), 0), 16) < ROWS
    of_first = jnp.where(first, 1.0, 0.0).astype(jnp.bfloat16)
    of_second = jnp.where(first, 0.0, 1.0).astype(jnp.bfloat16)

    def score_pair(step, slot, i):
        start = pl.multiple_of(step * CHUNK * ROWS, 16) + 16 * i
        q = [qbuf[role, pl.ds(start, 16), :] for role in range(4)]
        left = jnp.concatenate([jnp.concatenate([x * of_first, x * of_second], 1) for x in q], 0)
        right = jnp.concatenate([kbuf[slot, 2 * i], kbuf[slot, 2 * i + 1]], 1)
        return lax.dot_general(left, right, (((1,), (1,)), ((), ())), preferred_element_type=jnp.float32)

    def mask_pair(step, i, scores):
        for h in range(2):
            allowed = reach <= len_ref[step * CHUNK + 2 * i + h]
            for d in range(4):
                row = 16 * d + 8 * h
                s = jnp.where(allowed, scores[row : row + 8], LOWEST)
                sbuf[i, pl.ds(row, 8), :] = s
                peak = jnp.maximum(jnp.max(s, axis=1, keepdims=True), FLOOR)
                pbuf[i, pl.ds(row, 8), :] = jnp.broadcast_to(peak, (ROWS, 128))

    def weigh_pair(i, peaks, masses):
        for d in range(4):
            probs = []
            for h in range(2):
                row = 16 * d + 8 * h
                peak = pbuf[i, pl.ds(row, 8), :]
                s = sbuf[i, pl.ds(row, 8), :]
                p = jnp.exp2((s - jnp.concatenate([peak] * (span // 128), 1)) * rate)
                mass = jnp.sum(p, axis=1, keepdims=True)
                here = lane == (CHUNK * d + 2 * i + h)
                peaks = jnp.where(here, peak, peaks)
                masses = jnp.where(here, mass, masses)
                probs.append(p)
            ebuf[i, pl.ds(16 * d, 16), :] = jnp.concatenate(probs, 0).astype(jnp.bfloat16)
        return peaks, masses

    def sum_pair(step, slot, i):
        v = jnp.concatenate([vbuf[slot, 2 * i], vbuf[slot, 2 * i + 1]], 1)
        o = lax.dot_general(ebuf[i], v, (((1,), (0,)), ((), ())), preferred_element_type=jnp.float32)
        for h in range(2):
            for d in range(4):
                home = keep if d in (OWN, FAR) else give
                home[step, d % 2, 2 * i + h] = o[16 * d + 8 * h : 16 * d + 8 * h + 8, 128 * h : 128 * h + 128]

    def merge_chip(step):
        m_a, l_a = stat[step, 0], stat[step, 1]
        m_b, l_b = (pltpu.roll(peer_stat[step, j], 128 - SIB * CHUNK, 1) for j in range(2))
        top = jnp.maximum(m_a, m_b)
        w_a, w_b = jnp.exp2((m_a - top) * rate), jnp.exp2((m_b - top) * rate)
        total = w_a * l_a + w_b * l_b
        some = total > 0.0
        safe = jnp.where(some, total, 1.0)
        inverse = jnp.where(some, 1.0 / safe, 0.0)
        w_a, w_b = w_a * inverse, w_b * inverse
        lse = jnp.where(some, top * rate + jnp.log2(safe), LOWEST)
        own_lse[step] = lse
        send_lse[step] = pltpu.roll(lse, 128 - FAR * CHUNK, 1)

        def both(role, b):
            c = role * CHUNK + b
            return w_a[:, c : c + 1] * keep[step, role, b] + w_b[:, c : c + 1] * peer[step, role, b]

        for i in range(pairs):
            for b in (2 * i, 2 * i + 1):
                own_out[step, b] = both(OWN, b)
            far_out = [both(FAR, b) for b in (2 * i, 2 * i + 1)]
            send_out[step, pl.ds(16 * i, 16), :] = jnp.concatenate(far_out, 0).astype(jnp.bfloat16)

    def merge_final(step):
        mine, theirs = own_lse[step], recv_lse[step]
        top = jnp.maximum(mine, theirs)
        w_a, w_b = jnp.exp2(mine - top), jnp.exp2(theirs - top)
        inverse = 1.0 / (w_a + w_b)
        w_a, w_b = w_a * inverse, w_b * inverse
        for i in range(pairs):
            other = recv_out[step, pl.ds(16 * i, 16), :].astype(jnp.float32)
            outs = []
            for h in range(2):
                b = 2 * i + h
                outs.append(w_a[:, b : b + 1] * own_out[step, b] + w_b[:, b : b + 1] * other[8 * h : 8 * h + 8])
            out_buf[step, pl.ds(16 * i, 16), :] = jnp.concatenate(outs, 0).astype(jnp.bfloat16)

    def await_peer(step):
        give_part(step).wait_recv()
        give_stat(step).wait_recv()

    def send_far(step):
        give_out(step).start()
        give_lse(step).start()

    def await_far(step):
        give_out(step).wait_recv()
        give_lse(step).wait_recv()

    def final_stage(step):
        await_far(step)
        merge_final(step)
        store_out(step).start()

    def attend(step, with_next):
        slot, next_slot = lax.rem(step, RING), lax.rem(step + 1, RING)
        peaks = jnp.zeros((ROWS, 128), jnp.float32)
        masses = jnp.zeros((ROWS, 128), jnp.float32)
        scores = [None] * pairs
        for i in range(pairs + PV_LAG):
            if i < pairs:
                peaks, masses = weigh_pair(i, peaks, masses)
                if with_next:
                    scores[i] = score_pair(step + 1, next_slot, i)
            if i >= PV_LAG:
                sum_pair(step, slot, i - PV_LAG)
            if with_next and 1 <= i <= pairs:
                mask_pair(step + 1, i - 1, scores[i - 1])
        stat[step, 0] = peaks
        stat[step, 1] = masses

    last = n - 1
    for step in range(AHEAD):
        forward_q(step)
        q_to_far(2 * step + 4).start()
        q_to_far(2 * step + 5).start()
    await_q(0)
    load_k(0, 0).wait()
    for i in range(pairs):
        mask_pair(0, i, score_pair(0, 0, i))
    load_k(RING, 0).start()

    @pl.loop(0, last)
    def _(step):
        @pl.when(2 * step + 2 * AHEAD + 4 < n)
        def _():
            q_to_far(2 * step + 2 * AHEAD + 4).start()
            q_to_far(2 * step + 2 * AHEAD + 5).start()

        @pl.when(step + AHEAD < n)
        def _():
            forward_q(step + AHEAD)

        await_q(step + 1)
        load_k(step + 1, lax.rem(step + 1, RING)).wait()
        load_v(step, lax.rem(step, RING)).wait()

        @pl.when(step >= LAG)
        def _():
            await_peer(step - LAG)

        @pl.when(step >= FINAL_LAG)
        def _():
            await_far(step - FINAL_LAG)

        done = (step + n - FINAL_LAG) // n
        merge_final(done * (step - FINAL_LAG) + (1 - done) * n)
        ready = (step + n - LAG) // n
        merge_chip(ready * (step - LAG) + (1 - ready) * n)
        attend(step, True)
        give_part(step).start()
        give_stat(step).start()

        @pl.when(step >= LAG)
        def _():
            send_far(step - LAG)

        @pl.when(step >= FINAL_LAG)
        def _():
            store_out(step - FINAL_LAG).start()

        @pl.when(step + 1 + RING < n)
        def _():
            load_k(step + 1 + RING, lax.rem(step + 1, RING)).start()

        @pl.when(step + RING < n)
        def _():
            load_v(step + RING, lax.rem(step, RING)).start()

    load_v(last, lax.rem(last, RING)).wait()
    await_peer(last - LAG)
    await_far(last - FINAL_LAG)
    merge_final(last - FINAL_LAG)
    merge_chip(last - LAG)
    attend(last, False)
    store_out(last - FINAL_LAG).start()
    give_part(last).start()
    give_stat(last).start()
    send_far(last - LAG)

    @pl.loop(last - LAG + 1, last)
    def _(step):
        await_peer(step)
        merge_chip(step)
        send_far(step)

    @pl.loop(last - FINAL_LAG + 1, last - FINAL_LAG + 1 + EARLY_FINALS)
    def _(step):
        final_stage(step)

    await_peer(last)
    merge_chip(last)
    send_far(last)

    @pl.loop(last - FINAL_LAG + 1 + EARLY_FINALS, n)
    def _(step):
        final_stage(step)

    @pl.loop(0, n)
    def _(step):
        q_to_far(step).wait_send()
        q_to_sib(step).wait_send()
        q_forward(step).wait_send()
        give_part(step).wait_send()
        give_stat(step).wait_send()
        give_out(step).wait_send()
        give_lse(step).wait_send()
        store_out(step).wait()


def solution(mesh):
    def group_step(q_local, k_span, v_span, len_local):
        num_batch, span, dim = k_span.shape
        n = num_batch // CHUNK
        f32, bf16 = jnp.float32, jnp.bfloat16
        dma = lambda *shape: pltpu.SemaphoreType.DMA(shape)
        hbm = pl.BlockSpec(memory_space=pltpu.HBM)
        out = pl.pallas_call(
            functools.partial(kernel, n, dim**-0.5),
            out_shape=jax.ShapeDtypeStruct((num_batch * ROWS, dim), bf16),
            in_specs=[pl.BlockSpec(memory_space=pltpu.SMEM), hbm, hbm, hbm],
            out_specs=hbm,
            scratch_shapes=[
                pltpu.VMEM((RING, CHUNK, span, dim), bf16),
                pltpu.VMEM((RING, CHUNK, span, dim), bf16),
                pltpu.VMEM((4, num_batch * ROWS, dim), bf16),
                pltpu.VMEM((CHUNK // 2, 64, span), f32),
                pltpu.VMEM((CHUNK // 2, 64, 128), f32),
                pltpu.VMEM((CHUNK // 2, 64, span), bf16),
                pltpu.VMEM((n + 1, 2, CHUNK, ROWS, dim), f32),
                pltpu.VMEM((n, 2, CHUNK, ROWS, dim), f32),
                pltpu.VMEM((n + 1, 2, CHUNK, ROWS, dim), f32),
                pltpu.VMEM((n + 1, 2, ROWS, dim), f32),
                pltpu.VMEM((n + 1, 2, ROWS, dim), f32),
                pltpu.VMEM((n + 1, CHUNK, ROWS, dim), f32),
                pltpu.VMEM((n + 1, CHUNK * ROWS, dim), bf16),
                pltpu.VMEM((n + 1, ROWS, dim), f32),
                pltpu.VMEM((n + 1, CHUNK * ROWS, dim), bf16),
                pltpu.VMEM((n + 1, ROWS, dim), f32),
                pltpu.VMEM((n + 1, ROWS, dim), f32),
                pltpu.VMEM((n + 1, CHUNK * ROWS, dim), bf16),
                dma(RING),
                dma(RING),
                dma(1),
            ]
            + [dma(n)] * 15,
            compiler_params=pltpu.CompilerParams(
                collective_id=0, has_side_effects=True, vmem_limit_bytes=60 * 1024 * 1024
            ),
        )(len_local, q_local.reshape(num_batch * ROWS, dim), k_span, v_span)
        return out.reshape(num_batch, ROWS, dim)

    return jax.shard_map(
        group_step,
        mesh=mesh,
        in_specs=(P("kv", "dup", None), P("kv", "dup", None), P("kv", "dup", None), P("kv")),
        out_specs=P("kv", "dup", None),
        check_vma=False,
    )
```

```python
import functools
import math

import jax
import jax.numpy as jnp
from jax import lax
from jax.experimental import pallas as pl
from jax.experimental.pallas import tpu as pltpu
from jax.sharding import PartitionSpec as P

DRAFT = 4
CHUNK = 16
RING = 6
AHEAD = 2
LAG = 2
FINAL_LAG = 8
EARLY_FINALS = 4
PV_LAG = 2
ROWS = 8
OWN, FAR, SIB, FAR_SIB = range(4)
MESH = pl.DeviceIdType.MESH
LOWEST = -3.0e38
FLOOR = -2.0e38


def kernel(
    num_chunks,
    scale,
    len_ref,
    q_hbm,
    k_hbm,
    v_hbm,
    out_buf,
    kbuf,
    vbuf,
    qbuf,
    sbuf,
    pbuf,
    ebuf,
    keep,
    give,
    peer,
    stat,
    peer_stat,
    own_out,
    send_out,
    send_lse,
    recv_out,
    recv_lse,
    own_lse,
    k_sem,
    v_sem,
    q_local,
    q_chip_send,
    q_chip_recv,
    q_sib_send,
    q_sib_recv,
    q_fwd_send,
    q_fwd_recv,
    part_send,
    part_recv,
    stat_send,
    stat_recv,
    o_send,
    o_recv,
    l_send,
    l_recv,
):
    me = lax.axis_index("dup")
    chip, core = me // 2, lax.rem(me, 2)
    sib = 2 * chip + (1 - core)
    far = 2 * (1 - chip) + core
    span = kbuf.shape[2]
    pairs = CHUNK // 2
    n = num_chunks

    def load_k(step, slot):
        return pltpu.make_async_copy(k_hbm.at[pl.ds(step * CHUNK, CHUNK)], kbuf.at[slot], k_sem.at[slot])

    def load_v(step, slot):
        return pltpu.make_async_copy(v_hbm.at[pl.ds(step * CHUNK, CHUNK)], vbuf.at[slot], v_sem.at[slot])

    def q_rows(step, role):
        return qbuf.at[role, pl.ds(step * CHUNK * ROWS, CHUNK * ROWS)]

    def q_mine(step):
        return q_rows(step, OWN)

    def remote(src, dst, send, recv, dev):
        return pltpu.make_async_remote_copy(
            src_ref=src, dst_ref=dst, send_sem=send, recv_sem=recv, device_id={"dup": dev}, device_id_type=MESH
        )

    def q_to_far(step):
        return remote(q_mine(step), q_rows(step, FAR), q_chip_send.at[step], q_chip_recv.at[step], far)

    def q_to_sib(step):
        return remote(q_mine(step), q_rows(step, SIB), q_sib_send.at[step], q_sib_recv.at[step], sib)

    def q_forward(step):
        return remote(q_rows(step, FAR), q_rows(step, FAR_SIB), q_fwd_send.at[step], q_fwd_recv.at[step], sib)

    def give_part(step):
        return remote(give.at[step], peer.at[step], part_send.at[step], part_recv.at[step], sib)

    def give_stat(step):
        return remote(stat.at[step], peer_stat.at[step], stat_send.at[step], stat_recv.at[step], sib)

    def give_out(step):
        return remote(send_out.at[step], recv_out.at[step], o_send.at[step], o_recv.at[step], far)

    def give_lse(step):
        return remote(send_lse.at[step], recv_lse.at[step], l_send.at[step], l_recv.at[step], far)

    whole_q = pltpu.make_async_copy(q_hbm, qbuf.at[OWN], q_local.at[0])
    whole_q.start()
    load_k(0, 0).start()

    barrier = pltpu.get_barrier_semaphore()
    for dev in (sib, far):
        pl.semaphore_signal(barrier, inc=1, device_id={"dup": dev}, device_id_type=MESH)
    pl.semaphore_wait(barrier, 2)
    whole_q.wait()
    for step in range(4):
        q_to_far(step).start()

    @pl.loop(0, n)
    def _(step):
        q_to_sib(step).start()

    load_v(0, 0).start()
    for step in range(1, RING):
        load_k(step, step).start()
        load_v(step, step).start()

    def forward_q(step):
        q_to_far(step).wait_recv()
        q_forward(step).start()

    def await_q(step):
        q_to_sib(step).wait_recv()
        q_forward(step).wait_recv()

    lane = lax.broadcasted_iota(jnp.int32, (ROWS, 128), 1)
    draft_of_row = lax.rem(lax.broadcasted_iota(jnp.int32, (ROWS, span), 0), DRAFT)
    reach = lax.broadcasted_iota(jnp.int32, (ROWS, span), 1) - draft_of_row + (me * span + DRAFT)
    rate = scale / math.log(2.0)

    first = lax.rem(lax.broadcasted_iota(jnp.int32, (16, 128), 0), 16) < ROWS
    of_first = jnp.where(first, 1.0, 0.0).astype(jnp.bfloat16)
    of_second = jnp.where(first, 0.0, 1.0).astype(jnp.bfloat16)

    def score_pair(step, slot, i):
        start = pl.multiple_of(step * CHUNK * ROWS, 16) + 16 * i
        q = [qbuf[role, pl.ds(start, 16), :] for role in range(4)]
        left = jnp.concatenate([jnp.concatenate([x * of_first, x * of_second], 1) for x in q], 0)
        right = jnp.concatenate([kbuf[slot, 2 * i], kbuf[slot, 2 * i + 1]], 1)
        return lax.dot_general(left, right, (((1,), (1,)), ((), ())), preferred_element_type=jnp.float32)

    def mask_pair(step, i, scores):
        for h in range(2):
            allowed = reach <= len_ref[step * CHUNK + 2 * i + h]
            for d in range(4):
                row = 16 * d + 8 * h
                s = jnp.where(allowed, scores[row : row + 8], LOWEST)
                sbuf[i, pl.ds(row, 8), :] = s
                peak = jnp.maximum(jnp.max(s, axis=1, keepdims=True), FLOOR)
                pbuf[i, pl.ds(row, 8), :] = jnp.broadcast_to(peak, (ROWS, 128))

    def weigh_pair(i, peaks, masses):
        for d in range(4):
            probs = []
            for h in range(2):
                row = 16 * d + 8 * h
                peak = pbuf[i, pl.ds(row, 8), :]
                s = sbuf[i, pl.ds(row, 8), :]
                p = jnp.exp2((s - jnp.concatenate([peak] * (span // 128), 1)) * rate)
                mass = jnp.sum(p, axis=1, keepdims=True)
                here = lane == (CHUNK * d + 2 * i + h)
                peaks = jnp.where(here, peak, peaks)
                masses = jnp.where(here, mass, masses)
                probs.append(p)
            ebuf[i, pl.ds(16 * d, 16), :] = jnp.concatenate(probs, 0).astype(jnp.bfloat16)
        return peaks, masses

    def sum_pair(step, slot, i):
        v = jnp.concatenate([vbuf[slot, 2 * i], vbuf[slot, 2 * i + 1]], 1)
        o = lax.dot_general(ebuf[i], v, (((1,), (0,)), ((), ())), preferred_element_type=jnp.float32)
        for h in range(2):
            for d in range(4):
                home = keep if d in (OWN, FAR) else give
                home[step, d % 2, 2 * i + h] = o[16 * d + 8 * h : 16 * d + 8 * h + 8, 128 * h : 128 * h + 128]

    def merge_chip(step):
        m_a, l_a = stat[step, 0], stat[step, 1]
        m_b, l_b = (pltpu.roll(peer_stat[step, j], 128 - SIB * CHUNK, 1) for j in range(2))
        top = jnp.maximum(m_a, m_b)
        w_a, w_b = jnp.exp2((m_a - top) * rate), jnp.exp2((m_b - top) * rate)
        total = w_a * l_a + w_b * l_b
        some = total > 0.0
        safe = jnp.where(some, total, 1.0)
        inverse = jnp.where(some, 1.0 / safe, 0.0)
        w_a, w_b = w_a * inverse, w_b * inverse
        lse = jnp.where(some, top * rate + jnp.log2(safe), LOWEST)
        own_lse[step] = lse
        send_lse[step] = pltpu.roll(lse, 128 - FAR * CHUNK, 1)

        def both(role, b):
            c = role * CHUNK + b
            return w_a[:, c : c + 1] * keep[step, role, b] + w_b[:, c : c + 1] * peer[step, role, b]

        for i in range(pairs):
            for b in (2 * i, 2 * i + 1):
                own_out[step, b] = both(OWN, b)
            far_out = [both(FAR, b) for b in (2 * i, 2 * i + 1)]
            send_out[step, pl.ds(16 * i, 16), :] = jnp.concatenate(far_out, 0).astype(jnp.bfloat16)

    def merge_final(step):
        rows = lax.rem(step, n) * CHUNK * ROWS
        mine, theirs = own_lse[step], recv_lse[step]
        top = jnp.maximum(mine, theirs)
        w_a, w_b = jnp.exp2(mine - top), jnp.exp2(theirs - top)
        inverse = 1.0 / (w_a + w_b)
        w_a, w_b = w_a * inverse, w_b * inverse
        for i in range(pairs):
            other = recv_out[step, pl.ds(16 * i, 16), :].astype(jnp.float32)
            outs = []
            for h in range(2):
                b = 2 * i + h
                outs.append(w_a[:, b : b + 1] * own_out[step, b] + w_b[:, b : b + 1] * other[8 * h : 8 * h + 8])
            out_buf[pl.ds(pl.multiple_of(rows + 16 * i, 16), 16), :] = jnp.concatenate(outs, 0).astype(jnp.bfloat16)

    def await_peer(step):
        give_part(step).wait_recv()
        give_stat(step).wait_recv()

    def send_far(step):
        give_out(step).start()
        give_lse(step).start()

    def await_far(step):
        give_out(step).wait_recv()
        give_lse(step).wait_recv()

    def final_stage(step):
        await_far(step)
        merge_final(step)

    def attend(step, with_next):
        slot, next_slot = lax.rem(step, RING), lax.rem(step + 1, RING)
        peaks = jnp.zeros((ROWS, 128), jnp.float32)
        masses = jnp.zeros((ROWS, 128), jnp.float32)
        scores = [None] * pairs
        for i in range(pairs + PV_LAG):
            if i < pairs:
                peaks, masses = weigh_pair(i, peaks, masses)
                if with_next:
                    scores[i] = score_pair(step + 1, next_slot, i)
            if i >= PV_LAG:
                sum_pair(step, slot, i - PV_LAG)
            if with_next and 1 <= i <= pairs:
                mask_pair(step + 1, i - 1, scores[i - 1])
        stat[step, 0] = peaks
        stat[step, 1] = masses

    last = n - 1
    for step in range(AHEAD):
        forward_q(step)
        q_to_far(2 * step + 4).start()
        q_to_far(2 * step + 5).start()
    await_q(0)
    load_k(0, 0).wait()
    for i in range(pairs):
        mask_pair(0, i, score_pair(0, 0, i))
    load_k(RING, 0).start()

    @pl.loop(0, last)
    def _(step):
        @pl.when(2 * step + 2 * AHEAD + 4 < n)
        def _():
            q_to_far(2 * step + 2 * AHEAD + 4).start()
            q_to_far(2 * step + 2 * AHEAD + 5).start()

        @pl.when(step + AHEAD < n)
        def _():
            forward_q(step + AHEAD)

        await_q(step + 1)
        load_k(step + 1, lax.rem(step + 1, RING)).wait()
        load_v(step, lax.rem(step, RING)).wait()

        @pl.when(step >= LAG)
        def _():
            await_peer(step - LAG)

        @pl.when(step >= FINAL_LAG)
        def _():
            await_far(step - FINAL_LAG)

        done = (step + n - FINAL_LAG) // n
        merge_final(done * (step - FINAL_LAG) + (1 - done) * n)
        ready = (step + n - LAG) // n
        merge_chip(ready * (step - LAG) + (1 - ready) * n)
        attend(step, True)
        give_part(step).start()
        give_stat(step).start()

        @pl.when(step >= LAG)
        def _():
            send_far(step - LAG)

        @pl.when(step + 1 + RING < n)
        def _():
            load_k(step + 1 + RING, lax.rem(step + 1, RING)).start()

        @pl.when(step + RING < n)
        def _():
            load_v(step + RING, lax.rem(step, RING)).start()

    load_v(last, lax.rem(last, RING)).wait()
    await_peer(last - LAG)
    await_far(last - FINAL_LAG)
    merge_final(last - FINAL_LAG)
    merge_chip(last - LAG)
    attend(last, False)
    give_part(last).start()
    give_stat(last).start()
    send_far(last - LAG)

    @pl.loop(last - LAG + 1, last)
    def _(step):
        await_peer(step)
        merge_chip(step)
        send_far(step)

    @pl.loop(last - FINAL_LAG + 1, last - FINAL_LAG + 1 + EARLY_FINALS)
    def _(step):
        final_stage(step)

    await_peer(last)
    merge_chip(last)
    send_far(last)

    @pl.loop(last - FINAL_LAG + 1 + EARLY_FINALS, n)
    def _(step):
        final_stage(step)

    @pl.loop(0, n)
    def _(step):
        q_to_far(step).wait_send()
        q_to_sib(step).wait_send()
        q_forward(step).wait_send()
        give_part(step).wait_send()
        give_stat(step).wait_send()
        give_out(step).wait_send()
        give_lse(step).wait_send()


def solution(mesh):
    def group_step(q_local, k_span, v_span, len_local):
        num_batch, span, dim = k_span.shape
        n = num_batch // CHUNK
        f32, bf16 = jnp.float32, jnp.bfloat16
        dma = lambda *shape: pltpu.SemaphoreType.DMA(shape)
        hbm = pl.BlockSpec(memory_space=pltpu.HBM)
        out = pl.pallas_call(
            functools.partial(kernel, n, dim**-0.5),
            out_shape=pltpu.VMEM((num_batch * ROWS, dim), bf16),
            in_specs=[pl.BlockSpec(memory_space=pltpu.SMEM), hbm, hbm, hbm],
            out_specs=pl.BlockSpec(memory_space=pltpu.VMEM),
            scratch_shapes=[
                pltpu.VMEM((RING, CHUNK, span, dim), bf16),
                pltpu.VMEM((RING, CHUNK, span, dim), bf16),
                pltpu.VMEM((4, num_batch * ROWS, dim), bf16),
                pltpu.VMEM((CHUNK // 2, 64, span), f32),
                pltpu.VMEM((CHUNK // 2, 64, 128), f32),
                pltpu.VMEM((CHUNK // 2, 64, span), bf16),
                pltpu.VMEM((n + 1, 2, CHUNK, ROWS, dim), f32),
                pltpu.VMEM((n, 2, CHUNK, ROWS, dim), f32),
                pltpu.VMEM((n + 1, 2, CHUNK, ROWS, dim), f32),
                pltpu.VMEM((n + 1, 2, ROWS, dim), f32),
                pltpu.VMEM((n + 1, 2, ROWS, dim), f32),
                pltpu.VMEM((n + 1, CHUNK, ROWS, dim), f32),
                pltpu.VMEM((n + 1, CHUNK * ROWS, dim), bf16),
                pltpu.VMEM((n + 1, ROWS, dim), f32),
                pltpu.VMEM((n + 1, CHUNK * ROWS, dim), bf16),
                pltpu.VMEM((n + 1, ROWS, dim), f32),
                pltpu.VMEM((n + 1, ROWS, dim), f32),
                dma(RING),
                dma(RING),
                dma(1),
            ]
            + [dma(n)] * 14,
            compiler_params=pltpu.CompilerParams(
                collective_id=0, has_side_effects=True, vmem_limit_bytes=56 * 1024 * 1024
            ),
        )(len_local, q_local.reshape(num_batch * ROWS, dim), k_span, v_span)
        return out.reshape(num_batch, ROWS, dim)

    return jax.shard_map(
        group_step,
        mesh=mesh,
        in_specs=(P("kv", "dup", None), P("kv", "dup", None), P("kv", "dup", None), P("kv")),
        out_specs=P("kv", "dup", None),
        check_vma=False,
    )
```

```python
import functools
import math

import jax
import jax.numpy as jnp
from jax import lax
from jax.experimental import pallas as pl
from jax.experimental.pallas import tpu as pltpu
from jax.sharding import PartitionSpec as P

DRAFT = 4
CHUNK = 16
RING = 6
AHEAD = 2
LAG = 2
FINAL_LAG = 8
EARLY_FINALS = 4
PV_LAG = 2
ROWS = 8
OWN, FAR, SIB, FAR_SIB = range(4)
MESH = pl.DeviceIdType.MESH
LOWEST = -3.0e38
FLOOR = -2.0e38


def kernel(
    num_chunks,
    scale,
    len_ref,
    q_hbm,
    k_hbm,
    v_hbm,
    out_buf,
    kbuf,
    vbuf,
    qbuf,
    sbuf,
    pbuf,
    ebuf,
    keep,
    give,
    peer,
    stat,
    peer_stat,
    own_out,
    send_out,
    send_lse,
    recv_out,
    recv_lse,
    own_lse,
    k_sem,
    v_sem,
    q_local,
    q_chip_send,
    q_chip_recv,
    q_sib_send,
    q_sib_recv,
    q_fwd_send,
    q_fwd_recv,
    part_send,
    part_recv,
    stat_send,
    stat_recv,
    o_send,
    o_recv,
    l_send,
    l_recv,
):
    me = lax.axis_index("dup")
    chip, core = me // 2, lax.rem(me, 2)
    sib = 2 * chip + (1 - core)
    far = 2 * (1 - chip) + core
    span = kbuf.shape[2]
    pairs = CHUNK // 2
    n = num_chunks

    def load_k(step, slot):
        return pltpu.make_async_copy(k_hbm.at[pl.ds(step * CHUNK, CHUNK)], kbuf.at[slot], k_sem.at[slot])

    def load_v(step, slot):
        return pltpu.make_async_copy(v_hbm.at[pl.ds(step * CHUNK, CHUNK)], vbuf.at[slot], v_sem.at[slot])

    def q_rows(step, role):
        return qbuf.at[role, pl.ds(step * CHUNK * ROWS, CHUNK * ROWS)]

    def q_mine(step):
        return q_rows(step, OWN)

    def remote(src, dst, send, recv, dev):
        return pltpu.make_async_remote_copy(
            src_ref=src, dst_ref=dst, send_sem=send, recv_sem=recv, device_id={"dup": dev}, device_id_type=MESH
        )

    def q_to_far(step):
        return remote(q_mine(step), q_rows(step, FAR), q_chip_send.at[step], q_chip_recv.at[step], far)

    def q_to_sib(step):
        return remote(q_mine(step), q_rows(step, SIB), q_sib_send.at[step], q_sib_recv.at[step], sib)

    def q_forward(step):
        return remote(q_rows(step, FAR), q_rows(step, FAR_SIB), q_fwd_send.at[step], q_fwd_recv.at[step], sib)

    def give_part(step):
        return remote(give.at[step], peer.at[step], part_send.at[step], part_recv.at[step], sib)

    def give_stat(step):
        return remote(stat.at[step], peer_stat.at[step], stat_send.at[step], stat_recv.at[step], sib)

    def give_out(step):
        return remote(send_out.at[step], recv_out.at[step], o_send.at[step], o_recv.at[step], far)

    def give_lse(step):
        return remote(send_lse.at[step], recv_lse.at[step], l_send.at[step], l_recv.at[step], far)

    whole_q = pltpu.make_async_copy(q_hbm, qbuf.at[OWN], q_local.at[0])
    whole_q.start()
    for step in range(2):
        load_k(step, step).start()
        load_v(step, step).start()

    barrier = pltpu.get_barrier_semaphore()
    for dev in (sib, far):
        pl.semaphore_signal(barrier, inc=1, device_id={"dup": dev}, device_id_type=MESH)
    pl.semaphore_wait(barrier, 2)
    whole_q.wait()
    for step in range(4):
        q_to_far(step).start()

    @pl.loop(0, n)
    def _(step):
        q_to_sib(step).start()

    for step in range(2, RING):
        load_k(step, step).start()
        load_v(step, step).start()

    def forward_q(step):
        q_to_far(step).wait_recv()
        q_forward(step).start()

    def await_q(step):
        q_to_sib(step).wait_recv()
        q_forward(step).wait_recv()

    lane = lax.broadcasted_iota(jnp.int32, (ROWS, 128), 1)
    draft_of_row = lax.rem(lax.broadcasted_iota(jnp.int32, (ROWS, span), 0), DRAFT)
    reach = lax.broadcasted_iota(jnp.int32, (ROWS, span), 1) - draft_of_row + (me * span + DRAFT)
    rate = scale / math.log(2.0)

    first = lax.rem(lax.broadcasted_iota(jnp.int32, (16, 128), 0), 16) < ROWS
    of_first = jnp.where(first, 1.0, 0.0).astype(jnp.bfloat16)
    of_second = jnp.where(first, 0.0, 1.0).astype(jnp.bfloat16)

    def score_pair(step, slot, i):
        start = pl.multiple_of(step * CHUNK * ROWS, 16) + 16 * i
        q = [qbuf[role, pl.ds(start, 16), :] for role in range(4)]
        left = jnp.concatenate([jnp.concatenate([x * of_first, x * of_second], 1) for x in q], 0)
        k_a, k_b = kbuf[slot, 2 * i], kbuf[slot, 2 * i + 1]
        turned = span // 2
        right = jnp.concatenate([k_a[:turned], k_b[:turned]], 1)
        scores = lax.dot_general(left, right, (((1,), (1,)), ((), ())), preferred_element_type=jnp.float32)
        rest = jnp.concatenate([k_a[turned:].T, k_b[turned:].T], 0)
        more = lax.dot_general(left, rest, (((1,), (0,)), ((), ())), preferred_element_type=jnp.float32)
        return jnp.concatenate([scores, more], 1)

    def mask_pair(step, i, scores):
        for h in range(2):
            allowed = reach <= len_ref[step * CHUNK + 2 * i + h]
            for d in range(4):
                row = 16 * d + 8 * h
                s = jnp.where(allowed, scores[row : row + 8], LOWEST)
                sbuf[i, pl.ds(row, 8), :] = s
                peak = jnp.maximum(jnp.max(s, axis=1, keepdims=True), FLOOR)
                pbuf[i, pl.ds(row, 8), :] = jnp.broadcast_to(peak, (ROWS, 128))

    def weigh_pair(i, peaks, masses):
        for d in range(4):
            probs = []
            for h in range(2):
                row = 16 * d + 8 * h
                peak = pbuf[i, pl.ds(row, 8), :]
                s = sbuf[i, pl.ds(row, 8), :]
                p = jnp.exp2((s - jnp.concatenate([peak] * (span // 128), 1)) * rate)
                mass = jnp.sum(p, axis=1, keepdims=True)
                here = lane == (CHUNK * d + 2 * i + h)
                peaks = jnp.where(here, peak, peaks)
                masses = jnp.where(here, mass, masses)
                probs.append(p)
            ebuf[i, pl.ds(16 * d, 16), :] = jnp.concatenate(probs, 0).astype(jnp.bfloat16)
        return peaks, masses

    def sum_pair(step, slot, i):
        v = jnp.concatenate([vbuf[slot, 2 * i], vbuf[slot, 2 * i + 1]], 1)
        o = lax.dot_general(ebuf[i], v, (((1,), (0,)), ((), ())), preferred_element_type=jnp.float32)
        for h in range(2):
            for d in range(4):
                home = keep if d in (OWN, FAR) else give
                home[step, d % 2, 2 * i + h] = o[16 * d + 8 * h : 16 * d + 8 * h + 8, 128 * h : 128 * h + 128]

    def merge_chip(step):
        m_a, l_a = stat[step, 0], stat[step, 1]
        m_b, l_b = (pltpu.roll(peer_stat[step, j], 128 - SIB * CHUNK, 1) for j in range(2))
        top = jnp.maximum(m_a, m_b)
        w_a, w_b = jnp.exp2((m_a - top) * rate), jnp.exp2((m_b - top) * rate)
        total = w_a * l_a + w_b * l_b
        some = total > 0.0
        safe = jnp.where(some, total, 1.0)
        inverse = jnp.where(some, 1.0 / safe, 0.0)
        w_a, w_b = w_a * inverse, w_b * inverse
        lse = jnp.where(some, top * rate + jnp.log2(safe), LOWEST)
        own_lse[step] = lse
        send_lse[step] = pltpu.roll(lse, 128 - FAR * CHUNK, 1)

        def both(role, b):
            c = role * CHUNK + b
            return w_a[:, c : c + 1] * keep[step, role, b] + w_b[:, c : c + 1] * peer[step, role, b]

        for i in range(pairs):
            for b in (2 * i, 2 * i + 1):
                own_out[step, b] = both(OWN, b)
            far_out = [both(FAR, b) for b in (2 * i, 2 * i + 1)]
            send_out[step, pl.ds(16 * i, 16), :] = jnp.concatenate(far_out, 0).astype(jnp.bfloat16)

    def merge_final(step):
        rows = lax.rem(step, n) * CHUNK * ROWS
        mine, theirs = own_lse[step], recv_lse[step]
        top = jnp.maximum(mine, theirs)
        w_a, w_b = jnp.exp2(mine - top), jnp.exp2(theirs - top)
        inverse = 1.0 / (w_a + w_b)
        w_a, w_b = w_a * inverse, w_b * inverse
        for i in range(pairs):
            other = recv_out[step, pl.ds(16 * i, 16), :].astype(jnp.float32)
            outs = []
            for h in range(2):
                b = 2 * i + h
                outs.append(w_a[:, b : b + 1] * own_out[step, b] + w_b[:, b : b + 1] * other[8 * h : 8 * h + 8])
            out_buf[pl.ds(pl.multiple_of(rows + 16 * i, 16), 16), :] = jnp.concatenate(outs, 0).astype(jnp.bfloat16)

    def await_peer(step):
        give_part(step).wait_recv()
        give_stat(step).wait_recv()

    def send_far(step):
        give_out(step).start()
        give_lse(step).start()

    def await_far(step):
        give_out(step).wait_recv()
        give_lse(step).wait_recv()

    def final_stage(step):
        await_far(step)
        merge_final(step)

    def attend(step, with_next):
        slot, next_slot = lax.rem(step, RING), lax.rem(step + 1, RING)
        peaks = jnp.zeros((ROWS, 128), jnp.float32)
        masses = jnp.zeros((ROWS, 128), jnp.float32)
        scores = [None] * pairs
        for i in range(pairs + PV_LAG):
            if i < pairs:
                peaks, masses = weigh_pair(i, peaks, masses)
                if with_next:
                    scores[i] = score_pair(step + 1, next_slot, i)
            if i >= PV_LAG:
                sum_pair(step, slot, i - PV_LAG)
            if with_next and 1 <= i <= pairs:
                mask_pair(step + 1, i - 1, scores[i - 1])
        stat[step, 0] = peaks
        stat[step, 1] = masses

    last = n - 1
    for step in range(AHEAD):
        forward_q(step)
        q_to_far(2 * step + 4).start()
        q_to_far(2 * step + 5).start()
    await_q(0)
    load_k(0, 0).wait()
    for i in range(pairs):
        mask_pair(0, i, score_pair(0, 0, i))
    load_k(RING, 0).start()

    @pl.loop(0, last)
    def _(step):
        @pl.when(2 * step + 2 * AHEAD + 4 < n)
        def _():
            q_to_far(2 * step + 2 * AHEAD + 4).start()
            q_to_far(2 * step + 2 * AHEAD + 5).start()

        @pl.when(step + AHEAD < n)
        def _():
            forward_q(step + AHEAD)

        await_q(step + 1)
        load_k(step + 1, lax.rem(step + 1, RING)).wait()
        load_v(step, lax.rem(step, RING)).wait()

        @pl.when(step >= LAG)
        def _():
            await_peer(step - LAG)

        @pl.when(step >= FINAL_LAG)
        def _():
            await_far(step - FINAL_LAG)

        done = (step + n - FINAL_LAG) // n
        merge_final(done * (step - FINAL_LAG) + (1 - done) * n)
        ready = (step + n - LAG) // n
        merge_chip(ready * (step - LAG) + (1 - ready) * n)
        attend(step, True)
        give_part(step).start()
        give_stat(step).start()

        @pl.when(step >= LAG)
        def _():
            send_far(step - LAG)

        @pl.when(step + 1 + RING < n)
        def _():
            load_k(step + 1 + RING, lax.rem(step + 1, RING)).start()

        @pl.when(step + RING < n)
        def _():
            load_v(step + RING, lax.rem(step, RING)).start()

    load_v(last, lax.rem(last, RING)).wait()
    await_peer(last - LAG)
    await_far(last - FINAL_LAG)
    merge_final(last - FINAL_LAG)
    merge_chip(last - LAG)
    attend(last, False)
    give_part(last).start()
    give_stat(last).start()
    send_far(last - LAG)

    @pl.loop(last - LAG + 1, last)
    def _(step):
        await_peer(step)
        merge_chip(step)
        send_far(step)

    @pl.loop(last - FINAL_LAG + 1, last - FINAL_LAG + 1 + EARLY_FINALS)
    def _(step):
        final_stage(step)

    await_peer(last)
    merge_chip(last)
    send_far(last)

    @pl.loop(last - FINAL_LAG + 1 + EARLY_FINALS, n)
    def _(step):
        final_stage(step)

    @pl.loop(0, n)
    def _(step):
        q_to_far(step).wait_send()
        q_to_sib(step).wait_send()
        q_forward(step).wait_send()
        give_part(step).wait_send()
        give_stat(step).wait_send()
        give_out(step).wait_send()
        give_lse(step).wait_send()


def solution(mesh):
    def group_step(q_local, k_span, v_span, len_local):
        num_batch, span, dim = k_span.shape
        n = num_batch // CHUNK
        f32, bf16 = jnp.float32, jnp.bfloat16
        dma = lambda *shape: pltpu.SemaphoreType.DMA(shape)
        hbm = pl.BlockSpec(memory_space=pltpu.HBM)
        out = pl.pallas_call(
            functools.partial(kernel, n, dim**-0.5),
            out_shape=pltpu.VMEM((num_batch * ROWS, dim), bf16),
            in_specs=[pl.BlockSpec(memory_space=pltpu.SMEM), hbm, hbm, hbm],
            out_specs=pl.BlockSpec(memory_space=pltpu.VMEM),
            scratch_shapes=[
                pltpu.VMEM((RING, CHUNK, span, dim), bf16),
                pltpu.VMEM((RING, CHUNK, span, dim), bf16),
                pltpu.VMEM((4, num_batch * ROWS, dim), bf16),
                pltpu.VMEM((CHUNK // 2, 64, span), f32),
                pltpu.VMEM((CHUNK // 2, 64, 128), f32),
                pltpu.VMEM((CHUNK // 2, 64, span), bf16),
                pltpu.VMEM((n + 1, 2, CHUNK, ROWS, dim), f32),
                pltpu.VMEM((n, 2, CHUNK, ROWS, dim), f32),
                pltpu.VMEM((n + 1, 2, CHUNK, ROWS, dim), f32),
                pltpu.VMEM((n + 1, 2, ROWS, dim), f32),
                pltpu.VMEM((n + 1, 2, ROWS, dim), f32),
                pltpu.VMEM((n + 1, CHUNK, ROWS, dim), f32),
                pltpu.VMEM((n + 1, CHUNK * ROWS, dim), bf16),
                pltpu.VMEM((n + 1, ROWS, dim), f32),
                pltpu.VMEM((n + 1, CHUNK * ROWS, dim), bf16),
                pltpu.VMEM((n + 1, ROWS, dim), f32),
                pltpu.VMEM((n + 1, ROWS, dim), f32),
                dma(RING),
                dma(RING),
                dma(1),
            ]
            + [dma(n)] * 14,
            compiler_params=pltpu.CompilerParams(
                collective_id=0, has_side_effects=True, vmem_limit_bytes=56 * 1024 * 1024
            ),
        )(len_local, q_local.reshape(num_batch * ROWS, dim), k_span, v_span)
        return out.reshape(num_batch, ROWS, dim)

    return jax.shard_map(
        group_step,
        mesh=mesh,
        in_specs=(P("kv", "dup", None), P("kv", "dup", None), P("kv", "dup", None), P("kv")),
        out_specs=P("kv", "dup", None),
        check_vma=False,
    )
```

```python
import functools
import math

import jax
import jax.numpy as jnp
from jax import lax
from jax.experimental import pallas as pl
from jax.experimental.pallas import tpu as pltpu
from jax.sharding import PartitionSpec as P

DRAFT = 4
CHUNK = 16
RING = 6
AHEAD = 4
LAG = 3
FINAL_LAG = 8
EARLY_FINALS = 4
PV_LAG = 2
ROWS = 8
OWN, FAR, SIB, FAR_SIB = range(4)
MESH = pl.DeviceIdType.MESH
LOWEST = -3.0e38
FLOOR = -2.0e38


def kernel(
    num_chunks,
    scale,
    len_ref,
    q_hbm,
    k_hbm,
    v_hbm,
    out_buf,
    kbuf,
    vbuf,
    qbuf,
    sbuf,
    pbuf,
    ebuf,
    keep,
    give,
    peer,
    stat,
    peer_stat,
    own_out,
    send_out,
    send_lse,
    recv_out,
    recv_lse,
    own_lse,
    k_sem,
    v_sem,
    q_local,
    q_chip_send,
    q_chip_recv,
    q_sib_send,
    q_sib_recv,
    q_fwd_send,
    q_fwd_recv,
    part_send,
    part_recv,
    stat_send,
    stat_recv,
    o_send,
    o_recv,
    l_send,
    l_recv,
):
    me = lax.axis_index("dup")
    chip, core = me // 2, lax.rem(me, 2)
    sib = 2 * chip + (1 - core)
    far = 2 * (1 - chip) + core
    span = kbuf.shape[2]
    pairs = CHUNK // 2
    n = num_chunks

    def load_k(step, slot):
        return pltpu.make_async_copy(k_hbm.at[pl.ds(step * CHUNK, CHUNK)], kbuf.at[slot], k_sem.at[slot])

    def load_v(step, slot):
        return pltpu.make_async_copy(v_hbm.at[pl.ds(step * CHUNK, CHUNK)], vbuf.at[slot], v_sem.at[slot])

    def q_rows(step, role):
        return qbuf.at[role, pl.ds(step * CHUNK * ROWS, CHUNK * ROWS)]

    def q_mine(step):
        return q_rows(step, OWN)

    def remote(src, dst, send, recv, dev):
        return pltpu.make_async_remote_copy(
            src_ref=src, dst_ref=dst, send_sem=send, recv_sem=recv, device_id={"dup": dev}, device_id_type=MESH
        )

    def q_to_far(step):
        return remote(q_mine(step), q_rows(step, FAR), q_chip_send.at[step], q_chip_recv.at[step], far)

    def q_to_sib(step):
        return remote(q_mine(step), q_rows(step, SIB), q_sib_send.at[step], q_sib_recv.at[step], sib)

    def q_forward(step):
        return remote(q_rows(step, FAR), q_rows(step, FAR_SIB), q_fwd_send.at[step], q_fwd_recv.at[step], sib)

    def give_part(step):
        return remote(give.at[step], peer.at[step], part_send.at[step], part_recv.at[step], sib)

    def give_stat(step):
        return remote(stat.at[step], peer_stat.at[step], stat_send.at[step], stat_recv.at[step], sib)

    def give_out(step):
        return remote(send_out.at[step], recv_out.at[step], o_send.at[step], o_recv.at[step], far)

    def give_lse(step):
        return remote(send_lse.at[step], recv_lse.at[step], l_send.at[step], l_recv.at[step], far)

    whole_q = pltpu.make_async_copy(q_hbm, qbuf.at[OWN], q_local.at[0])
    whole_q.start()
    for step in range(2):
        load_k(step, step).start()
        load_v(step, step).start()

    barrier = pltpu.get_barrier_semaphore()
    for dev in (sib, far):
        pl.semaphore_signal(barrier, inc=1, device_id={"dup": dev}, device_id_type=MESH)
    pl.semaphore_wait(barrier, 2)
    whole_q.wait()
    for step in range(4):
        q_to_far(step).start()

    @pl.loop(0, n)
    def _(step):
        q_to_sib(step).start()

    for step in range(2, RING):
        load_k(step, step).start()
        load_v(step, step).start()

    def forward_q(step):
        q_to_far(step).wait_recv()
        q_forward(step).start()

    def await_q(step):
        q_to_sib(step).wait_recv()
        q_forward(step).wait_recv()

    lane = lax.broadcasted_iota(jnp.int32, (ROWS, 128), 1)
    draft_of_row = lax.rem(lax.broadcasted_iota(jnp.int32, (ROWS, span), 0), DRAFT)
    reach = lax.broadcasted_iota(jnp.int32, (ROWS, span), 1) - draft_of_row + (me * span + DRAFT)
    rate = scale / math.log(2.0)

    first = lax.rem(lax.broadcasted_iota(jnp.int32, (16, 128), 0), 16) < ROWS
    of_first = jnp.where(first, 1.0, 0.0).astype(jnp.bfloat16)
    of_second = jnp.where(first, 0.0, 1.0).astype(jnp.bfloat16)

    def score_pair(step, slot, i):
        start = pl.multiple_of(step * CHUNK * ROWS, 16) + 16 * i
        q = [qbuf[role, pl.ds(start, 16), :] for role in range(4)]
        left = jnp.concatenate([jnp.concatenate([x * of_first, x * of_second], 1) for x in q], 0)
        k_a, k_b = kbuf[slot, 2 * i], kbuf[slot, 2 * i + 1]
        turned = span // 2
        right = jnp.concatenate([k_a[:turned], k_b[:turned]], 1)
        scores = lax.dot_general(left, right, (((1,), (1,)), ((), ())), preferred_element_type=jnp.float32)
        rest = jnp.concatenate([k_a[turned:].T, k_b[turned:].T], 0)
        more = lax.dot_general(left, rest, (((1,), (0,)), ((), ())), preferred_element_type=jnp.float32)
        return jnp.concatenate([scores, more], 1)

    def mask_pair(step, i, scores):
        for h in range(2):
            allowed = reach <= len_ref[step * CHUNK + 2 * i + h]
            for d in range(4):
                row = 16 * d + 8 * h
                s = jnp.where(allowed, scores[row : row + 8], LOWEST)
                sbuf[i, pl.ds(row, 8), :] = s
                peak = jnp.maximum(jnp.max(s, axis=1, keepdims=True), FLOOR)
                pbuf[i, pl.ds(row, 8), :] = jnp.broadcast_to(peak, (ROWS, 128))

    def weigh_pair(i, peaks, masses):
        for d in range(4):
            probs = []
            for h in range(2):
                row = 16 * d + 8 * h
                peak = pbuf[i, pl.ds(row, 8), :]
                s = sbuf[i, pl.ds(row, 8), :]
                p = jnp.exp2((s - jnp.concatenate([peak] * (span // 128), 1)) * rate)
                mass = jnp.sum(p, axis=1, keepdims=True)
                here = lane == (CHUNK * d + 2 * i + h)
                peaks = jnp.where(here, peak, peaks)
                masses = jnp.where(here, mass, masses)
                probs.append(p)
            ebuf[i, pl.ds(16 * d, 16), :] = jnp.concatenate(probs, 0).astype(jnp.bfloat16)
        return peaks, masses

    def sum_pair(step, slot, i):
        v = jnp.concatenate([vbuf[slot, 2 * i], vbuf[slot, 2 * i + 1]], 1)
        o = lax.dot_general(ebuf[i], v, (((1,), (0,)), ((), ())), preferred_element_type=jnp.float32)
        for h in range(2):
            for d in range(4):
                home = keep if d in (OWN, FAR) else give
                home[step, d % 2, 2 * i + h] = o[16 * d + 8 * h : 16 * d + 8 * h + 8, 128 * h : 128 * h + 128]

    def merge_chip(step):
        m_a, l_a = stat[step, 0], stat[step, 1]
        m_b, l_b = (pltpu.roll(peer_stat[step, j], 128 - SIB * CHUNK, 1) for j in range(2))
        top = jnp.maximum(m_a, m_b)
        w_a, w_b = jnp.exp2((m_a - top) * rate), jnp.exp2((m_b - top) * rate)
        total = w_a * l_a + w_b * l_b
        some = total > 0.0
        safe = jnp.where(some, total, 1.0)
        inverse = jnp.where(some, 1.0 / safe, 0.0)
        w_a, w_b = w_a * inverse, w_b * inverse
        lse = jnp.where(some, top * rate + jnp.log2(safe), LOWEST)
        own_lse[step] = lse
        send_lse[step] = pltpu.roll(lse, 128 - FAR * CHUNK, 1)

        def both(role, b):
            c = role * CHUNK + b
            return w_a[:, c : c + 1] * keep[step, role, b] + w_b[:, c : c + 1] * peer[step, role, b]

        for i in range(pairs):
            for b in (2 * i, 2 * i + 1):
                own_out[step, b] = both(OWN, b)
            far_out = [both(FAR, b) for b in (2 * i, 2 * i + 1)]
            send_out[step, pl.ds(16 * i, 16), :] = jnp.concatenate(far_out, 0).astype(jnp.bfloat16)

    def merge_final(step):
        rows = lax.rem(step, n) * CHUNK * ROWS
        mine, theirs = own_lse[step], recv_lse[step]
        top = jnp.maximum(mine, theirs)
        w_a, w_b = jnp.exp2(mine - top), jnp.exp2(theirs - top)
        inverse = 1.0 / (w_a + w_b)
        w_a, w_b = w_a * inverse, w_b * inverse
        for i in range(pairs):
            other = recv_out[step, pl.ds(16 * i, 16), :].astype(jnp.float32)
            outs = []
            for h in range(2):
                b = 2 * i + h
                outs.append(w_a[:, b : b + 1] * own_out[step, b] + w_b[:, b : b + 1] * other[8 * h : 8 * h + 8])
            out_buf[pl.ds(pl.multiple_of(rows + 16 * i, 16), 16), :] = jnp.concatenate(outs, 0).astype(jnp.bfloat16)

    def await_peer(step):
        give_part(step).wait_recv()
        give_stat(step).wait_recv()

    def send_far(step):
        give_out(step).start()
        give_lse(step).start()

    def await_far(step):
        give_out(step).wait_recv()
        give_lse(step).wait_recv()

    def final_stage(step):
        await_far(step)
        merge_final(step)

    def attend(step, with_next):
        slot, next_slot = lax.rem(step, RING), lax.rem(step + 1, RING)
        peaks = jnp.zeros((ROWS, 128), jnp.float32)
        masses = jnp.zeros((ROWS, 128), jnp.float32)
        scores = [None] * pairs
        for i in range(pairs + PV_LAG):
            if i < pairs:
                peaks, masses = weigh_pair(i, peaks, masses)
                if with_next:
                    scores[i] = score_pair(step + 1, next_slot, i)
            if i >= PV_LAG:
                sum_pair(step, slot, i - PV_LAG)
            if with_next and 1 <= i <= pairs:
                mask_pair(step + 1, i - 1, scores[i - 1])
        stat[step, 0] = peaks
        stat[step, 1] = masses

    last = n - 1
    for step in range(AHEAD):
        forward_q(step)
        q_to_far(2 * step + 4).start()
        q_to_far(2 * step + 5).start()
    await_q(0)
    load_k(0, 0).wait()
    for i in range(pairs):
        mask_pair(0, i, score_pair(0, 0, i))
    load_k(RING, 0).start()

    @pl.loop(0, last)
    def _(step):
        @pl.when(2 * step + 2 * AHEAD + 4 < n)
        def _():
            q_to_far(2 * step + 2 * AHEAD + 4).start()
            q_to_far(2 * step + 2 * AHEAD + 5).start()

        @pl.when(step + AHEAD < n)
        def _():
            forward_q(step + AHEAD)

        await_q(step + 1)
        load_k(step + 1, lax.rem(step + 1, RING)).wait()
        load_v(step, lax.rem(step, RING)).wait()

        @pl.when(step >= LAG)
        def _():
            await_peer(step - LAG)

        @pl.when(step >= FINAL_LAG)
        def _():
            await_far(step - FINAL_LAG)

        done = (step + n - FINAL_LAG) // n
        merge_final(done * (step - FINAL_LAG) + (1 - done) * n)
        ready = (step + n - LAG) // n
        merge_chip(ready * (step - LAG) + (1 - ready) * n)
        attend(step, True)
        give_part(step).start()
        give_stat(step).start()

        @pl.when(step >= LAG)
        def _():
            send_far(step - LAG)

        @pl.when(step + 1 + RING < n)
        def _():
            load_k(step + 1 + RING, lax.rem(step + 1, RING)).start()

        @pl.when(step + RING < n)
        def _():
            load_v(step + RING, lax.rem(step, RING)).start()

    load_v(last, lax.rem(last, RING)).wait()
    await_peer(last - LAG)
    await_far(last - FINAL_LAG)
    merge_final(last - FINAL_LAG)
    merge_chip(last - LAG)
    attend(last, False)
    give_part(last).start()
    give_stat(last).start()
    send_far(last - LAG)

    @pl.loop(last - LAG + 1, last)
    def _(step):
        await_peer(step)
        merge_chip(step)
        send_far(step)

    @pl.loop(last - FINAL_LAG + 1, last - FINAL_LAG + 1 + EARLY_FINALS)
    def _(step):
        final_stage(step)

    await_peer(last)
    merge_chip(last)
    send_far(last)

    @pl.loop(last - FINAL_LAG + 1 + EARLY_FINALS, n)
    def _(step):
        final_stage(step)

    @pl.loop(0, n)
    def _(step):
        q_to_far(step).wait_send()
        q_to_sib(step).wait_send()
        q_forward(step).wait_send()
        give_part(step).wait_send()
        give_stat(step).wait_send()
        give_out(step).wait_send()
        give_lse(step).wait_send()


def solution(mesh):
    def group_step(q_local, k_span, v_span, len_local):
        num_batch, span, dim = k_span.shape
        n = num_batch // CHUNK
        f32, bf16 = jnp.float32, jnp.bfloat16
        dma = lambda *shape: pltpu.SemaphoreType.DMA(shape)
        hbm = pl.BlockSpec(memory_space=pltpu.HBM)
        out = pl.pallas_call(
            functools.partial(kernel, n, dim**-0.5),
            out_shape=pltpu.VMEM((num_batch * ROWS, dim), bf16),
            in_specs=[pl.BlockSpec(memory_space=pltpu.SMEM), hbm, hbm, hbm],
            out_specs=pl.BlockSpec(memory_space=pltpu.VMEM),
            scratch_shapes=[
                pltpu.VMEM((RING, CHUNK, span, dim), bf16),
                pltpu.VMEM((RING, CHUNK, span, dim), bf16),
                pltpu.VMEM((4, num_batch * ROWS, dim), bf16),
                pltpu.VMEM((CHUNK // 2, 64, span), f32),
                pltpu.VMEM((CHUNK // 2, 64, 128), f32),
                pltpu.VMEM((CHUNK // 2, 64, span), bf16),
                pltpu.VMEM((n + 1, 2, CHUNK, ROWS, dim), f32),
                pltpu.VMEM((n, 2, CHUNK, ROWS, dim), f32),
                pltpu.VMEM((n + 1, 2, CHUNK, ROWS, dim), f32),
                pltpu.VMEM((n + 1, 2, ROWS, dim), f32),
                pltpu.VMEM((n + 1, 2, ROWS, dim), f32),
                pltpu.VMEM((n + 1, CHUNK, ROWS, dim), f32),
                pltpu.VMEM((n + 1, CHUNK * ROWS, dim), bf16),
                pltpu.VMEM((n + 1, ROWS, dim), f32),
                pltpu.VMEM((n + 1, CHUNK * ROWS, dim), bf16),
                pltpu.VMEM((n + 1, ROWS, dim), f32),
                pltpu.VMEM((n + 1, ROWS, dim), f32),
                dma(RING),
                dma(RING),
                dma(1),
            ]
            + [dma(n)] * 14,
            compiler_params=pltpu.CompilerParams(
                collective_id=0, has_side_effects=True, vmem_limit_bytes=56 * 1024 * 1024
            ),
        )(len_local, q_local.reshape(num_batch * ROWS, dim), k_span, v_span)
        return out.reshape(num_batch, ROWS, dim)

    return jax.shard_map(
        group_step,
        mesh=mesh,
        in_specs=(P("kv", "dup", None), P("kv", "dup", None), P("kv", "dup", None), P("kv")),
        out_specs=P("kv", "dup", None),
        check_vma=False,
    )
```

```python
import functools
import math

import jax
import jax.numpy as jnp
from jax import lax
from jax.experimental import pallas as pl
from jax.experimental.pallas import tpu as pltpu
from jax.sharding import PartitionSpec as P

DRAFT = 4
CHUNK = 16
RING = 6
AHEAD = 2
LAG = 2
FINAL_LAG = 8
EARLY_FINALS = 4
PV_LAG = 2
ROWS = 8
OWN, FAR, SIB, FAR_SIB = range(4)
MESH = pl.DeviceIdType.MESH
LOWEST = -3.0e38
FLOOR = -2.0e38


def kernel(
    num_chunks,
    scale,
    len_ref,
    q_hbm,
    k_hbm,
    v_hbm,
    out_buf,
    kbuf,
    vbuf,
    qbuf,
    sbuf,
    pbuf,
    ebuf,
    keep,
    give,
    peer,
    stat,
    peer_stat,
    own_out,
    send_out,
    send_lse,
    recv_out,
    recv_lse,
    own_lse,
    k_sem,
    v_sem,
    q_local,
    q_chip_send,
    q_chip_recv,
    q_sib_send,
    q_sib_recv,
    q_fwd_send,
    q_fwd_recv,
    part_send,
    part_recv,
    stat_send,
    stat_recv,
    o_send,
    o_recv,
    l_send,
    l_recv,
):
    me = lax.axis_index("dup")
    chip, core = me // 2, lax.rem(me, 2)
    sib = 2 * chip + (1 - core)
    far = 2 * (1 - chip) + core
    span = kbuf.shape[2]
    pairs = CHUNK // 2
    n = num_chunks

    def load_k(step, slot):
        return pltpu.make_async_copy(k_hbm.at[pl.ds(step * CHUNK, CHUNK)], kbuf.at[slot], k_sem.at[slot])

    def load_v(step, slot):
        return pltpu.make_async_copy(v_hbm.at[pl.ds(step * CHUNK, CHUNK)], vbuf.at[slot], v_sem.at[slot])

    def q_rows(step, role):
        return qbuf.at[role, pl.ds(step * CHUNK * ROWS, CHUNK * ROWS)]

    def q_mine(step):
        return q_rows(step, OWN)

    def remote(src, dst, send, recv, dev):
        return pltpu.make_async_remote_copy(
            src_ref=src, dst_ref=dst, send_sem=send, recv_sem=recv, device_id={"dup": dev}, device_id_type=MESH
        )

    def q_to_far(step):
        return remote(q_mine(step), q_rows(step, FAR), q_chip_send.at[step], q_chip_recv.at[step], far)

    def q_to_sib(step):
        return remote(q_mine(step), q_rows(step, SIB), q_sib_send.at[step], q_sib_recv.at[step], sib)

    def q_forward(step):
        return remote(q_rows(step, FAR), q_rows(step, FAR_SIB), q_fwd_send.at[step], q_fwd_recv.at[step], sib)

    def give_part(step):
        return remote(give.at[step], peer.at[step], part_send.at[step], part_recv.at[step], sib)

    def give_stat(step):
        return remote(stat.at[step], peer_stat.at[step], stat_send.at[step], stat_recv.at[step], sib)

    def give_out(step):
        return remote(send_out.at[step], recv_out.at[step], o_send.at[step], o_recv.at[step], far)

    def give_lse(step):
        return remote(send_lse.at[step], recv_lse.at[step], l_send.at[step], l_recv.at[step], far)

    whole_q = pltpu.make_async_copy(q_hbm, qbuf.at[OWN], q_local.at[0])
    whole_q.start()
    load_k(0, 0).start()

    barrier = pltpu.get_barrier_semaphore()
    for dev in (sib, far):
        pl.semaphore_signal(barrier, inc=1, device_id={"dup": dev}, device_id_type=MESH)
    pl.semaphore_wait(barrier, 2)
    whole_q.wait()
    for step in range(4):
        q_to_far(step).start()

    @pl.loop(0, n)
    def _(step):
        q_to_sib(step).start()

    load_v(0, 0).start()
    for step in range(1, RING):
        load_k(step, step).start()
        load_v(step, step).start()

    def forward_q(step):
        q_to_far(step).wait_recv()
        q_forward(step).start()

    def await_q(step):
        q_to_sib(step).wait_recv()
        q_forward(step).wait_recv()

    lane = lax.broadcasted_iota(jnp.int32, (ROWS, 128), 1)
    draft_of_row = lax.rem(lax.broadcasted_iota(jnp.int32, (ROWS, span), 0), DRAFT)
    reach = lax.broadcasted_iota(jnp.int32, (ROWS, span), 1) - draft_of_row + (me * span + DRAFT)
    rate = scale / math.log(2.0)

    first = lax.rem(lax.broadcasted_iota(jnp.int32, (16, 128), 0), 16) < ROWS
    of_first = jnp.where(first, 1.0, 0.0).astype(jnp.bfloat16)
    of_second = jnp.where(first, 0.0, 1.0).astype(jnp.bfloat16)

    def score_pair(step, slot, i):
        start = pl.multiple_of(step * CHUNK * ROWS, 16) + 16 * i
        q = [qbuf[role, pl.ds(start, 16), :] for role in range(4)]
        left = jnp.concatenate([jnp.concatenate([x * of_first, x * of_second], 1) for x in q], 0)
        k_a, k_b = kbuf[slot, 2 * i], kbuf[slot, 2 * i + 1]
        turned = span // 2
        right = jnp.concatenate([k_a[:turned], k_b[:turned]], 1)
        scores = lax.dot_general(left, right, (((1,), (1,)), ((), ())), preferred_element_type=jnp.float32)
        rest = jnp.concatenate([k_a[turned:].T, k_b[turned:].T], 0)
        more = lax.dot_general(left, rest, (((1,), (0,)), ((), ())), preferred_element_type=jnp.float32)
        return jnp.concatenate([scores, more], 1)

    def mask_pair(step, i, scores):
        for h in range(2):
            allowed = reach <= len_ref[step * CHUNK + 2 * i + h]
            for d in range(4):
                row = 16 * d + 8 * h
                s = jnp.where(allowed, scores[row : row + 8], LOWEST)
                sbuf[i, pl.ds(row, 8), :] = s
                peak = jnp.maximum(jnp.max(s, axis=1, keepdims=True), FLOOR)
                pbuf[i, pl.ds(row, 8), :] = jnp.broadcast_to(peak, (ROWS, 128))

    def weigh_pair(i, peaks, masses):
        for d in range(4):
            probs = []
            for h in range(2):
                row = 16 * d + 8 * h
                peak = pbuf[i, pl.ds(row, 8), :]
                s = sbuf[i, pl.ds(row, 8), :]
                p = jnp.exp2((s - jnp.concatenate([peak] * (span // 128), 1)) * rate)
                mass = jnp.sum(p, axis=1, keepdims=True)
                here = lane == (CHUNK * d + 2 * i + h)
                peaks = jnp.where(here, peak, peaks)
                masses = jnp.where(here, mass, masses)
                probs.append(p)
            ebuf[i, pl.ds(16 * d, 16), :] = jnp.concatenate(probs, 0).astype(jnp.bfloat16)
        return peaks, masses

    def sum_pair(step, slot, i):
        v = jnp.concatenate([vbuf[slot, 2 * i], vbuf[slot, 2 * i + 1]], 1)
        o = lax.dot_general(ebuf[i], v, (((1,), (0,)), ((), ())), preferred_element_type=jnp.float32)
        for h in range(2):
            for d in range(4):
                home = keep if d in (OWN, FAR) else give
                home[step, d % 2, 2 * i + h] = o[16 * d + 8 * h : 16 * d + 8 * h + 8, 128 * h : 128 * h + 128]

    def merge_chip(step):
        m_a, l_a = stat[step, 0], stat[step, 1]
        m_b, l_b = (pltpu.roll(peer_stat[step, j], 128 - SIB * CHUNK, 1) for j in range(2))
        top = jnp.maximum(m_a, m_b)
        w_a, w_b = jnp.exp2((m_a - top) * rate), jnp.exp2((m_b - top) * rate)
        total = w_a * l_a + w_b * l_b
        some = total > 0.0
        safe = jnp.where(some, total, 1.0)
        inverse = jnp.where(some, 1.0 / safe, 0.0)
        w_a, w_b = w_a * inverse, w_b * inverse
        lse = jnp.where(some, top * rate + jnp.log2(safe), LOWEST)
        own_lse[step] = lse
        send_lse[step] = pltpu.roll(lse, 128 - FAR * CHUNK, 1)

        def both(role, b):
            c = role * CHUNK + b
            return w_a[:, c : c + 1] * keep[step, role, b] + w_b[:, c : c + 1] * peer[step, role, b]

        for i in range(pairs):
            for b in (2 * i, 2 * i + 1):
                own_out[step, b] = both(OWN, b)
            far_out = [both(FAR, b) for b in (2 * i, 2 * i + 1)]
            send_out[step, pl.ds(16 * i, 16), :] = jnp.concatenate(far_out, 0).astype(jnp.bfloat16)

    def merge_final(step):
        rows = lax.rem(step, n) * CHUNK * ROWS
        mine, theirs = own_lse[step], recv_lse[step]
        top = jnp.maximum(mine, theirs)
        w_a, w_b = jnp.exp2(mine - top), jnp.exp2(theirs - top)
        inverse = 1.0 / (w_a + w_b)
        w_a, w_b = w_a * inverse, w_b * inverse
        for i in range(pairs):
            other = recv_out[step, pl.ds(16 * i, 16), :].astype(jnp.float32)
            outs = []
            for h in range(2):
                b = 2 * i + h
                outs.append(w_a[:, b : b + 1] * own_out[step, b] + w_b[:, b : b + 1] * other[8 * h : 8 * h + 8])
            out_buf[pl.ds(pl.multiple_of(rows + 16 * i, 16), 16), :] = jnp.concatenate(outs, 0).astype(jnp.bfloat16)

    def await_peer(step):
        give_part(step).wait_recv()
        give_stat(step).wait_recv()

    def send_far(step):
        give_out(step).start()
        give_lse(step).start()

    def await_far(step):
        give_out(step).wait_recv()
        give_lse(step).wait_recv()

    def final_stage(step):
        await_far(step)
        merge_final(step)

    def attend(step, with_next):
        slot, next_slot = lax.rem(step, RING), lax.rem(step + 1, RING)
        peaks = jnp.zeros((ROWS, 128), jnp.float32)
        masses = jnp.zeros((ROWS, 128), jnp.float32)
        scores = [None] * pairs
        for i in range(pairs + PV_LAG):
            if i < pairs:
                peaks, masses = weigh_pair(i, peaks, masses)
                if with_next:
                    scores[i] = score_pair(step + 1, next_slot, i)
            if i >= PV_LAG:
                sum_pair(step, slot, i - PV_LAG)
            if with_next and 1 <= i <= pairs:
                mask_pair(step + 1, i - 1, scores[i - 1])
        stat[step, 0] = peaks
        stat[step, 1] = masses

    last = n - 1
    for step in range(AHEAD):
        forward_q(step)
        q_to_far(2 * step + 4).start()
        q_to_far(2 * step + 5).start()
    await_q(0)
    load_k(0, 0).wait()
    for i in range(pairs):
        mask_pair(0, i, score_pair(0, 0, i))
    load_k(RING, 0).start()

    @pl.loop(0, last)
    def _(step):
        @pl.when(2 * step + 2 * AHEAD + 4 < n)
        def _():
            q_to_far(2 * step + 2 * AHEAD + 4).start()
            q_to_far(2 * step + 2 * AHEAD + 5).start()

        @pl.when(step + AHEAD < n)
        def _():
            forward_q(step + AHEAD)

        await_q(step + 1)
        load_k(step + 1, lax.rem(step + 1, RING)).wait()
        load_v(step, lax.rem(step, RING)).wait()

        @pl.when(step >= LAG)
        def _():
            await_peer(step - LAG)

        @pl.when(step >= FINAL_LAG)
        def _():
            await_far(step - FINAL_LAG)

        done = (step + n - FINAL_LAG) // n
        merge_final(done * (step - FINAL_LAG) + (1 - done) * n)
        ready = (step + n - LAG) // n
        merge_chip(ready * (step - LAG) + (1 - ready) * n)
        attend(step, True)
        give_part(step).start()
        give_stat(step).start()

        @pl.when(step >= LAG)
        def _():
            send_far(step - LAG)

        @pl.when(step + 1 + RING < n)
        def _():
            load_k(step + 1 + RING, lax.rem(step + 1, RING)).start()

        @pl.when(step + RING < n)
        def _():
            load_v(step + RING, lax.rem(step, RING)).start()

    load_v(last, lax.rem(last, RING)).wait()
    await_peer(last - LAG)
    await_far(last - FINAL_LAG)
    merge_final(last - FINAL_LAG)
    merge_chip(last - LAG)
    attend(last, False)
    give_part(last).start()
    give_stat(last).start()
    send_far(last - LAG)

    @pl.loop(last - LAG + 1, last)
    def _(step):
        await_peer(step)
        merge_chip(step)
        send_far(step)

    @pl.loop(last - FINAL_LAG + 1, last - FINAL_LAG + 1 + EARLY_FINALS)
    def _(step):
        final_stage(step)

    await_peer(last)
    merge_chip(last)
    send_far(last)

    @pl.loop(last - FINAL_LAG + 1 + EARLY_FINALS, n)
    def _(step):
        final_stage(step)

    @pl.loop(0, n)
    def _(step):
        q_to_far(step).wait_send()
        q_to_sib(step).wait_send()
        q_forward(step).wait_send()
        give_part(step).wait_send()
        give_stat(step).wait_send()
        give_out(step).wait_send()
        give_lse(step).wait_send()


def solution(mesh):
    def group_step(q_local, k_span, v_span, len_local):
        num_batch, span, dim = k_span.shape
        n = num_batch // CHUNK
        f32, bf16 = jnp.float32, jnp.bfloat16
        dma = lambda *shape: pltpu.SemaphoreType.DMA(shape)
        hbm = pl.BlockSpec(memory_space=pltpu.HBM)
        out = pl.pallas_call(
            functools.partial(kernel, n, dim**-0.5),
            out_shape=pltpu.VMEM((num_batch * ROWS, dim), bf16),
            in_specs=[pl.BlockSpec(memory_space=pltpu.SMEM), hbm, hbm, hbm],
            out_specs=pl.BlockSpec(memory_space=pltpu.VMEM),
            scratch_shapes=[
                pltpu.VMEM((RING, CHUNK, span, dim), bf16),
                pltpu.VMEM((RING, CHUNK, span, dim), bf16),
                pltpu.VMEM((4, num_batch * ROWS, dim), bf16),
                pltpu.VMEM((CHUNK // 2, 64, span), f32),
                pltpu.VMEM((CHUNK // 2, 64, 128), f32),
                pltpu.VMEM((CHUNK // 2, 64, span), bf16),
                pltpu.VMEM((n + 1, 2, CHUNK, ROWS, dim), f32),
                pltpu.VMEM((n, 2, CHUNK, ROWS, dim), f32),
                pltpu.VMEM((n + 1, 2, CHUNK, ROWS, dim), f32),
                pltpu.VMEM((n + 1, 2, ROWS, dim), f32),
                pltpu.VMEM((n + 1, 2, ROWS, dim), f32),
                pltpu.VMEM((n + 1, CHUNK, ROWS, dim), f32),
                pltpu.VMEM((n + 1, CHUNK * ROWS, dim), bf16),
                pltpu.VMEM((n + 1, ROWS, dim), f32),
                pltpu.VMEM((n + 1, CHUNK * ROWS, dim), bf16),
                pltpu.VMEM((n + 1, ROWS, dim), f32),
                pltpu.VMEM((n + 1, ROWS, dim), f32),
                dma(RING),
                dma(RING),
                dma(1),
            ]
            + [dma(n)] * 14,
            compiler_params=pltpu.CompilerParams(
                collective_id=0, has_side_effects=True, vmem_limit_bytes=56 * 1024 * 1024
            ),
        )(len_local, q_local.reshape(num_batch * ROWS, dim), k_span, v_span)
        return out.reshape(num_batch, ROWS, dim)

    return jax.shard_map(
        group_step,
        mesh=mesh,
        in_specs=(P("kv", "dup", None), P("kv", "dup", None), P("kv", "dup", None), P("kv")),
        out_specs=P("kv", "dup", None),
        check_vma=False,
    )
```

```python
import functools
import math

import jax
import jax.numpy as jnp
from jax import lax
from jax.experimental import pallas as pl
from jax.experimental.pallas import tpu as pltpu
from jax.sharding import PartitionSpec as P

DRAFT = 4
CHUNK = 16
RING = 4
AHEAD = 2
LAG = 2
FINAL_LAG = 8
EARLY_FINALS = 4
PV_LAG = 2
ROWS = 8
OWN, FAR, SIB, FAR_SIB = range(4)
MESH = pl.DeviceIdType.MESH
LOWEST = -3.0e38
FLOOR = -2.0e38


def kernel(
    num_chunks,
    scale,
    len_ref,
    q_hbm,
    k_hbm,
    v_hbm,
    out_buf,
    kbuf,
    vbuf,
    qbuf,
    sbuf,
    pbuf,
    ebuf,
    keep,
    give,
    peer,
    stat,
    peer_stat,
    own_out,
    send_out,
    send_lse,
    recv_out,
    recv_lse,
    own_lse,
    k_sem,
    v_sem,
    q_local,
    q_chip_send,
    q_chip_recv,
    q_sib_send,
    q_sib_recv,
    q_fwd_send,
    q_fwd_recv,
    part_send,
    part_recv,
    stat_send,
    stat_recv,
    o_send,
    o_recv,
    l_send,
    l_recv,
):
    me = lax.axis_index("dup")
    chip, core = me // 2, lax.rem(me, 2)
    sib = 2 * chip + (1 - core)
    far = 2 * (1 - chip) + core
    span = kbuf.shape[2]
    pairs = CHUNK // 2
    n = num_chunks

    def load_k(step, slot):
        return pltpu.make_async_copy(k_hbm.at[pl.ds(step * CHUNK, CHUNK)], kbuf.at[slot], k_sem.at[slot])

    def load_v(step, slot):
        return pltpu.make_async_copy(v_hbm.at[pl.ds(step * CHUNK, CHUNK)], vbuf.at[slot], v_sem.at[slot])

    def q_rows(step, role):
        return qbuf.at[role, pl.ds(step * CHUNK * ROWS, CHUNK * ROWS)]

    def q_mine(step):
        return q_rows(step, OWN)

    def remote(src, dst, send, recv, dev):
        return pltpu.make_async_remote_copy(
            src_ref=src, dst_ref=dst, send_sem=send, recv_sem=recv, device_id={"dup": dev}, device_id_type=MESH
        )

    def q_to_far(step):
        return remote(q_mine(step), q_rows(step, FAR), q_chip_send.at[step], q_chip_recv.at[step], far)

    def q_to_sib(step):
        return remote(q_mine(step), q_rows(step, SIB), q_sib_send.at[step], q_sib_recv.at[step], sib)

    def q_forward(step):
        return remote(q_rows(step, FAR), q_rows(step, FAR_SIB), q_fwd_send.at[step], q_fwd_recv.at[step], sib)

    def give_part(step):
        return remote(give.at[step], peer.at[step], part_send.at[step], part_recv.at[step], sib)

    def give_stat(step):
        return remote(stat.at[step], peer_stat.at[step], stat_send.at[step], stat_recv.at[step], sib)

    def give_out(step):
        return remote(send_out.at[step], recv_out.at[step], o_send.at[step], o_recv.at[step], far)

    def give_lse(step):
        return remote(send_lse.at[step], recv_lse.at[step], l_send.at[step], l_recv.at[step], far)

    whole_q = pltpu.make_async_copy(q_hbm, qbuf.at[OWN], q_local.at[0])
    whole_q.start()
    load_k(0, 0).start()

    barrier = pltpu.get_barrier_semaphore()
    for dev in (sib, far):
        pl.semaphore_signal(barrier, inc=1, device_id={"dup": dev}, device_id_type=MESH)
    pl.semaphore_wait(barrier, 2)
    whole_q.wait()
    for step in range(4):
        q_to_far(step).start()

    @pl.loop(0, n)
    def _(step):
        q_to_sib(step).start()

    load_v(0, 0).start()
    load_k(1, 1).start()

    def forward_q(step):
        q_to_far(step).wait_recv()
        q_forward(step).start()

    def await_q(step):
        q_to_sib(step).wait_recv()
        q_forward(step).wait_recv()

    lane = lax.broadcasted_iota(jnp.int32, (ROWS, 128), 1)
    draft_of_row = lax.rem(lax.broadcasted_iota(jnp.int32, (ROWS, span), 0), DRAFT)
    reach = lax.broadcasted_iota(jnp.int32, (ROWS, span), 1) - draft_of_row + (me * span + DRAFT)
    rate = scale / math.log(2.0)

    first = lax.rem(lax.broadcasted_iota(jnp.int32, (16, 128), 0), 16) < ROWS
    of_first = jnp.where(first, 1.0, 0.0).astype(jnp.bfloat16)
    of_second = jnp.where(first, 0.0, 1.0).astype(jnp.bfloat16)

    def score_pair(step, slot, i):
        start = pl.multiple_of(step * CHUNK * ROWS, 16) + 16 * i
        q = [qbuf[role, pl.ds(start, 16), :] for role in range(4)]
        left = jnp.concatenate([jnp.concatenate([x * of_first, x * of_second], 1) for x in q], 0)
        k_a, k_b = kbuf[slot, 2 * i], kbuf[slot, 2 * i + 1]
        turned = span // 2
        right = jnp.concatenate([k_a[:turned], k_b[:turned]], 1)
        scores = lax.dot_general(left, right, (((1,), (1,)), ((), ())), preferred_element_type=jnp.float32)
        rest = jnp.concatenate([k_a[turned:].T, k_b[turned:].T], 0)
        more = lax.dot_general(left, rest, (((1,), (0,)), ((), ())), preferred_element_type=jnp.float32)
        return jnp.concatenate([scores, more], 1)

    def mask_pair(step, i, scores):
        for h in range(2):
            allowed = reach <= len_ref[step * CHUNK + 2 * i + h]
            for d in range(4):
                row = 16 * d + 8 * h
                s = jnp.where(allowed, scores[row : row + 8], LOWEST)
                sbuf[i, pl.ds(row, 8), :] = s
                peak = jnp.maximum(jnp.max(s, axis=1, keepdims=True), FLOOR)
                pbuf[i, pl.ds(row, 8), :] = jnp.broadcast_to(peak, (ROWS, 128))

    def weigh_pair(i, peaks, masses):
        for d in range(4):
            probs = []
            for h in range(2):
                row = 16 * d + 8 * h
                peak = pbuf[i, pl.ds(row, 8), :]
                s = sbuf[i, pl.ds(row, 8), :]
                p = jnp.exp2((s - jnp.concatenate([peak] * (span // 128), 1)) * rate)
                mass = jnp.sum(p, axis=1, keepdims=True)
                here = lane == (CHUNK * d + 2 * i + h)
                peaks = jnp.where(here, peak, peaks)
                masses = jnp.where(here, mass, masses)
                probs.append(p)
            ebuf[i, pl.ds(16 * d, 16), :] = jnp.concatenate(probs, 0).astype(jnp.bfloat16)
        return peaks, masses

    def sum_pair(step, slot, i):
        v = jnp.concatenate([vbuf[slot, 2 * i], vbuf[slot, 2 * i + 1]], 1)
        o = lax.dot_general(ebuf[i], v, (((1,), (0,)), ((), ())), preferred_element_type=jnp.float32)
        for h in range(2):
            for d in range(4):
                home = keep if d in (OWN, FAR) else give
                home[step, d % 2, 2 * i + h] = o[16 * d + 8 * h : 16 * d + 8 * h + 8, 128 * h : 128 * h + 128]

    def merge_chip(step):
        m_a, l_a = stat[step, 0], stat[step, 1]
        m_b, l_b = (pltpu.roll(peer_stat[step, j], 128 - SIB * CHUNK, 1) for j in range(2))
        top = jnp.maximum(m_a, m_b)
        w_a, w_b = jnp.exp2((m_a - top) * rate), jnp.exp2((m_b - top) * rate)
        total = w_a * l_a + w_b * l_b
        some = total > 0.0
        safe = jnp.where(some, total, 1.0)
        inverse = jnp.where(some, 1.0 / safe, 0.0)
        w_a, w_b = w_a * inverse, w_b * inverse
        lse = jnp.where(some, top * rate + jnp.log2(safe), LOWEST)
        own_lse[step] = lse
        send_lse[step] = pltpu.roll(lse, 128 - FAR * CHUNK, 1)

        def both(role, b):
            c = role * CHUNK + b
            return w_a[:, c : c + 1] * keep[step, role, b] + w_b[:, c : c + 1] * peer[step, role, b]

        for i in range(pairs):
            for b in (2 * i, 2 * i + 1):
                own_out[step, b] = both(OWN, b)
            far_out = [both(FAR, b) for b in (2 * i, 2 * i + 1)]
            send_out[step, pl.ds(16 * i, 16), :] = jnp.concatenate(far_out, 0).astype(jnp.bfloat16)

    def merge_final(step):
        rows = lax.rem(step, n) * CHUNK * ROWS
        mine, theirs = own_lse[step], recv_lse[step]
        top = jnp.maximum(mine, theirs)
        w_a, w_b = jnp.exp2(mine - top), jnp.exp2(theirs - top)
        inverse = 1.0 / (w_a + w_b)
        w_a, w_b = w_a * inverse, w_b * inverse
        for i in range(pairs):
            other = recv_out[step, pl.ds(16 * i, 16), :].astype(jnp.float32)
            outs = []
            for h in range(2):
                b = 2 * i + h
                outs.append(w_a[:, b : b + 1] * own_out[step, b] + w_b[:, b : b + 1] * other[8 * h : 8 * h + 8])
            out_buf[pl.ds(pl.multiple_of(rows + 16 * i, 16), 16), :] = jnp.concatenate(outs, 0).astype(jnp.bfloat16)

    def await_peer(step):
        give_part(step).wait_recv()
        give_stat(step).wait_recv()

    def send_far(step):
        give_out(step).start()
        give_lse(step).start()

    def await_far(step):
        give_out(step).wait_recv()
        give_lse(step).wait_recv()

    def final_stage(step):
        await_far(step)
        merge_final(step)

    def attend(step, with_next):
        slot, next_slot = lax.rem(step, RING), lax.rem(step + 1, RING)
        peaks = jnp.zeros((ROWS, 128), jnp.float32)
        masses = jnp.zeros((ROWS, 128), jnp.float32)
        scores = [None] * pairs
        for i in range(pairs + PV_LAG):
            if i < pairs:
                peaks, masses = weigh_pair(i, peaks, masses)
                if with_next:
                    scores[i] = score_pair(step + 1, next_slot, i)
            if i >= PV_LAG:
                sum_pair(step, slot, i - PV_LAG)
            if with_next and 1 <= i <= pairs:
                mask_pair(step + 1, i - 1, scores[i - 1])
        stat[step, 0] = peaks
        stat[step, 1] = masses

    last = n - 1
    for step in range(AHEAD):
        forward_q(step)
        q_to_far(2 * step + 4).start()
        q_to_far(2 * step + 5).start()
    load_v(1, 1).start()
    load_k(2, 2).start()
    await_q(0)
    load_k(0, 0).wait()
    for i in range(pairs):
        mask_pair(0, i, score_pair(0, 0, i))
    load_v(2, 2).start()
    load_k(3, 3).start()

    @pl.loop(0, last)
    def _(step):
        @pl.when(2 * step + 2 * AHEAD + 4 < n)
        def _():
            q_to_far(2 * step + 2 * AHEAD + 4).start()
            q_to_far(2 * step + 2 * AHEAD + 5).start()

        @pl.when(step + AHEAD < n)
        def _():
            forward_q(step + AHEAD)

        @pl.when(step + RING < n)
        def _():
            load_k(step + RING, lax.rem(step, RING)).start()

        @pl.when(step + RING - 1 < n)
        def _():
            load_v(step + RING - 1, lax.rem(step + RING - 1, RING)).start()

        await_q(step + 1)
        load_k(step + 1, lax.rem(step + 1, RING)).wait()
        load_v(step, lax.rem(step, RING)).wait()

        @pl.when(step >= LAG)
        def _():
            await_peer(step - LAG)

        @pl.when(step >= FINAL_LAG)
        def _():
            await_far(step - FINAL_LAG)

        done = (step + n - FINAL_LAG) // n
        merge_final(done * (step - FINAL_LAG) + (1 - done) * n)
        ready = (step + n - LAG) // n
        merge_chip(ready * (step - LAG) + (1 - ready) * n)
        attend(step, True)
        give_part(step).start()
        give_stat(step).start()

        @pl.when(step >= LAG)
        def _():
            send_far(step - LAG)

    load_v(last, lax.rem(last, RING)).wait()
    await_peer(last - LAG)
    await_far(last - FINAL_LAG)
    merge_final(last - FINAL_LAG)
    merge_chip(last - LAG)
    attend(last, False)
    give_part(last).start()
    give_stat(last).start()
    send_far(last - LAG)

    @pl.loop(last - LAG + 1, last)
    def _(step):
        await_peer(step)
        merge_chip(step)
        send_far(step)

    @pl.loop(last - FINAL_LAG + 1, last - FINAL_LAG + 1 + EARLY_FINALS)
    def _(step):
        final_stage(step)

    await_peer(last)
    merge_chip(last)
    send_far(last)

    @pl.loop(last - FINAL_LAG + 1 + EARLY_FINALS, n)
    def _(step):
        final_stage(step)

    @pl.loop(0, n)
    def _(step):
        q_to_far(step).wait_send()
        q_to_sib(step).wait_send()
        q_forward(step).wait_send()
        give_part(step).wait_send()
        give_stat(step).wait_send()
        give_out(step).wait_send()
        give_lse(step).wait_send()


def solution(mesh):
    def group_step(q_local, k_span, v_span, len_local):
        num_batch, span, dim = k_span.shape
        n = num_batch // CHUNK
        f32, bf16 = jnp.float32, jnp.bfloat16
        dma = lambda *shape: pltpu.SemaphoreType.DMA(shape)
        hbm = pl.BlockSpec(memory_space=pltpu.HBM)
        out = pl.pallas_call(
            functools.partial(kernel, n, dim**-0.5),
            out_shape=pltpu.VMEM((num_batch * ROWS, dim), bf16),
            in_specs=[pl.BlockSpec(memory_space=pltpu.SMEM), hbm, hbm, hbm],
            out_specs=pl.BlockSpec(memory_space=pltpu.VMEM),
            scratch_shapes=[
                pltpu.VMEM((RING, CHUNK, span, dim), bf16),
                pltpu.VMEM((RING, CHUNK, span, dim), bf16),
                pltpu.VMEM((4, num_batch * ROWS, dim), bf16),
                pltpu.VMEM((CHUNK // 2, 64, span), f32),
                pltpu.VMEM((CHUNK // 2, 64, 128), f32),
                pltpu.VMEM((CHUNK // 2, 64, span), bf16),
                pltpu.VMEM((n + 1, 2, CHUNK, ROWS, dim), f32),
                pltpu.VMEM((n, 2, CHUNK, ROWS, dim), f32),
                pltpu.VMEM((n + 1, 2, CHUNK, ROWS, dim), f32),
                pltpu.VMEM((n + 1, 2, ROWS, dim), f32),
                pltpu.VMEM((n + 1, 2, ROWS, dim), f32),
                pltpu.VMEM((n + 1, CHUNK, ROWS, dim), f32),
                pltpu.VMEM((n + 1, CHUNK * ROWS, dim), bf16),
                pltpu.VMEM((n + 1, ROWS, dim), f32),
                pltpu.VMEM((n + 1, CHUNK * ROWS, dim), bf16),
                pltpu.VMEM((n + 1, ROWS, dim), f32),
                pltpu.VMEM((n + 1, ROWS, dim), f32),
                dma(RING),
                dma(RING),
                dma(1),
            ]
            + [dma(n)] * 14,
            compiler_params=pltpu.CompilerParams(
                collective_id=0, has_side_effects=True, vmem_limit_bytes=56 * 1024 * 1024
            ),
        )(len_local, q_local.reshape(num_batch * ROWS, dim), k_span, v_span)
        return out.reshape(num_batch, ROWS, dim)

    return jax.shard_map(
        group_step,
        mesh=mesh,
        in_specs=(P("kv", "dup", None), P("kv", "dup", None), P("kv", "dup", None), P("kv")),
        out_specs=P("kv", "dup", None),
        check_vma=False,
    )
```

```python
import functools
import math

import jax
import jax.numpy as jnp
from jax import lax
from jax.experimental import pallas as pl
from jax.experimental.pallas import tpu as pltpu
from jax.sharding import PartitionSpec as P

DRAFT = 4
CHUNK = 16
RING = 6
AHEAD = 3
LAG = 2
FINAL_LAG = 8
EARLY_FINALS = 4
PV_LAG = 2
ROWS = 8
OWN, FAR, SIB, FAR_SIB = range(4)
MESH = pl.DeviceIdType.MESH
LOWEST = -3.0e38
FLOOR = -2.0e38


def kernel(
    num_chunks,
    scale,
    len_ref,
    q_hbm,
    k_hbm,
    v_hbm,
    out_buf,
    kbuf,
    vbuf,
    qbuf,
    sbuf,
    pbuf,
    ebuf,
    keep,
    give,
    peer,
    stat,
    peer_stat,
    own_out,
    send_out,
    send_lse,
    recv_out,
    recv_lse,
    own_lse,
    k_sem,
    v_sem,
    q_local,
    q_chip_send,
    q_chip_recv,
    q_sib_send,
    q_sib_recv,
    q_fwd_send,
    q_fwd_recv,
    part_send,
    part_recv,
    stat_send,
    stat_recv,
    o_send,
    o_recv,
    l_send,
    l_recv,
):
    me = lax.axis_index("dup")
    chip, core = me // 2, lax.rem(me, 2)
    sib = 2 * chip + (1 - core)
    far = 2 * (1 - chip) + core
    span = kbuf.shape[2]
    pairs = CHUNK // 2
    n = num_chunks

    def load_k(step, slot):
        return pltpu.make_async_copy(k_hbm.at[pl.ds(step * CHUNK, CHUNK)], kbuf.at[slot], k_sem.at[slot])

    def load_v(step, slot):
        return pltpu.make_async_copy(v_hbm.at[pl.ds(step * CHUNK, CHUNK)], vbuf.at[slot], v_sem.at[slot])

    def refill(first, end):
        for step in range(first, end):
            load_v(step, step).start()
            if step + 1 < RING:
                load_k(step + 1, step + 1).start()

    def q_rows(step, role):
        return qbuf.at[role, pl.ds(step * CHUNK * ROWS, CHUNK * ROWS)]

    def q_mine(step):
        return q_rows(step, OWN)

    def remote(src, dst, send, recv, dev):
        return pltpu.make_async_remote_copy(
            src_ref=src, dst_ref=dst, send_sem=send, recv_sem=recv, device_id={"dup": dev}, device_id_type=MESH
        )

    def q_to_far(step):
        return remote(q_mine(step), q_rows(step, FAR), q_chip_send.at[step], q_chip_recv.at[step], far)

    def q_to_sib(step):
        return remote(q_mine(step), q_rows(step, SIB), q_sib_send.at[step], q_sib_recv.at[step], sib)

    def q_forward(step):
        return remote(q_rows(step, FAR), q_rows(step, FAR_SIB), q_fwd_send.at[step], q_fwd_recv.at[step], sib)

    def give_part(step):
        return remote(give.at[step], peer.at[step], part_send.at[step], part_recv.at[step], sib)

    def give_stat(step):
        return remote(stat.at[step], peer_stat.at[step], stat_send.at[step], stat_recv.at[step], sib)

    def give_out(step):
        return remote(send_out.at[step], recv_out.at[step], o_send.at[step], o_recv.at[step], far)

    def give_lse(step):
        return remote(send_lse.at[step], recv_lse.at[step], l_send.at[step], l_recv.at[step], far)

    whole_q = pltpu.make_async_copy(q_hbm, qbuf.at[OWN], q_local.at[0])
    whole_q.start()
    load_k(0, 0).start()

    barrier = pltpu.get_barrier_semaphore()
    for dev in (sib, far):
        pl.semaphore_signal(barrier, inc=1, device_id={"dup": dev}, device_id_type=MESH)
    pl.semaphore_wait(barrier, 2)
    whole_q.wait()
    for step in range(4):
        q_to_far(step).start()

    @pl.loop(0, n)
    def _(step):
        q_to_sib(step).start()

    refill(0, 2)

    def forward_q(step):
        q_to_far(step).wait_recv()
        q_forward(step).start()

    def await_q(step):
        q_to_sib(step).wait_recv()
        q_forward(step).wait_recv()

    lane = lax.broadcasted_iota(jnp.int32, (ROWS, 128), 1)
    draft_of_row = lax.rem(lax.broadcasted_iota(jnp.int32, (ROWS, span), 0), DRAFT)
    reach = lax.broadcasted_iota(jnp.int32, (ROWS, span), 1) - draft_of_row + (me * span + DRAFT)
    rate = scale / math.log(2.0)

    first = lax.rem(lax.broadcasted_iota(jnp.int32, (16, 128), 0), 16) < ROWS
    of_first = jnp.where(first, 1.0, 0.0).astype(jnp.bfloat16)
    of_second = jnp.where(first, 0.0, 1.0).astype(jnp.bfloat16)

    def score_pair(step, slot, i):
        start = pl.multiple_of(step * CHUNK * ROWS, 16) + 16 * i
        q = [qbuf[role, pl.ds(start, 16), :] for role in range(4)]
        left = jnp.concatenate([jnp.concatenate([x * of_first, x * of_second], 1) for x in q], 0)
        k_a, k_b = kbuf[slot, 2 * i], kbuf[slot, 2 * i + 1]
        turned = span // 2
        right = jnp.concatenate([k_a[:turned], k_b[:turned]], 1)
        scores = lax.dot_general(left, right, (((1,), (1,)), ((), ())), preferred_element_type=jnp.float32)
        rest = jnp.concatenate([k_a[turned:].T, k_b[turned:].T], 0)
        more = lax.dot_general(left, rest, (((1,), (0,)), ((), ())), preferred_element_type=jnp.float32)
        return jnp.concatenate([scores, more], 1)

    def mask_pair(step, i, scores):
        for h in range(2):
            allowed = reach <= len_ref[step * CHUNK + 2 * i + h]
            for d in range(4):
                row = 16 * d + 8 * h
                s = jnp.where(allowed, scores[row : row + 8], LOWEST)
                sbuf[i, pl.ds(row, 8), :] = s
                peak = jnp.maximum(jnp.max(s, axis=1, keepdims=True), FLOOR)
                pbuf[i, pl.ds(row, 8), :] = jnp.broadcast_to(peak, (ROWS, 128))

    def weigh_pair(i, peaks, masses):
        for d in range(4):
            probs = []
            for h in range(2):
                row = 16 * d + 8 * h
                peak = pbuf[i, pl.ds(row, 8), :]
                s = sbuf[i, pl.ds(row, 8), :]
                p = jnp.exp2((s - jnp.concatenate([peak] * (span // 128), 1)) * rate)
                mass = jnp.sum(p, axis=1, keepdims=True)
                here = lane == (CHUNK * d + 2 * i + h)
                peaks = jnp.where(here, peak, peaks)
                masses = jnp.where(here, mass, masses)
                probs.append(p)
            ebuf[i, pl.ds(16 * d, 16), :] = jnp.concatenate(probs, 0).astype(jnp.bfloat16)
        return peaks, masses

    def sum_pair(step, slot, i):
        v = jnp.concatenate([vbuf[slot, 2 * i], vbuf[slot, 2 * i + 1]], 1)
        o = lax.dot_general(ebuf[i], v, (((1,), (0,)), ((), ())), preferred_element_type=jnp.float32)
        for h in range(2):
            for d in range(4):
                home = keep if d in (OWN, FAR) else give
                home[step, d % 2, 2 * i + h] = o[16 * d + 8 * h : 16 * d + 8 * h + 8, 128 * h : 128 * h + 128]

    def merge_chip(step):
        m_a, l_a = stat[step, 0], stat[step, 1]
        m_b, l_b = (pltpu.roll(peer_stat[step, j], 128 - SIB * CHUNK, 1) for j in range(2))
        top = jnp.maximum(m_a, m_b)
        w_a, w_b = jnp.exp2((m_a - top) * rate), jnp.exp2((m_b - top) * rate)
        total = w_a * l_a + w_b * l_b
        some = total > 0.0
        safe = jnp.where(some, total, 1.0)
        inverse = jnp.where(some, 1.0 / safe, 0.0)
        w_a, w_b = w_a * inverse, w_b * inverse
        lse = jnp.where(some, top * rate + jnp.log2(safe), LOWEST)
        own_lse[step] = lse
        send_lse[step] = pltpu.roll(lse, 128 - FAR * CHUNK, 1)

        def both(role, b):
            c = role * CHUNK + b
            return w_a[:, c : c + 1] * keep[step, role, b] + w_b[:, c : c + 1] * peer[step, role, b]

        for i in range(pairs):
            for b in (2 * i, 2 * i + 1):
                own_out[step, b] = both(OWN, b)
            far_out = [both(FAR, b) for b in (2 * i, 2 * i + 1)]
            send_out[step, pl.ds(16 * i, 16), :] = jnp.concatenate(far_out, 0).astype(jnp.bfloat16)

    def merge_final(step):
        rows = lax.rem(step, n) * CHUNK * ROWS
        mine, theirs = own_lse[step], recv_lse[step]
        top = jnp.maximum(mine, theirs)
        w_a, w_b = jnp.exp2(mine - top), jnp.exp2(theirs - top)
        inverse = 1.0 / (w_a + w_b)
        w_a, w_b = w_a * inverse, w_b * inverse
        for i in range(pairs):
            other = recv_out[step, pl.ds(16 * i, 16), :].astype(jnp.float32)
            outs = []
            for h in range(2):
                b = 2 * i + h
                outs.append(w_a[:, b : b + 1] * own_out[step, b] + w_b[:, b : b + 1] * other[8 * h : 8 * h + 8])
            out_buf[pl.ds(pl.multiple_of(rows + 16 * i, 16), 16), :] = jnp.concatenate(outs, 0).astype(jnp.bfloat16)

    def await_peer(step):
        give_part(step).wait_recv()
        give_stat(step).wait_recv()

    def send_far(step):
        give_out(step).start()
        give_lse(step).start()

    def await_far(step):
        give_out(step).wait_recv()
        give_lse(step).wait_recv()

    def final_stage(step):
        await_far(step)
        merge_final(step)

    def attend(step, with_next):
        slot, next_slot = lax.rem(step, RING), lax.rem(step + 1, RING)
        peaks = jnp.zeros((ROWS, 128), jnp.float32)
        masses = jnp.zeros((ROWS, 128), jnp.float32)
        scores = [None] * pairs
        for i in range(pairs + PV_LAG):
            if i < pairs:
                peaks, masses = weigh_pair(i, peaks, masses)
                if with_next:
                    scores[i] = score_pair(step + 1, next_slot, i)
            if i >= PV_LAG:
                sum_pair(step, slot, i - PV_LAG)
            if with_next and 1 <= i <= pairs:
                mask_pair(step + 1, i - 1, scores[i - 1])
        stat[step, 0] = peaks
        stat[step, 1] = masses

    last = n - 1
    def start_q(step):
        forward_q(step)
        q_to_far(2 * step + 4).start()
        q_to_far(2 * step + 5).start()

    start_q(0)
    start_q(1)
    refill(2, 3)
    await_q(0)
    load_k(0, 0).wait()
    start_q(2)
    refill(3, RING)
    for i in range(pairs):
        mask_pair(0, i, score_pair(0, 0, i))
    load_k(RING, 0).start()

    @pl.loop(0, last)
    def _(step):
        @pl.when(2 * step + 2 * AHEAD + 4 < n)
        def _():
            q_to_far(2 * step + 2 * AHEAD + 4).start()
            q_to_far(2 * step + 2 * AHEAD + 5).start()

        @pl.when(step + AHEAD < n)
        def _():
            forward_q(step + AHEAD)

        await_q(step + 1)
        load_k(step + 1, lax.rem(step + 1, RING)).wait()
        load_v(step, lax.rem(step, RING)).wait()

        @pl.when(step >= LAG)
        def _():
            await_peer(step - LAG)

        @pl.when(step >= FINAL_LAG)
        def _():
            await_far(step - FINAL_LAG)

        done = (step + n - FINAL_LAG) // n
        merge_final(done * (step - FINAL_LAG) + (1 - done) * n)
        ready = (step + n - LAG) // n
        merge_chip(ready * (step - LAG) + (1 - ready) * n)
        attend(step, True)
        give_part(step).start()
        give_stat(step).start()

        @pl.when(step >= LAG)
        def _():
            send_far(step - LAG)

        @pl.when(step + 1 + RING < n)
        def _():
            load_k(step + 1 + RING, lax.rem(step + 1, RING)).start()

        @pl.when(step + RING < n)
        def _():
            load_v(step + RING, lax.rem(step, RING)).start()

    load_v(last, lax.rem(last, RING)).wait()
    await_peer(last - LAG)
    await_far(last - FINAL_LAG)
    merge_final(last - FINAL_LAG)
    merge_chip(last - LAG)
    attend(last, False)
    give_part(last).start()
    give_stat(last).start()
    send_far(last - LAG)

    @pl.loop(last - LAG + 1, last)
    def _(step):
        await_peer(step)
        merge_chip(step)
        send_far(step)

    @pl.loop(last - FINAL_LAG + 1, last - FINAL_LAG + 1 + EARLY_FINALS)
    def _(step):
        final_stage(step)

    await_peer(last)
    merge_chip(last)
    send_far(last)

    @pl.loop(last - FINAL_LAG + 1 + EARLY_FINALS, n)
    def _(step):
        final_stage(step)

    @pl.loop(0, n)
    def _(step):
        q_to_far(step).wait_send()
        q_to_sib(step).wait_send()
        q_forward(step).wait_send()
        give_part(step).wait_send()
        give_stat(step).wait_send()
        give_out(step).wait_send()
        give_lse(step).wait_send()


def solution(mesh):
    def group_step(q_local, k_span, v_span, len_local):
        num_batch, span, dim = k_span.shape
        n = num_batch // CHUNK
        f32, bf16 = jnp.float32, jnp.bfloat16
        dma = lambda *shape: pltpu.SemaphoreType.DMA(shape)
        hbm = pl.BlockSpec(memory_space=pltpu.HBM)
        out = pl.pallas_call(
            functools.partial(kernel, n, dim**-0.5),
            out_shape=pltpu.VMEM((num_batch * ROWS, dim), bf16),
            in_specs=[pl.BlockSpec(memory_space=pltpu.SMEM), hbm, hbm, hbm],
            out_specs=pl.BlockSpec(memory_space=pltpu.VMEM),
            scratch_shapes=[
                pltpu.VMEM((RING, CHUNK, span, dim), bf16),
                pltpu.VMEM((RING, CHUNK, span, dim), bf16),
                pltpu.VMEM((4, num_batch * ROWS, dim), bf16),
                pltpu.VMEM((CHUNK // 2, 64, span), f32),
                pltpu.VMEM((CHUNK // 2, 64, 128), f32),
                pltpu.VMEM((CHUNK // 2, 64, span), bf16),
                pltpu.VMEM((n + 1, 2, CHUNK, ROWS, dim), f32),
                pltpu.VMEM((n, 2, CHUNK, ROWS, dim), f32),
                pltpu.VMEM((n + 1, 2, CHUNK, ROWS, dim), f32),
                pltpu.VMEM((n + 1, 2, ROWS, dim), f32),
                pltpu.VMEM((n + 1, 2, ROWS, dim), f32),
                pltpu.VMEM((n + 1, CHUNK, ROWS, dim), f32),
                pltpu.VMEM((n + 1, CHUNK * ROWS, dim), bf16),
                pltpu.VMEM((n + 1, ROWS, dim), f32),
                pltpu.VMEM((n + 1, CHUNK * ROWS, dim), bf16),
                pltpu.VMEM((n + 1, ROWS, dim), f32),
                pltpu.VMEM((n + 1, ROWS, dim), f32),
                dma(RING),
                dma(RING),
                dma(1),
            ]
            + [dma(n)] * 14,
            compiler_params=pltpu.CompilerParams(
                collective_id=0, has_side_effects=True, vmem_limit_bytes=56 * 1024 * 1024
            ),
        )(len_local, q_local.reshape(num_batch * ROWS, dim), k_span, v_span)
        return out.reshape(num_batch, ROWS, dim)

    return jax.shard_map(
        group_step,
        mesh=mesh,
        in_specs=(P("kv", "dup", None), P("kv", "dup", None), P("kv", "dup", None), P("kv")),
        out_specs=P("kv", "dup", None),
        check_vma=False,
    )
```

```python
import functools
import math

import jax
import jax.numpy as jnp
from jax import lax
from jax.experimental import pallas as pl
from jax.experimental.pallas import tpu as pltpu
from jax.sharding import PartitionSpec as P

DRAFT = 4
CHUNK = 16
RING = 6
AHEAD = 2
LAG = 2
FINAL_LAG = 8
EARLY_FINALS = 4
PV_LAG = 2
ROWS = 8
OWN, FAR, SIB, FAR_SIB = range(4)
MESH = pl.DeviceIdType.MESH
LOWEST = -3.0e38
FLOOR = -2.0e38


def kernel(
    num_chunks,
    scale,
    len_ref,
    q_hbm,
    k_hbm,
    v_hbm,
    out_buf,
    kbuf,
    vbuf,
    qbuf,
    sbuf,
    pbuf,
    ebuf,
    keep,
    give,
    peer,
    stat,
    own_out,
    send_out,
    send_lse,
    recv_out,
    recv_lse,
    own_lse,
    k_sem,
    v_sem,
    q_local,
    q_chip_send,
    q_chip_recv,
    q_sib_send,
    q_sib_recv,
    q_fwd_send,
    q_fwd_recv,
    part_send,
    part_recv,
    o_send,
    o_recv,
    l_send,
    l_recv,
):
    me = lax.axis_index("dup")
    chip, core = me // 2, lax.rem(me, 2)
    sib = 2 * chip + (1 - core)
    far = 2 * (1 - chip) + core
    span = kbuf.shape[2]
    pairs = CHUNK // 2
    n = num_chunks

    def load_k(step, slot):
        return pltpu.make_async_copy(k_hbm.at[pl.ds(step * CHUNK, CHUNK)], kbuf.at[slot], k_sem.at[slot])

    def load_v(step, slot):
        return pltpu.make_async_copy(v_hbm.at[pl.ds(step * CHUNK, CHUNK)], vbuf.at[slot], v_sem.at[slot])

    def q_rows(step, role):
        return qbuf.at[role, pl.ds(step * CHUNK * ROWS, CHUNK * ROWS)]

    def q_mine(step):
        return q_rows(step, OWN)

    def remote(src, dst, send, recv, dev):
        return pltpu.make_async_remote_copy(
            src_ref=src, dst_ref=dst, send_sem=send, recv_sem=recv, device_id={"dup": dev}, device_id_type=MESH
        )

    def q_to_far(step):
        return remote(q_mine(step), q_rows(step, FAR), q_chip_send.at[step], q_chip_recv.at[step], far)

    q_to_sib = remote(qbuf.at[OWN], qbuf.at[SIB], q_sib_send.at[0], q_sib_recv.at[0], sib)

    def q_forward(step):
        return remote(q_rows(step, FAR), q_rows(step, FAR_SIB), q_fwd_send.at[step], q_fwd_recv.at[step], sib)

    def give_part(step):
        return remote(give.at[step], peer.at[step], part_send.at[step], part_recv.at[step], sib)

    def give_out(step):
        return remote(send_out.at[step], recv_out.at[step], o_send.at[step], o_recv.at[step], far)

    def give_lse(step):
        return remote(send_lse.at[step], recv_lse.at[step], l_send.at[step], l_recv.at[step], far)

    whole_q = pltpu.make_async_copy(q_hbm, qbuf.at[OWN], q_local.at[0])
    whole_q.start()
    load_k(0, 0).start()

    barrier = pltpu.get_barrier_semaphore()
    for dev in (sib, far):
        pl.semaphore_signal(barrier, inc=1, device_id={"dup": dev}, device_id_type=MESH)
    pl.semaphore_wait(barrier, 2)
    whole_q.wait()
    @pl.loop(0, n)
    def _(step):
        q_to_far(step).start()

    q_to_sib.start()
    load_v(0, 0).start()
    for step in range(1, RING):
        load_k(step, step).start()
        load_v(step, step).start()

    def forward_q(step):
        q_to_far(step).wait_recv()
        q_forward(step).start()

    def await_q(step):
        q_forward(step).wait_recv()

    lane = lax.broadcasted_iota(jnp.int32, (ROWS, 128), 1)
    draft_of_row = lax.rem(lax.broadcasted_iota(jnp.int32, (ROWS, span), 0), DRAFT)
    reach = lax.broadcasted_iota(jnp.int32, (ROWS, span), 1) - draft_of_row + (me * span + DRAFT)
    rate = scale / math.log(2.0)

    first = lax.rem(lax.broadcasted_iota(jnp.int32, (16, 128), 0), 16) < ROWS
    of_first = jnp.where(first, 1.0, 0.0).astype(jnp.bfloat16)
    of_second = jnp.where(first, 0.0, 1.0).astype(jnp.bfloat16)

    def score_pair(step, slot, i):
        start = pl.multiple_of(step * CHUNK * ROWS, 16) + 16 * i
        q = [qbuf[role, pl.ds(start, 16), :] for role in range(4)]
        left = jnp.concatenate([jnp.concatenate([x * of_first, x * of_second], 1) for x in q], 0)
        k_a, k_b = kbuf[slot, 2 * i], kbuf[slot, 2 * i + 1]
        turned = span // 2
        right = jnp.concatenate([k_a[:turned], k_b[:turned]], 1)
        scores = lax.dot_general(left, right, (((1,), (1,)), ((), ())), preferred_element_type=jnp.float32)
        rest = jnp.concatenate([k_a[turned:].T, k_b[turned:].T], 0)
        more = lax.dot_general(left, rest, (((1,), (0,)), ((), ())), preferred_element_type=jnp.float32)
        return jnp.concatenate([scores, more], 1)

    def mask_pair(step, i, scores):
        for h in range(2):
            allowed = reach <= len_ref[step * CHUNK + 2 * i + h]
            for d in range(4):
                row = 16 * d + 8 * h
                s = jnp.where(allowed, scores[row : row + 8], LOWEST)
                sbuf[i, pl.ds(row, 8), :] = s
                peak = jnp.maximum(jnp.max(s, axis=1, keepdims=True), FLOOR)
                pbuf[i, pl.ds(row, 8), :] = jnp.broadcast_to(peak, (ROWS, 128))

    def weigh_pair(i, peaks, masses):
        for d in range(4):
            probs = []
            for h in range(2):
                row = 16 * d + 8 * h
                peak = pbuf[i, pl.ds(row, 8), :]
                s = sbuf[i, pl.ds(row, 8), :]
                p = jnp.exp2((s - jnp.concatenate([peak] * (span // 128), 1)) * rate)
                mass = jnp.sum(p, axis=1, keepdims=True)
                here = lane == (CHUNK * d + 2 * i + h)
                peaks = jnp.where(here, peak, peaks)
                masses = jnp.where(here, mass, masses)
                probs.append(p)
            ebuf[i, pl.ds(16 * d, 16), :] = jnp.concatenate(probs, 0).astype(jnp.bfloat16)
        return peaks, masses

    def sum_pair(step, slot, i):
        v = jnp.concatenate([vbuf[slot, 2 * i], vbuf[slot, 2 * i + 1]], 1)
        o = lax.dot_general(ebuf[i], v, (((1,), (0,)), ((), ())), preferred_element_type=jnp.float32)
        for h in range(2):
            for d in range(4):
                home = keep if d in (OWN, FAR) else give
                home[step, CHUNK * (d % 2) + 2 * i + h] = o[16 * d + 8 * h : 16 * d + 8 * h + 8, 128 * h : 128 * h + 128]

    def merge_chip(step):
        m_a, l_a = stat[step, 0], stat[step, 1]
        m_b, l_b = (pltpu.roll(peer[step, 2 * CHUNK + j], 128 - SIB * CHUNK, 1) for j in range(2))
        top = jnp.maximum(m_a, m_b)
        w_a, w_b = jnp.exp2((m_a - top) * rate), jnp.exp2((m_b - top) * rate)
        total = w_a * l_a + w_b * l_b
        some = total > 0.0
        safe = jnp.where(some, total, 1.0)
        inverse = jnp.where(some, 1.0 / safe, 0.0)
        w_a, w_b = w_a * inverse, w_b * inverse
        lse = jnp.where(some, top * rate + jnp.log2(safe), LOWEST)
        own_lse[step] = lse
        send_lse[step] = pltpu.roll(lse, 128 - FAR * CHUNK, 1)

        def both(role, b):
            c = role * CHUNK + b
            return w_a[:, c : c + 1] * keep[step, c] + w_b[:, c : c + 1] * peer[step, c]

        for i in range(pairs):
            for b in (2 * i, 2 * i + 1):
                own_out[step, b] = both(OWN, b)
            far_out = [both(FAR, b) for b in (2 * i, 2 * i + 1)]
            send_out[step, pl.ds(16 * i, 16), :] = jnp.concatenate(far_out, 0).astype(jnp.bfloat16)

    def merge_final(step):
        rows = lax.rem(step, n) * CHUNK * ROWS
        mine, theirs = own_lse[step], recv_lse[step]
        top = jnp.maximum(mine, theirs)
        w_a, w_b = jnp.exp2(mine - top), jnp.exp2(theirs - top)
        inverse = 1.0 / (w_a + w_b)
        w_a, w_b = w_a * inverse, w_b * inverse
        for i in range(pairs):
            other = recv_out[step, pl.ds(16 * i, 16), :].astype(jnp.float32)
            outs = []
            for h in range(2):
                b = 2 * i + h
                outs.append(w_a[:, b : b + 1] * own_out[step, b] + w_b[:, b : b + 1] * other[8 * h : 8 * h + 8])
            out_buf[pl.ds(pl.multiple_of(rows + 16 * i, 16), 16), :] = jnp.concatenate(outs, 0).astype(jnp.bfloat16)

    def await_peer(step):
        give_part(step).wait_recv()

    def send_far(step):
        give_out(step).start()
        give_lse(step).start()

    def await_far(step):
        give_out(step).wait_recv()
        give_lse(step).wait_recv()

    def final_stage(step):
        await_far(step)
        merge_final(step)

    def attend(step, with_next):
        slot, next_slot = lax.rem(step, RING), lax.rem(step + 1, RING)
        peaks = jnp.zeros((ROWS, 128), jnp.float32)
        masses = jnp.zeros((ROWS, 128), jnp.float32)
        scores = [None] * pairs
        for i in range(pairs + PV_LAG):
            if i < pairs:
                peaks, masses = weigh_pair(i, peaks, masses)
                if with_next:
                    scores[i] = score_pair(step + 1, next_slot, i)
            if i >= PV_LAG:
                sum_pair(step, slot, i - PV_LAG)
            if with_next and 1 <= i <= pairs:
                mask_pair(step + 1, i - 1, scores[i - 1])
        stat[step, 0] = peaks
        stat[step, 1] = masses
        give[step, 2 * CHUNK] = peaks
        give[step, 2 * CHUNK + 1] = masses

    last = n - 1
    for step in range(AHEAD):
        forward_q(step)
    q_to_sib.wait_recv()
    await_q(0)
    load_k(0, 0).wait()
    for i in range(pairs):
        mask_pair(0, i, score_pair(0, 0, i))
    load_k(RING, 0).start()

    @pl.loop(0, last)
    def _(step):
        @pl.when(step + AHEAD < n)
        def _():
            forward_q(step + AHEAD)

        await_q(step + 1)
        load_k(step + 1, lax.rem(step + 1, RING)).wait()
        load_v(step, lax.rem(step, RING)).wait()

        @pl.when(step >= LAG)
        def _():
            await_peer(step - LAG)

        @pl.when(step >= FINAL_LAG)
        def _():
            await_far(step - FINAL_LAG)

        done = (step + n - FINAL_LAG) // n
        merge_final(done * (step - FINAL_LAG) + (1 - done) * n)
        ready = (step + n - LAG) // n
        merge_chip(ready * (step - LAG) + (1 - ready) * n)
        attend(step, True)
        give_part(step).start()

        @pl.when(step >= LAG)
        def _():
            send_far(step - LAG)

        @pl.when(step + 1 + RING < n)
        def _():
            load_k(step + 1 + RING, lax.rem(step + 1, RING)).start()

        @pl.when(step + RING < n)
        def _():
            load_v(step + RING, lax.rem(step, RING)).start()

    load_v(last, lax.rem(last, RING)).wait()
    await_peer(last - LAG)
    await_far(last - FINAL_LAG)
    merge_final(last - FINAL_LAG)
    merge_chip(last - LAG)
    attend(last, False)
    give_part(last).start()
    send_far(last - LAG)

    @pl.loop(last - LAG + 1, last)
    def _(step):
        await_peer(step)
        merge_chip(step)
        send_far(step)

    @pl.loop(last - FINAL_LAG + 1, last - FINAL_LAG + 1 + EARLY_FINALS)
    def _(step):
        final_stage(step)

    await_peer(last)
    merge_chip(last)
    send_far(last)

    @pl.loop(last - FINAL_LAG + 1 + EARLY_FINALS, n)
    def _(step):
        final_stage(step)

    q_to_sib.wait_send()

    @pl.loop(0, n)
    def _(step):
        q_to_far(step).wait_send()
        q_forward(step).wait_send()
        give_part(step).wait_send()
        give_out(step).wait_send()
        give_lse(step).wait_send()


def solution(mesh):
    def group_step(q_local, k_span, v_span, len_local):
        num_batch, span, dim = k_span.shape
        n = num_batch // CHUNK
        f32, bf16 = jnp.float32, jnp.bfloat16
        dma = lambda *shape: pltpu.SemaphoreType.DMA(shape)
        hbm = pl.BlockSpec(memory_space=pltpu.HBM)
        out = pl.pallas_call(
            functools.partial(kernel, n, dim**-0.5),
            out_shape=pltpu.VMEM((num_batch * ROWS, dim), bf16),
            in_specs=[pl.BlockSpec(memory_space=pltpu.SMEM), hbm, hbm, hbm],
            out_specs=pl.BlockSpec(memory_space=pltpu.VMEM),
            scratch_shapes=[
                pltpu.VMEM((RING, CHUNK, span, dim), bf16),
                pltpu.VMEM((RING, CHUNK, span, dim), bf16),
                pltpu.VMEM((4, num_batch * ROWS, dim), bf16),
                pltpu.VMEM((CHUNK // 2, 64, span), f32),
                pltpu.VMEM((CHUNK // 2, 64, 128), f32),
                pltpu.VMEM((CHUNK // 2, 64, span), bf16),
                pltpu.VMEM((n + 1, 2 * CHUNK, ROWS, dim), f32),
                pltpu.VMEM((n, 2 * CHUNK + 2, ROWS, dim), f32),
                pltpu.VMEM((n + 1, 2 * CHUNK + 2, ROWS, dim), f32),
                pltpu.VMEM((n + 1, 2, ROWS, dim), f32),
                pltpu.VMEM((n + 1, CHUNK, ROWS, dim), f32),
                pltpu.VMEM((n + 1, CHUNK * ROWS, dim), bf16),
                pltpu.VMEM((n + 1, ROWS, dim), f32),
                pltpu.VMEM((n + 1, CHUNK * ROWS, dim), bf16),
                pltpu.VMEM((n + 1, ROWS, dim), f32),
                pltpu.VMEM((n + 1, ROWS, dim), f32),
                dma(RING),
                dma(RING),
                dma(1),
            ]
            + [dma(n)] * 12,
            compiler_params=pltpu.CompilerParams(
                collective_id=0, has_side_effects=True, vmem_limit_bytes=56 * 1024 * 1024
            ),
        )(len_local, q_local.reshape(num_batch * ROWS, dim), k_span, v_span)
        return out.reshape(num_batch, ROWS, dim)

    return jax.shard_map(
        group_step,
        mesh=mesh,
        in_specs=(P("kv", "dup", None), P("kv", "dup", None), P("kv", "dup", None), P("kv")),
        out_specs=P("kv", "dup", None),
        check_vma=False,
    )
```

```python
import functools
import math

import jax
import jax.numpy as jnp
from jax import lax
from jax.experimental import pallas as pl
from jax.experimental.pallas import tpu as pltpu
from jax.sharding import PartitionSpec as P

DRAFT = 4
CHUNK = 16
RING = 6
AHEAD = 2
LAG = 2
FINAL_LAG = 8
EARLY_FINALS = 4
PV_LAG = 2
ROWS = 8
OWN, FAR, SIB, FAR_SIB = range(4)
MESH = pl.DeviceIdType.MESH
LOWEST = -3.0e38
FLOOR = -2.0e38


def kernel(
    num_chunks,
    scale,
    len_ref,
    q_hbm,
    k_hbm,
    v_hbm,
    out_buf,
    kbuf,
    vbuf,
    qbuf,
    sbuf,
    pbuf,
    ebuf,
    keep,
    give,
    peer,
    stat,
    own_out,
    send_out,
    send_lse,
    recv_out,
    recv_lse,
    own_lse,
    k_sem,
    v_sem,
    q_local,
    q_chip_send,
    q_chip_recv,
    q_sib_send,
    q_sib_recv,
    q_fwd_send,
    q_fwd_recv,
    part_send,
    part_recv,
    o_send,
    o_recv,
    l_send,
    l_recv,
):
    me = lax.axis_index("dup")
    chip, core = me // 2, lax.rem(me, 2)
    sib = 2 * chip + (1 - core)
    far = 2 * (1 - chip) + core
    span = kbuf.shape[2]
    pairs = CHUNK // 2
    n = num_chunks

    def load_k(step, slot):
        return pltpu.make_async_copy(k_hbm.at[pl.ds(step * CHUNK, CHUNK)], kbuf.at[slot], k_sem.at[slot])

    def load_v(step, slot):
        return pltpu.make_async_copy(v_hbm.at[pl.ds(step * CHUNK, CHUNK)], vbuf.at[slot], v_sem.at[slot])

    def q_rows(step, role):
        return qbuf.at[role, pl.ds(step * CHUNK * ROWS, CHUNK * ROWS)]

    def q_mine(step):
        return q_rows(step, OWN)

    def remote(src, dst, send, recv, dev):
        return pltpu.make_async_remote_copy(
            src_ref=src, dst_ref=dst, send_sem=send, recv_sem=recv, device_id={"dup": dev}, device_id_type=MESH
        )

    def q_to_far(step):
        return remote(q_mine(step), q_rows(step, FAR), q_chip_send.at[step], q_chip_recv.at[step], far)

    q_to_sib = remote(qbuf.at[OWN], qbuf.at[SIB], q_sib_send.at[0], q_sib_recv.at[0], sib)

    def q_forward(step):
        return remote(q_rows(step, FAR), q_rows(step, FAR_SIB), q_fwd_send.at[step], q_fwd_recv.at[step], sib)

    def give_part(step):
        return remote(give.at[step], peer.at[step], part_send.at[step], part_recv.at[step], sib)

    def give_out(step):
        return remote(send_out.at[step], recv_out.at[step], o_send.at[step], o_recv.at[step], far)

    def give_lse(step):
        return remote(send_lse.at[step], recv_lse.at[step], l_send.at[step], l_recv.at[step], far)

    whole_q = pltpu.make_async_copy(q_hbm, qbuf.at[OWN], q_local.at[0])
    whole_q.start()
    load_k(0, 0).start()

    barrier = pltpu.get_barrier_semaphore()
    for dev in (sib, far):
        pl.semaphore_signal(barrier, inc=1, device_id={"dup": dev}, device_id_type=MESH)
    pl.semaphore_wait(barrier, 2)
    whole_q.wait()
    for step in range(4):
        q_to_far(step).start()
    q_to_sib.start()
    load_v(0, 0).start()
    for step in range(1, RING):
        load_k(step, step).start()
        load_v(step, step).start()

    def forward_q(step):
        q_to_far(step).wait_recv()
        q_forward(step).start()

    def await_q(step):
        q_forward(step).wait_recv()

    lane = lax.broadcasted_iota(jnp.int32, (ROWS, 128), 1)
    draft_of_row = lax.rem(lax.broadcasted_iota(jnp.int32, (ROWS, span), 0), DRAFT)
    reach = lax.broadcasted_iota(jnp.int32, (ROWS, span), 1) - draft_of_row + (me * span + DRAFT)
    rate = scale / math.log(2.0)

    first = lax.rem(lax.broadcasted_iota(jnp.int32, (16, 128), 0), 16) < ROWS
    of_first = jnp.where(first, 1.0, 0.0).astype(jnp.bfloat16)
    of_second = jnp.where(first, 0.0, 1.0).astype(jnp.bfloat16)

    def score_pair(step, slot, i):
        start = pl.multiple_of(step * CHUNK * ROWS, 16) + 16 * i
        q = [qbuf[role, pl.ds(start, 16), :] for role in range(4)]
        left = jnp.concatenate([jnp.concatenate([x * of_first, x * of_second], 1) for x in q], 0)
        k_a, k_b = kbuf[slot, 2 * i], kbuf[slot, 2 * i + 1]
        turned = span // 2
        right = jnp.concatenate([k_a[:turned], k_b[:turned]], 1)
        scores = lax.dot_general(left, right, (((1,), (1,)), ((), ())), preferred_element_type=jnp.float32)
        rest = jnp.concatenate([k_a[turned:].T, k_b[turned:].T], 0)
        more = lax.dot_general(left, rest, (((1,), (0,)), ((), ())), preferred_element_type=jnp.float32)
        return jnp.concatenate([scores, more], 1)

    def mask_pair(step, i, scores):
        for h in range(2):
            allowed = reach <= len_ref[step * CHUNK + 2 * i + h]
            for d in range(4):
                row = 16 * d + 8 * h
                s = jnp.where(allowed, scores[row : row + 8], LOWEST)
                sbuf[i, pl.ds(row, 8), :] = s
                peak = jnp.maximum(jnp.max(s, axis=1, keepdims=True), FLOOR)
                pbuf[i, pl.ds(row, 8), :] = jnp.broadcast_to(peak, (ROWS, 128))

    def weigh_pair(i, peaks, masses):
        for d in range(4):
            probs = []
            for h in range(2):
                row = 16 * d + 8 * h
                peak = pbuf[i, pl.ds(row, 8), :]
                s = sbuf[i, pl.ds(row, 8), :]
                p = jnp.exp2((s - jnp.concatenate([peak] * (span // 128), 1)) * rate)
                mass = jnp.sum(p, axis=1, keepdims=True)
                here = lane == (CHUNK * d + 2 * i + h)
                peaks = jnp.where(here, peak, peaks)
                masses = jnp.where(here, mass, masses)
                probs.append(p)
            ebuf[i, pl.ds(16 * d, 16), :] = jnp.concatenate(probs, 0).astype(jnp.bfloat16)
        return peaks, masses

    def sum_pair(step, slot, i):
        v = jnp.concatenate([vbuf[slot, 2 * i], vbuf[slot, 2 * i + 1]], 1)
        o = lax.dot_general(ebuf[i], v, (((1,), (0,)), ((), ())), preferred_element_type=jnp.float32)
        for h in range(2):
            for d in range(4):
                home = keep if d in (OWN, FAR) else give
                home[step, CHUNK * (d % 2) + 2 * i + h] = o[16 * d + 8 * h : 16 * d + 8 * h + 8, 128 * h : 128 * h + 128]

    def merge_chip(step):
        m_a, l_a = stat[step, 0], stat[step, 1]
        m_b, l_b = (pltpu.roll(peer[step, 2 * CHUNK + j], 128 - SIB * CHUNK, 1) for j in range(2))
        top = jnp.maximum(m_a, m_b)
        w_a, w_b = jnp.exp2((m_a - top) * rate), jnp.exp2((m_b - top) * rate)
        total = w_a * l_a + w_b * l_b
        some = total > 0.0
        safe = jnp.where(some, total, 1.0)
        inverse = jnp.where(some, 1.0 / safe, 0.0)
        w_a, w_b = w_a * inverse, w_b * inverse
        lse = jnp.where(some, top * rate + jnp.log2(safe), LOWEST)
        own_lse[step] = lse
        send_lse[step] = pltpu.roll(lse, 128 - FAR * CHUNK, 1)

        def both(role, b):
            c = role * CHUNK + b
            return w_a[:, c : c + 1] * keep[step, c] + w_b[:, c : c + 1] * peer[step, c]

        for i in range(pairs):
            for b in (2 * i, 2 * i + 1):
                own_out[step, b] = both(OWN, b)
            far_out = [both(FAR, b) for b in (2 * i, 2 * i + 1)]
            send_out[step, pl.ds(16 * i, 16), :] = jnp.concatenate(far_out, 0).astype(jnp.bfloat16)

    def merge_final(step):
        rows = lax.rem(step, n) * CHUNK * ROWS
        mine, theirs = own_lse[step], recv_lse[step]
        top = jnp.maximum(mine, theirs)
        w_a, w_b = jnp.exp2(mine - top), jnp.exp2(theirs - top)
        inverse = 1.0 / (w_a + w_b)
        w_a, w_b = w_a * inverse, w_b * inverse
        for i in range(pairs):
            other = recv_out[step, pl.ds(16 * i, 16), :].astype(jnp.float32)
            outs = []
            for h in range(2):
                b = 2 * i + h
                outs.append(w_a[:, b : b + 1] * own_out[step, b] + w_b[:, b : b + 1] * other[8 * h : 8 * h + 8])
            out_buf[pl.ds(pl.multiple_of(rows + 16 * i, 16), 16), :] = jnp.concatenate(outs, 0).astype(jnp.bfloat16)

    def await_peer(step):
        give_part(step).wait_recv()

    def send_far(step):
        give_out(step).start()
        give_lse(step).start()

    def await_far(step):
        give_out(step).wait_recv()
        give_lse(step).wait_recv()

    def final_stage(step):
        await_far(step)
        merge_final(step)

    def attend(step, with_next):
        slot, next_slot = lax.rem(step, RING), lax.rem(step + 1, RING)
        peaks = jnp.zeros((ROWS, 128), jnp.float32)
        masses = jnp.zeros((ROWS, 128), jnp.float32)
        scores = [None] * pairs
        for i in range(pairs + PV_LAG):
            if i < pairs:
                peaks, masses = weigh_pair(i, peaks, masses)
                if with_next:
                    scores[i] = score_pair(step + 1, next_slot, i)
            if i >= PV_LAG:
                sum_pair(step, slot, i - PV_LAG)
            if with_next and 1 <= i <= pairs:
                mask_pair(step + 1, i - 1, scores[i - 1])
        stat[step, 0] = peaks
        stat[step, 1] = masses
        give[step, 2 * CHUNK] = peaks
        give[step, 2 * CHUNK + 1] = masses

    last = n - 1
    for step in range(AHEAD):
        forward_q(step)
        q_to_far(2 * step + 4).start()
        q_to_far(2 * step + 5).start()
    q_to_sib.wait_recv()
    await_q(0)
    load_k(0, 0).wait()
    for i in range(pairs):
        mask_pair(0, i, score_pair(0, 0, i))
    load_k(RING, 0).start()

    @pl.loop(0, last)
    def _(step):
        @pl.when(2 * step + 2 * AHEAD + 4 < n)
        def _():
            q_to_far(2 * step + 2 * AHEAD + 4).start()
            q_to_far(2 * step + 2 * AHEAD + 5).start()

        @pl.when(step + AHEAD < n)
        def _():
            forward_q(step + AHEAD)

        await_q(step + 1)
        load_k(step + 1, lax.rem(step + 1, RING)).wait()
        load_v(step, lax.rem(step, RING)).wait()

        @pl.when(step >= LAG)
        def _():
            await_peer(step - LAG)

        @pl.when(step >= FINAL_LAG)
        def _():
            await_far(step - FINAL_LAG)

        done = (step + n - FINAL_LAG) // n
        merge_final(done * (step - FINAL_LAG) + (1 - done) * n)
        ready = (step + n - LAG) // n
        merge_chip(ready * (step - LAG) + (1 - ready) * n)
        attend(step, True)
        give_part(step).start()

        @pl.when(step >= LAG)
        def _():
            send_far(step - LAG)

        @pl.when(step + 1 + RING < n)
        def _():
            load_k(step + 1 + RING, lax.rem(step + 1, RING)).start()

        @pl.when(step + RING < n)
        def _():
            load_v(step + RING, lax.rem(step, RING)).start()

    load_v(last, lax.rem(last, RING)).wait()
    await_peer(last - LAG)
    await_far(last - FINAL_LAG)
    merge_final(last - FINAL_LAG)
    merge_chip(last - LAG)
    attend(last, False)
    give_part(last).start()
    send_far(last - LAG)

    @pl.loop(last - LAG + 1, last)
    def _(step):
        await_peer(step)
        merge_chip(step)
        send_far(step)

    @pl.loop(last - FINAL_LAG + 1, last - FINAL_LAG + 1 + EARLY_FINALS)
    def _(step):
        final_stage(step)

    await_peer(last)
    merge_chip(last)
    send_far(last)

    @pl.loop(last - FINAL_LAG + 1 + EARLY_FINALS, n)
    def _(step):
        final_stage(step)

    q_to_sib.wait_send()

    @pl.loop(0, n)
    def _(step):
        q_to_far(step).wait_send()
        q_forward(step).wait_send()
        give_part(step).wait_send()
        give_out(step).wait_send()
        give_lse(step).wait_send()


def solution(mesh):
    def group_step(q_local, k_span, v_span, len_local):
        num_batch, span, dim = k_span.shape
        n = num_batch // CHUNK
        f32, bf16 = jnp.float32, jnp.bfloat16
        dma = lambda *shape: pltpu.SemaphoreType.DMA(shape)
        hbm = pl.BlockSpec(memory_space=pltpu.HBM)
        out = pl.pallas_call(
            functools.partial(kernel, n, dim**-0.5),
            out_shape=pltpu.VMEM((num_batch * ROWS, dim), bf16),
            in_specs=[pl.BlockSpec(memory_space=pltpu.SMEM), hbm, hbm, hbm],
            out_specs=pl.BlockSpec(memory_space=pltpu.VMEM),
            scratch_shapes=[
                pltpu.VMEM((RING, CHUNK, span, dim), bf16),
                pltpu.VMEM((RING, CHUNK, span, dim), bf16),
                pltpu.VMEM((4, num_batch * ROWS, dim), bf16),
                pltpu.VMEM((CHUNK // 2, 64, span), f32),
                pltpu.VMEM((CHUNK // 2, 64, 128), f32),
                pltpu.VMEM((CHUNK // 2, 64, span), bf16),
                pltpu.VMEM((n + 1, 2 * CHUNK, ROWS, dim), f32),
                pltpu.VMEM((n, 2 * CHUNK + 2, ROWS, dim), f32),
                pltpu.VMEM((n + 1, 2 * CHUNK + 2, ROWS, dim), f32),
                pltpu.VMEM((n + 1, 2, ROWS, dim), f32),
                pltpu.VMEM((n + 1, CHUNK, ROWS, dim), f32),
                pltpu.VMEM((n + 1, CHUNK * ROWS, dim), bf16),
                pltpu.VMEM((n + 1, ROWS, dim), f32),
                pltpu.VMEM((n + 1, CHUNK * ROWS, dim), bf16),
                pltpu.VMEM((n + 1, ROWS, dim), f32),
                pltpu.VMEM((n + 1, ROWS, dim), f32),
                dma(RING),
                dma(RING),
                dma(1),
            ]
            + [dma(n)] * 12,
            compiler_params=pltpu.CompilerParams(
                collective_id=0, has_side_effects=True, vmem_limit_bytes=56 * 1024 * 1024
            ),
        )(len_local, q_local.reshape(num_batch * ROWS, dim), k_span, v_span)
        return out.reshape(num_batch, ROWS, dim)

    return jax.shard_map(
        group_step,
        mesh=mesh,
        in_specs=(P("kv", "dup", None), P("kv", "dup", None), P("kv", "dup", None), P("kv")),
        out_specs=P("kv", "dup", None),
        check_vma=False,
    )
```

```python
import functools
import math

import jax
import jax.numpy as jnp
from jax import lax
from jax.experimental import pallas as pl
from jax.experimental.pallas import tpu as pltpu
from jax.sharding import PartitionSpec as P

DRAFT = 4
CHUNK = 16
RING = 6
AHEAD = 2
LAG = 2
FINAL_LAG = 8
EARLY_FINALS = 4
PV_LAG = 2
ROWS = 8
OWN, FAR, SIB, FAR_SIB = range(4)
MESH = pl.DeviceIdType.MESH
LOWEST = -3.0e38
FLOOR = -2.0e38


def kernel(
    num_chunks,
    scale,
    len_ref,
    q_hbm,
    k_hbm,
    v_hbm,
    out_buf,
    kbuf,
    vbuf,
    qbuf,
    sbuf,
    pbuf,
    ebuf,
    keep,
    give,
    peer,
    stat,
    own_out,
    send_out,
    send_lse,
    recv_out,
    recv_lse,
    own_lse,
    k_sem,
    v_sem,
    q_local,
    q_chip_send,
    q_chip_recv,
    q_sib_send,
    q_sib_recv,
    q_fwd_send,
    q_fwd_recv,
    part_send,
    part_recv,
    o_send,
    o_recv,
    l_send,
    l_recv,
):
    me = lax.axis_index("dup")
    chip, core = me // 2, lax.rem(me, 2)
    sib = 2 * chip + (1 - core)
    far = 2 * (1 - chip) + core
    span = kbuf.shape[2]
    pairs = CHUNK // 2
    n = num_chunks

    def load_k(step, slot):
        return pltpu.make_async_copy(k_hbm.at[pl.ds(step * CHUNK, CHUNK)], kbuf.at[slot], k_sem.at[slot])

    def load_v(step, slot):
        return pltpu.make_async_copy(v_hbm.at[pl.ds(step * CHUNK, CHUNK)], vbuf.at[slot], v_sem.at[slot])

    def q_rows(step, role):
        return qbuf.at[role, pl.ds(step * CHUNK * ROWS, CHUNK * ROWS)]

    def q_mine(step):
        return q_rows(step, OWN)

    def remote(src, dst, send, recv, dev):
        return pltpu.make_async_remote_copy(
            src_ref=src, dst_ref=dst, send_sem=send, recv_sem=recv, device_id={"dup": dev}, device_id_type=MESH
        )

    def q_to_far(step):
        return remote(q_mine(step), q_rows(step, FAR), q_chip_send.at[step], q_chip_recv.at[step], far)

    q_to_sib = remote(qbuf.at[OWN], qbuf.at[SIB], q_sib_send.at[0], q_sib_recv.at[0], sib)

    def q_forward(step):
        return remote(q_rows(step, FAR), q_rows(step, FAR_SIB), q_fwd_send.at[step], q_fwd_recv.at[step], sib)

    def give_part(step):
        return remote(give.at[step], peer.at[step], part_send.at[step], part_recv.at[step], sib)

    def give_out(step):
        return remote(send_out.at[step], recv_out.at[step], o_send.at[step], o_recv.at[step], far)

    def give_lse(step):
        return remote(send_lse.at[step], recv_lse.at[step], l_send.at[step], l_recv.at[step], far)

    whole_q = pltpu.make_async_copy(q_hbm, qbuf.at[OWN], q_local.at[0])
    whole_q.start()
    load_k(0, 0).start()

    barrier = pltpu.get_barrier_semaphore()
    for dev in (sib, far):
        pl.semaphore_signal(barrier, inc=1, device_id={"dup": dev}, device_id_type=MESH)
    pl.semaphore_wait(barrier, 2)
    whole_q.wait()
    for step in range(2):
        q_to_far(step).start()
    q_to_sib.start()
    load_v(0, 0).start()
    for step in range(1, RING):
        load_k(step, step).start()
        load_v(step, step).start()

    def forward_q(step):
        q_to_far(step).wait_recv()
        q_forward(step).start()

    def await_q(step):
        q_forward(step).wait_recv()

    lane = lax.broadcasted_iota(jnp.int32, (ROWS, 128), 1)
    draft_of_row = lax.rem(lax.broadcasted_iota(jnp.int32, (ROWS, span), 0), DRAFT)
    reach = lax.broadcasted_iota(jnp.int32, (ROWS, span), 1) - draft_of_row + (me * span + DRAFT)
    rate = scale / math.log(2.0)

    first = lax.rem(lax.broadcasted_iota(jnp.int32, (16, 128), 0), 16) < ROWS
    of_first = jnp.where(first, 1.0, 0.0).astype(jnp.bfloat16)
    of_second = jnp.where(first, 0.0, 1.0).astype(jnp.bfloat16)

    def score_pair(step, slot, i):
        start = pl.multiple_of(step * CHUNK * ROWS, 16) + 16 * i
        q = [qbuf[role, pl.ds(start, 16), :] for role in range(4)]
        left = jnp.concatenate([jnp.concatenate([x * of_first, x * of_second], 1) for x in q], 0)
        k_a, k_b = kbuf[slot, 2 * i], kbuf[slot, 2 * i + 1]
        turned = span // 2
        right = jnp.concatenate([k_a[:turned], k_b[:turned]], 1)
        scores = lax.dot_general(left, right, (((1,), (1,)), ((), ())), preferred_element_type=jnp.float32)
        rest = jnp.concatenate([k_a[turned:].T, k_b[turned:].T], 0)
        more = lax.dot_general(left, rest, (((1,), (0,)), ((), ())), preferred_element_type=jnp.float32)
        return jnp.concatenate([scores, more], 1)

    def mask_pair(step, i, scores):
        for h in range(2):
            allowed = reach <= len_ref[step * CHUNK + 2 * i + h]
            for d in range(4):
                row = 16 * d + 8 * h
                s = jnp.where(allowed, scores[row : row + 8], LOWEST)
                sbuf[i, pl.ds(row, 8), :] = s
                peak = jnp.maximum(jnp.max(s, axis=1, keepdims=True), FLOOR)
                pbuf[i, pl.ds(row, 8), :] = jnp.broadcast_to(peak, (ROWS, 128))

    def weigh_pair(i, peaks, masses):
        for d in range(4):
            probs = []
            for h in range(2):
                row = 16 * d + 8 * h
                peak = pbuf[i, pl.ds(row, 8), :]
                s = sbuf[i, pl.ds(row, 8), :]
                p = jnp.exp2((s - jnp.concatenate([peak] * (span // 128), 1)) * rate)
                mass = jnp.sum(p, axis=1, keepdims=True)
                here = lane == (CHUNK * d + 2 * i + h)
                peaks = jnp.where(here, peak, peaks)
                masses = jnp.where(here, mass, masses)
                probs.append(p)
            ebuf[i, pl.ds(16 * d, 16), :] = jnp.concatenate(probs, 0).astype(jnp.bfloat16)
        return peaks, masses

    def sum_pair(step, slot, i):
        v = jnp.concatenate([vbuf[slot, 2 * i], vbuf[slot, 2 * i + 1]], 1)
        o = lax.dot_general(ebuf[i], v, (((1,), (0,)), ((), ())), preferred_element_type=jnp.float32)
        for h in range(2):
            for d in range(4):
                home = keep if d in (OWN, FAR) else give
                home[step, CHUNK * (d % 2) + 2 * i + h] = o[16 * d + 8 * h : 16 * d + 8 * h + 8, 128 * h : 128 * h + 128]

    def merge_chip(step):
        m_a, l_a = stat[step, 0], stat[step, 1]
        m_b, l_b = (pltpu.roll(peer[step, 2 * CHUNK + j], 128 - SIB * CHUNK, 1) for j in range(2))
        top = jnp.maximum(m_a, m_b)
        w_a, w_b = jnp.exp2((m_a - top) * rate), jnp.exp2((m_b - top) * rate)
        total = w_a * l_a + w_b * l_b
        some = total > 0.0
        safe = jnp.where(some, total, 1.0)
        inverse = jnp.where(some, 1.0 / safe, 0.0)
        w_a, w_b = w_a * inverse, w_b * inverse
        lse = jnp.where(some, top * rate + jnp.log2(safe), LOWEST)
        own_lse[step] = lse
        send_lse[step] = pltpu.roll(lse, 128 - FAR * CHUNK, 1)

        def both(role, b):
            c = role * CHUNK + b
            return w_a[:, c : c + 1] * keep[step, c] + w_b[:, c : c + 1] * peer[step, c]

        for i in range(pairs):
            for b in (2 * i, 2 * i + 1):
                own_out[step, b] = both(OWN, b)
            far_out = [both(FAR, b) for b in (2 * i, 2 * i + 1)]
            send_out[step, pl.ds(16 * i, 16), :] = jnp.concatenate(far_out, 0).astype(jnp.bfloat16)

    def merge_final(step):
        rows = lax.rem(step, n) * CHUNK * ROWS
        mine, theirs = own_lse[step], recv_lse[step]
        top = jnp.maximum(mine, theirs)
        w_a, w_b = jnp.exp2(mine - top), jnp.exp2(theirs - top)
        inverse = 1.0 / (w_a + w_b)
        w_a, w_b = w_a * inverse, w_b * inverse
        for i in range(pairs):
            other = recv_out[step, pl.ds(16 * i, 16), :].astype(jnp.float32)
            outs = []
            for h in range(2):
                b = 2 * i + h
                outs.append(w_a[:, b : b + 1] * own_out[step, b] + w_b[:, b : b + 1] * other[8 * h : 8 * h + 8])
            out_buf[pl.ds(pl.multiple_of(rows + 16 * i, 16), 16), :] = jnp.concatenate(outs, 0).astype(jnp.bfloat16)

    def await_peer(step):
        give_part(step).wait_recv()

    def send_far(step):
        give_out(step).start()
        give_lse(step).start()

    def await_far(step):
        give_out(step).wait_recv()
        give_lse(step).wait_recv()

    def final_stage(step):
        await_far(step)
        merge_final(step)

    def attend(step, with_next):
        slot, next_slot = lax.rem(step, RING), lax.rem(step + 1, RING)
        peaks = jnp.zeros((ROWS, 128), jnp.float32)
        masses = jnp.zeros((ROWS, 128), jnp.float32)
        scores = [None] * pairs
        for i in range(pairs + PV_LAG):
            if i < pairs:
                peaks, masses = weigh_pair(i, peaks, masses)
                if with_next:
                    scores[i] = score_pair(step + 1, next_slot, i)
            if i >= PV_LAG:
                sum_pair(step, slot, i - PV_LAG)
            if with_next and 1 <= i <= pairs:
                mask_pair(step + 1, i - 1, scores[i - 1])
        stat[step, 0] = peaks
        stat[step, 1] = masses
        give[step, 2 * CHUNK] = peaks
        give[step, 2 * CHUNK + 1] = masses

    last = n - 1
    for step in range(AHEAD):
        q_to_far(step).wait_send()
        q_to_far(step + 2).start()
        forward_q(step)
    for step in range(4, 4 + 2 * AHEAD):
        q_to_far(step).start()
    q_to_sib.wait_recv()
    await_q(0)
    load_k(0, 0).wait()
    for i in range(pairs):
        mask_pair(0, i, score_pair(0, 0, i))
    load_k(RING, 0).start()

    @pl.loop(0, last)
    def _(step):
        @pl.when(2 * step + 2 * AHEAD + 4 < n)
        def _():
            q_to_far(2 * step + 2 * AHEAD + 4).start()
            q_to_far(2 * step + 2 * AHEAD + 5).start()

        @pl.when(step + AHEAD < n)
        def _():
            forward_q(step + AHEAD)

        await_q(step + 1)
        load_k(step + 1, lax.rem(step + 1, RING)).wait()
        load_v(step, lax.rem(step, RING)).wait()

        @pl.when(step >= LAG)
        def _():
            await_peer(step - LAG)

        @pl.when(step >= FINAL_LAG)
        def _():
            await_far(step - FINAL_LAG)

        done = (step + n - FINAL_LAG) // n
        merge_final(done * (step - FINAL_LAG) + (1 - done) * n)
        ready = (step + n - LAG) // n
        merge_chip(ready * (step - LAG) + (1 - ready) * n)
        attend(step, True)
        give_part(step).start()

        @pl.when(step >= LAG)
        def _():
            send_far(step - LAG)

        @pl.when(step + 1 + RING < n)
        def _():
            load_k(step + 1 + RING, lax.rem(step + 1, RING)).start()

        @pl.when(step + RING < n)
        def _():
            load_v(step + RING, lax.rem(step, RING)).start()

    load_v(last, lax.rem(last, RING)).wait()
    await_peer(last - LAG)
    await_far(last - FINAL_LAG)
    merge_final(last - FINAL_LAG)
    merge_chip(last - LAG)
    attend(last, False)
    give_part(last).start()
    send_far(last - LAG)

    @pl.loop(last - LAG + 1, last)
    def _(step):
        await_peer(step)
        merge_chip(step)
        send_far(step)

    @pl.loop(last - FINAL_LAG + 1, last - FINAL_LAG + 1 + EARLY_FINALS)
    def _(step):
        final_stage(step)

    await_peer(last)
    merge_chip(last)
    send_far(last)

    @pl.loop(last - FINAL_LAG + 1 + EARLY_FINALS, n)
    def _(step):
        final_stage(step)

    q_to_sib.wait_send()

    @pl.loop(AHEAD, n)
    def _(step):
        q_to_far(step).wait_send()

    @pl.loop(0, n)
    def _(step):
        q_forward(step).wait_send()
        give_part(step).wait_send()
        give_out(step).wait_send()
        give_lse(step).wait_send()


def solution(mesh):
    def group_step(q_local, k_span, v_span, len_local):
        num_batch, span, dim = k_span.shape
        n = num_batch // CHUNK
        f32, bf16 = jnp.float32, jnp.bfloat16
        dma = lambda *shape: pltpu.SemaphoreType.DMA(shape)
        hbm = pl.BlockSpec(memory_space=pltpu.HBM)
        out = pl.pallas_call(
            functools.partial(kernel, n, dim**-0.5),
            out_shape=pltpu.VMEM((num_batch * ROWS, dim), bf16),
            in_specs=[pl.BlockSpec(memory_space=pltpu.SMEM), hbm, hbm, hbm],
            out_specs=pl.BlockSpec(memory_space=pltpu.VMEM),
            scratch_shapes=[
                pltpu.VMEM((RING, CHUNK, span, dim), bf16),
                pltpu.VMEM((RING, CHUNK, span, dim), bf16),
                pltpu.VMEM((4, num_batch * ROWS, dim), bf16),
                pltpu.VMEM((CHUNK // 2, 64, span), f32),
                pltpu.VMEM((CHUNK // 2, 64, 128), f32),
                pltpu.VMEM((CHUNK // 2, 64, span), bf16),
                pltpu.VMEM((n + 1, 2 * CHUNK, ROWS, dim), f32),
                pltpu.VMEM((n, 2 * CHUNK + 2, ROWS, dim), f32),
                pltpu.VMEM((n + 1, 2 * CHUNK + 2, ROWS, dim), f32),
                pltpu.VMEM((n + 1, 2, ROWS, dim), f32),
                pltpu.VMEM((n + 1, CHUNK, ROWS, dim), f32),
                pltpu.VMEM((n + 1, CHUNK * ROWS, dim), bf16),
                pltpu.VMEM((n + 1, ROWS, dim), f32),
                pltpu.VMEM((n + 1, CHUNK * ROWS, dim), bf16),
                pltpu.VMEM((n + 1, ROWS, dim), f32),
                pltpu.VMEM((n + 1, ROWS, dim), f32),
                dma(RING),
                dma(RING),
                dma(1),
            ]
            + [dma(n)] * 12,
            compiler_params=pltpu.CompilerParams(
                collective_id=0, has_side_effects=True, vmem_limit_bytes=56 * 1024 * 1024
            ),
        )(len_local, q_local.reshape(num_batch * ROWS, dim), k_span, v_span)
        return out.reshape(num_batch, ROWS, dim)

    return jax.shard_map(
        group_step,
        mesh=mesh,
        in_specs=(P("kv", "dup", None), P("kv", "dup", None), P("kv", "dup", None), P("kv")),
        out_specs=P("kv", "dup", None),
        check_vma=False,
    )
```

```python
import functools
import math

import jax
import jax.numpy as jnp
from jax import lax
from jax.experimental import pallas as pl
from jax.experimental.pallas import tpu as pltpu
from jax.sharding import PartitionSpec as P

DRAFT = 4
CHUNK = 16
RING = 6
AHEAD = 2
LAG = 2
FINAL_LAG = 8
EARLY_FINALS = 4
PV_LAG = 3
ROWS = 8
OWN, FAR, SIB, FAR_SIB = range(4)
MESH = pl.DeviceIdType.MESH
LOWEST = -3.0e38
FLOOR = -2.0e38


def kernel(
    num_chunks,
    scale,
    len_ref,
    q_hbm,
    k_hbm,
    v_hbm,
    out_buf,
    kbuf,
    vbuf,
    qbuf,
    sbuf,
    pbuf,
    ebuf,
    keep,
    give,
    peer,
    stat,
    own_out,
    send_out,
    send_lse,
    recv_out,
    recv_lse,
    own_lse,
    k_sem,
    v_sem,
    q_local,
    q_chip_send,
    q_chip_recv,
    q_sib_send,
    q_sib_recv,
    q_fwd_send,
    q_fwd_recv,
    part_send,
    part_recv,
    o_send,
    o_recv,
    l_send,
    l_recv,
):
    me = lax.axis_index("dup")
    chip, core = me // 2, lax.rem(me, 2)
    sib = 2 * chip + (1 - core)
    far = 2 * (1 - chip) + core
    span = kbuf.shape[2]
    pairs = CHUNK // 2
    n = num_chunks

    def load_k(step, slot):
        return pltpu.make_async_copy(k_hbm.at[pl.ds(step * CHUNK, CHUNK)], kbuf.at[slot], k_sem.at[slot])

    def load_v(step, slot):
        return pltpu.make_async_copy(v_hbm.at[pl.ds(step * CHUNK, CHUNK)], vbuf.at[slot], v_sem.at[slot])

    def q_rows(step, role):
        return qbuf.at[role, pl.ds(step * CHUNK * ROWS, CHUNK * ROWS)]

    def q_mine(step):
        return q_rows(step, OWN)

    def remote(src, dst, send, recv, dev):
        return pltpu.make_async_remote_copy(
            src_ref=src, dst_ref=dst, send_sem=send, recv_sem=recv, device_id={"dup": dev}, device_id_type=MESH
        )

    def q_to_far(step):
        return remote(q_mine(step), q_rows(step, FAR), q_chip_send.at[step], q_chip_recv.at[step], far)

    q_to_sib = remote(qbuf.at[OWN], qbuf.at[SIB], q_sib_send.at[0], q_sib_recv.at[0], sib)

    def q_forward(step):
        return remote(q_rows(step, FAR), q_rows(step, FAR_SIB), q_fwd_send.at[step], q_fwd_recv.at[step], sib)

    def give_part(step):
        return remote(give.at[step], peer.at[step], part_send.at[step], part_recv.at[step], sib)

    def give_out(step):
        return remote(send_out.at[step], recv_out.at[step], o_send.at[step], o_recv.at[step], far)

    def give_lse(step):
        return remote(send_lse.at[step], recv_lse.at[step], l_send.at[step], l_recv.at[step], far)

    whole_q = pltpu.make_async_copy(q_hbm, qbuf.at[OWN], q_local.at[0])
    whole_q.start()
    load_k(0, 0).start()

    barrier = pltpu.get_barrier_semaphore()
    for dev in (sib, far):
        pl.semaphore_signal(barrier, inc=1, device_id={"dup": dev}, device_id_type=MESH)
    pl.semaphore_wait(barrier, 2)
    whole_q.wait()
    for step in range(4):
        q_to_far(step).start()
    q_to_sib.start()
    load_v(0, 0).start()
    for step in range(1, RING):
        load_k(step, step).start()
        load_v(step, step).start()

    def forward_q(step):
        q_to_far(step).wait_recv()
        q_forward(step).start()

    def await_q(step):
        q_forward(step).wait_recv()

    lane = lax.broadcasted_iota(jnp.int32, (ROWS, 128), 1)
    draft_of_row = lax.rem(lax.broadcasted_iota(jnp.int32, (ROWS, span), 0), DRAFT)
    reach = lax.broadcasted_iota(jnp.int32, (ROWS, span), 1) - draft_of_row + (me * span + DRAFT)
    rate = scale / math.log(2.0)

    first = lax.rem(lax.broadcasted_iota(jnp.int32, (16, 128), 0), 16) < ROWS
    of_first = jnp.where(first, 1.0, 0.0).astype(jnp.bfloat16)
    of_second = jnp.where(first, 0.0, 1.0).astype(jnp.bfloat16)

    def score_pair(step, slot, i):
        start = pl.multiple_of(step * CHUNK * ROWS, 16) + 16 * i
        q = [qbuf[role, pl.ds(start, 16), :] for role in range(4)]
        left = jnp.concatenate([jnp.concatenate([x * of_first, x * of_second], 1) for x in q], 0)
        k_a, k_b = kbuf[slot, 2 * i], kbuf[slot, 2 * i + 1]
        turned = span // 2
        right = jnp.concatenate([k_a[:turned], k_b[:turned]], 1)
        scores = lax.dot_general(left, right, (((1,), (1,)), ((), ())), preferred_element_type=jnp.float32)
        rest = jnp.concatenate([k_a[turned:].T, k_b[turned:].T], 0)
        more = lax.dot_general(left, rest, (((1,), (0,)), ((), ())), preferred_element_type=jnp.float32)
        return jnp.concatenate([scores, more], 1)

    def mask_pair(step, i, scores):
        for h in range(2):
            allowed = reach <= len_ref[step * CHUNK + 2 * i + h]
            for d in range(4):
                row = 16 * d + 8 * h
                s = jnp.where(allowed, scores[row : row + 8], LOWEST)
                sbuf[i, pl.ds(row, 8), :] = s
                peak = jnp.maximum(jnp.max(s, axis=1, keepdims=True), FLOOR)
                pbuf[i, pl.ds(row, 8), :] = jnp.broadcast_to(peak, (ROWS, 128))

    def weigh_pair(i, peaks, masses):
        for d in range(4):
            probs = []
            for h in range(2):
                row = 16 * d + 8 * h
                peak = pbuf[i, pl.ds(row, 8), :]
                s = sbuf[i, pl.ds(row, 8), :]
                p = jnp.exp2((s - jnp.concatenate([peak] * (span // 128), 1)) * rate)
                mass = jnp.sum(p, axis=1, keepdims=True)
                here = lane == (CHUNK * d + 2 * i + h)
                peaks = jnp.where(here, peak, peaks)
                masses = jnp.where(here, mass, masses)
                probs.append(p)
            ebuf[i, pl.ds(16 * d, 16), :] = jnp.concatenate(probs, 0).astype(jnp.bfloat16)
        return peaks, masses

    def sum_pair(step, slot, i):
        v = jnp.concatenate([vbuf[slot, 2 * i], vbuf[slot, 2 * i + 1]], 1)
        o = lax.dot_general(ebuf[i], v, (((1,), (0,)), ((), ())), preferred_element_type=jnp.float32)
        for h in range(2):
            for d in range(4):
                home = keep if d in (OWN, FAR) else give
                home[step, CHUNK * (d % 2) + 2 * i + h] = o[16 * d + 8 * h : 16 * d + 8 * h + 8, 128 * h : 128 * h + 128]

    def merge_chip(step):
        m_a, l_a = stat[step, 0], stat[step, 1]
        m_b, l_b = (pltpu.roll(peer[step, 2 * CHUNK + j], 128 - SIB * CHUNK, 1) for j in range(2))
        top = jnp.maximum(m_a, m_b)
        w_a, w_b = jnp.exp2((m_a - top) * rate), jnp.exp2((m_b - top) * rate)
        total = w_a * l_a + w_b * l_b
        some = total > 0.0
        safe = jnp.where(some, total, 1.0)
        inverse = jnp.where(some, 1.0 / safe, 0.0)
        w_a, w_b = w_a * inverse, w_b * inverse
        lse = jnp.where(some, top * rate + jnp.log2(safe), LOWEST)
        own_lse[step] = lse
        send_lse[step] = pltpu.roll(lse, 128 - FAR * CHUNK, 1)

        def both(role, b):
            c = role * CHUNK + b
            return w_a[:, c : c + 1] * keep[step, c] + w_b[:, c : c + 1] * peer[step, c]

        for i in range(pairs):
            for b in (2 * i, 2 * i + 1):
                own_out[step, b] = both(OWN, b)
            far_out = [both(FAR, b) for b in (2 * i, 2 * i + 1)]
            send_out[step, pl.ds(16 * i, 16), :] = jnp.concatenate(far_out, 0).astype(jnp.bfloat16)

    def merge_final(step):
        rows = lax.rem(step, n) * CHUNK * ROWS
        mine, theirs = own_lse[step], recv_lse[step]
        top = jnp.maximum(mine, theirs)
        w_a, w_b = jnp.exp2(mine - top), jnp.exp2(theirs - top)
        inverse = 1.0 / (w_a + w_b)
        w_a, w_b = w_a * inverse, w_b * inverse
        for i in range(pairs):
            other = recv_out[step, pl.ds(16 * i, 16), :].astype(jnp.float32)
            outs = []
            for h in range(2):
                b = 2 * i + h
                outs.append(w_a[:, b : b + 1] * own_out[step, b] + w_b[:, b : b + 1] * other[8 * h : 8 * h + 8])
            out_buf[pl.ds(pl.multiple_of(rows + 16 * i, 16), 16), :] = jnp.concatenate(outs, 0).astype(jnp.bfloat16)

    def await_peer(step):
        give_part(step).wait_recv()

    def send_far(step):
        give_out(step).start()
        give_lse(step).start()

    def await_far(step):
        give_out(step).wait_recv()
        give_lse(step).wait_recv()

    def final_stage(step):
        await_far(step)
        merge_final(step)

    def attend(step, with_next):
        slot, next_slot = lax.rem(step, RING), lax.rem(step + 1, RING)
        peaks = jnp.zeros((ROWS, 128), jnp.float32)
        masses = jnp.zeros((ROWS, 128), jnp.float32)
        scores = [None] * pairs
        for i in range(pairs + PV_LAG):
            if i < pairs:
                peaks, masses = weigh_pair(i, peaks, masses)
                if with_next:
                    scores[i] = score_pair(step + 1, next_slot, i)
            if i >= PV_LAG:
                sum_pair(step, slot, i - PV_LAG)
            if with_next and 1 <= i <= pairs:
                mask_pair(step + 1, i - 1, scores[i - 1])
        stat[step, 0] = peaks
        stat[step, 1] = masses
        give[step, 2 * CHUNK] = peaks
        give[step, 2 * CHUNK + 1] = masses

    last = n - 1
    for step in range(AHEAD):
        forward_q(step)
        q_to_far(2 * step + 4).start()
        q_to_far(2 * step + 5).start()
    q_to_sib.wait_recv()
    await_q(0)
    load_k(0, 0).wait()
    for i in range(pairs):
        mask_pair(0, i, score_pair(0, 0, i))
    load_k(RING, 0).start()

    @pl.loop(0, last)
    def _(step):
        @pl.when(2 * step + 2 * AHEAD + 4 < n)
        def _():
            q_to_far(2 * step + 2 * AHEAD + 4).start()
            q_to_far(2 * step + 2 * AHEAD + 5).start()

        @pl.when(step + AHEAD < n)
        def _():
            forward_q(step + AHEAD)

        await_q(step + 1)
        load_k(step + 1, lax.rem(step + 1, RING)).wait()
        load_v(step, lax.rem(step, RING)).wait()

        @pl.when(step >= LAG)
        def _():
            await_peer(step - LAG)

        @pl.when(step >= FINAL_LAG)
        def _():
            await_far(step - FINAL_LAG)

        done = (step + n - FINAL_LAG) // n
        merge_final(done * (step - FINAL_LAG) + (1 - done) * n)
        ready = (step + n - LAG) // n
        merge_chip(ready * (step - LAG) + (1 - ready) * n)
        attend(step, True)
        give_part(step).start()

        @pl.when(step >= LAG)
        def _():
            send_far(step - LAG)

        @pl.when(step + 1 + RING < n)
        def _():
            load_k(step + 1 + RING, lax.rem(step + 1, RING)).start()

        @pl.when(step + RING < n)
        def _():
            load_v(step + RING, lax.rem(step, RING)).start()

    load_v(last, lax.rem(last, RING)).wait()
    await_peer(last - LAG)
    await_far(last - FINAL_LAG)
    merge_final(last - FINAL_LAG)
    merge_chip(last - LAG)
    attend(last, False)
    give_part(last).start()
    send_far(last - LAG)

    @pl.loop(last - LAG + 1, last)
    def _(step):
        await_peer(step)
        merge_chip(step)
        send_far(step)

    @pl.loop(last - FINAL_LAG + 1, last - FINAL_LAG + 1 + EARLY_FINALS)
    def _(step):
        final_stage(step)

    await_peer(last)
    merge_chip(last)
    send_far(last)

    @pl.loop(last - FINAL_LAG + 1 + EARLY_FINALS, n)
    def _(step):
        final_stage(step)

    q_to_sib.wait_send()

    @pl.loop(0, n)
    def _(step):
        q_to_far(step).wait_send()
        q_forward(step).wait_send()
        give_part(step).wait_send()
        give_out(step).wait_send()
        give_lse(step).wait_send()


def solution(mesh):
    def group_step(q_local, k_span, v_span, len_local):
        num_batch, span, dim = k_span.shape
        n = num_batch // CHUNK
        f32, bf16 = jnp.float32, jnp.bfloat16
        dma = lambda *shape: pltpu.SemaphoreType.DMA(shape)
        hbm = pl.BlockSpec(memory_space=pltpu.HBM)
        out = pl.pallas_call(
            functools.partial(kernel, n, dim**-0.5),
            out_shape=pltpu.VMEM((num_batch * ROWS, dim), bf16),
            in_specs=[pl.BlockSpec(memory_space=pltpu.SMEM), hbm, hbm, hbm],
            out_specs=pl.BlockSpec(memory_space=pltpu.VMEM),
            scratch_shapes=[
                pltpu.VMEM((RING, CHUNK, span, dim), bf16),
                pltpu.VMEM((RING, CHUNK, span, dim), bf16),
                pltpu.VMEM((4, num_batch * ROWS, dim), bf16),
                pltpu.VMEM((CHUNK // 2, 64, span), f32),
                pltpu.VMEM((CHUNK // 2, 64, 128), f32),
                pltpu.VMEM((CHUNK // 2, 64, span), bf16),
                pltpu.VMEM((n + 1, 2 * CHUNK, ROWS, dim), f32),
                pltpu.VMEM((n, 2 * CHUNK + 2, ROWS, dim), f32),
                pltpu.VMEM((n + 1, 2 * CHUNK + 2, ROWS, dim), f32),
                pltpu.VMEM((n + 1, 2, ROWS, dim), f32),
                pltpu.VMEM((n + 1, CHUNK, ROWS, dim), f32),
                pltpu.VMEM((n + 1, CHUNK * ROWS, dim), bf16),
                pltpu.VMEM((n + 1, ROWS, dim), f32),
                pltpu.VMEM((n + 1, CHUNK * ROWS, dim), bf16),
                pltpu.VMEM((n + 1, ROWS, dim), f32),
                pltpu.VMEM((n + 1, ROWS, dim), f32),
                dma(RING),
                dma(RING),
                dma(1),
            ]
            + [dma(n)] * 12,
            compiler_params=pltpu.CompilerParams(
                collective_id=0, has_side_effects=True, vmem_limit_bytes=56 * 1024 * 1024
            ),
        )(len_local, q_local.reshape(num_batch * ROWS, dim), k_span, v_span)
        return out.reshape(num_batch, ROWS, dim)

    return jax.shard_map(
        group_step,
        mesh=mesh,
        in_specs=(P("kv", "dup", None), P("kv", "dup", None), P("kv", "dup", None), P("kv")),
        out_specs=P("kv", "dup", None),
        check_vma=False,
    )
```

```python
import functools
import math

import jax
import jax.numpy as jnp
from jax import lax
from jax.experimental import pallas as pl
from jax.experimental.pallas import tpu as pltpu
from jax.sharding import PartitionSpec as P

DRAFT = 4
CHUNK = 16
RING = 6
AHEAD = 2
LAG = 2
FINAL_LAG = 8
EARLY_FINALS = 4
PV_LAG = 2
ROWS = 8
OWN, FAR, SIB, FAR_SIB = range(4)
MESH = pl.DeviceIdType.MESH
LOWEST = -3.0e38
FLOOR = -2.0e38


def kernel(
    num_chunks,
    scale,
    len_ref,
    q_hbm,
    k_hbm,
    v_hbm,
    out_buf,
    kbuf,
    vbuf,
    qbuf,
    sbuf,
    pbuf,
    ebuf,
    keep,
    give,
    peer,
    stat,
    own_out,
    send_out,
    send_lse,
    recv_out,
    recv_lse,
    own_lse,
    k_sem,
    v_sem,
    q_local,
    q_chip_send,
    q_chip_recv,
    q_sib_send,
    q_sib_recv,
    q_fwd_send,
    q_fwd_recv,
    part_send,
    part_recv,
    o_send,
    o_recv,
    l_send,
    l_recv,
):
    me = lax.axis_index("dup")
    chip, core = me // 2, lax.rem(me, 2)
    sib = 2 * chip + (1 - core)
    far = 2 * (1 - chip) + core
    span = kbuf.shape[2]
    pairs = CHUNK // 2
    n = num_chunks

    def load_k(step, slot):
        return pltpu.make_async_copy(k_hbm.at[pl.ds(step * CHUNK, CHUNK)], kbuf.at[slot], k_sem.at[slot])

    def load_v(step, slot):
        return pltpu.make_async_copy(v_hbm.at[pl.ds(step * CHUNK, CHUNK)], vbuf.at[slot], v_sem.at[slot])

    def q_rows(step, role):
        return qbuf.at[role, pl.ds(step * CHUNK * ROWS, CHUNK * ROWS)]

    def q_mine(step):
        return q_rows(step, OWN)

    def remote(src, dst, send, recv, dev):
        return pltpu.make_async_remote_copy(
            src_ref=src, dst_ref=dst, send_sem=send, recv_sem=recv, device_id={"dup": dev}, device_id_type=MESH
        )

    def q_to_far(step):
        return remote(q_mine(step), q_rows(step, FAR), q_chip_send.at[step], q_chip_recv.at[step], far)

    q_to_sib = remote(qbuf.at[OWN], qbuf.at[SIB], q_sib_send.at[0], q_sib_recv.at[0], sib)

    def q_forward(step):
        return remote(q_rows(step, FAR), q_rows(step, FAR_SIB), q_fwd_send.at[step], q_fwd_recv.at[step], sib)

    def give_part(step):
        return remote(give.at[step], peer.at[step], part_send.at[step], part_recv.at[step], sib)

    def give_out(step):
        return remote(send_out.at[step], recv_out.at[step], o_send.at[step], o_recv.at[step], far)

    def give_lse(step):
        return remote(send_lse.at[step], recv_lse.at[step], l_send.at[step], l_recv.at[step], far)

    whole_q = pltpu.make_async_copy(q_hbm, qbuf.at[OWN], q_local.at[0])
    whole_q.start()
    load_k(0, 0).start()

    barrier = pltpu.get_barrier_semaphore()
    for dev in (sib, far):
        pl.semaphore_signal(barrier, inc=1, device_id={"dup": dev}, device_id_type=MESH)
    pl.semaphore_wait(barrier, 2)
    whole_q.wait()
    for step in range(4):
        q_to_far(step).start()
    q_to_sib.start()
    load_v(0, 0).start()
    for step in range(1, RING):
        load_k(step, step).start()
        load_v(step, step).start()

    def forward_q(step):
        q_to_far(step).wait_recv()
        q_forward(step).start()

    def await_q(step):
        q_forward(step).wait_recv()

    lane = lax.broadcasted_iota(jnp.int32, (ROWS, 128), 1)
    draft_of_row = lax.rem(lax.broadcasted_iota(jnp.int32, (ROWS, span), 0), DRAFT)
    reach = lax.broadcasted_iota(jnp.int32, (ROWS, span), 1) - draft_of_row + (me * span + DRAFT)
    rate = scale / math.log(2.0)

    first = lax.rem(lax.broadcasted_iota(jnp.int32, (16, 128), 0), 16) < ROWS
    of_first = jnp.where(first, 1.0, 0.0).astype(jnp.bfloat16)
    of_second = jnp.where(first, 0.0, 1.0).astype(jnp.bfloat16)

    def score_pair(step, slot, i):
        start = pl.multiple_of(step * CHUNK * ROWS, 16) + 16 * i
        q = [qbuf[role, pl.ds(start, 16), :] for role in range(4)]
        left = jnp.concatenate([jnp.concatenate([x * of_first, x * of_second], 1) for x in q], 0)
        k_a, k_b = kbuf[slot, 2 * i], kbuf[slot, 2 * i + 1]
        turned = span // 2
        right = jnp.concatenate([k_a[:turned], k_b[:turned]], 1)
        scores = lax.dot_general(left, right, (((1,), (1,)), ((), ())), preferred_element_type=jnp.float32)
        rest = jnp.concatenate([k_a[turned:].T, k_b[turned:].T], 0)
        more = lax.dot_general(left, rest, (((1,), (0,)), ((), ())), preferred_element_type=jnp.float32)
        return jnp.concatenate([scores, more], 1)

    def mask_pair(step, i, scores):
        for h in range(2):
            allowed = reach <= len_ref[step * CHUNK + 2 * i + h]
            for d in range(4):
                row = 16 * d + 8 * h
                s = jnp.where(allowed, scores[row : row + 8], LOWEST)
                sbuf[i, pl.ds(row, 8), :] = s
                peak = jnp.maximum(jnp.max(s, axis=1, keepdims=True), FLOOR)
                pbuf[i, pl.ds(row, 8), :] = jnp.broadcast_to(peak, (ROWS, 128))

    def weigh_pair(i, peaks, masses):
        for d in range(4):
            probs = []
            for h in range(2):
                row = 16 * d + 8 * h
                peak = pbuf[i, pl.ds(row, 8), :]
                s = sbuf[i, pl.ds(row, 8), :]
                p = jnp.exp2((s - jnp.concatenate([peak] * (span // 128), 1)) * rate)
                mass = jnp.sum(p, axis=1, keepdims=True)
                here = lane == (CHUNK * d + 2 * i + h)
                peaks = jnp.where(here, peak, peaks)
                masses = jnp.where(here, mass, masses)
                probs.append(p)
            ebuf[i, pl.ds(16 * d, 16), :] = jnp.concatenate(probs, 0).astype(jnp.bfloat16)
        return peaks, masses

    def sum_pair(step, slot, i):
        v = jnp.concatenate([vbuf[slot, 2 * i], vbuf[slot, 2 * i + 1]], 1)
        o = lax.dot_general(ebuf[i], v, (((1,), (0,)), ((), ())), preferred_element_type=jnp.float32)
        for h in range(2):
            for d in range(4):
                home = keep if d in (OWN, FAR) else give
                home[step, CHUNK * (d % 2) + 2 * i + h] = o[16 * d + 8 * h : 16 * d + 8 * h + 8, 128 * h : 128 * h + 128]

    def merge_chip(step):
        m_a, l_a = stat[step, 0], stat[step, 1]
        m_b, l_b = (pltpu.roll(peer[step, 2 * CHUNK + j], 128 - SIB * CHUNK, 1) for j in range(2))
        top = jnp.maximum(m_a, m_b)
        w_a, w_b = jnp.exp2((m_a - top) * rate), jnp.exp2((m_b - top) * rate)
        total = w_a * l_a + w_b * l_b
        some = total > 0.0
        safe = jnp.where(some, total, 1.0)
        inverse = jnp.where(some, 1.0 / safe, 0.0)
        w_a, w_b = w_a * inverse, w_b * inverse
        lse = jnp.where(some, top * rate + jnp.log2(safe), LOWEST)
        own_lse[step] = lse
        send_lse[step] = pltpu.roll(lse, 128 - FAR * CHUNK, 1)

        def both(role, b):
            c = role * CHUNK + b
            return w_a[:, c : c + 1] * keep[step, c] + w_b[:, c : c + 1] * peer[step, c]

        for i in range(pairs):
            for b in (2 * i, 2 * i + 1):
                own_out[step, b] = both(OWN, b)
            far_out = [both(FAR, b) for b in (2 * i, 2 * i + 1)]
            send_out[step, pl.ds(16 * i, 16), :] = jnp.concatenate(far_out, 0).astype(jnp.bfloat16)

    def merge_final(step):
        rows = lax.rem(step, n) * CHUNK * ROWS
        mine, theirs = own_lse[step], recv_lse[step]
        top = jnp.maximum(mine, theirs)
        w_a, w_b = jnp.exp2(mine - top), jnp.exp2(theirs - top)
        inverse = 1.0 / (w_a + w_b)
        w_a, w_b = w_a * inverse, w_b * inverse
        for i in range(pairs):
            other = recv_out[step, pl.ds(16 * i, 16), :].astype(jnp.float32)
            outs = []
            for h in range(2):
                b = 2 * i + h
                outs.append(w_a[:, b : b + 1] * own_out[step, b] + w_b[:, b : b + 1] * other[8 * h : 8 * h + 8])
            out_buf[pl.ds(pl.multiple_of(rows + 16 * i, 16), 16), :] = jnp.concatenate(outs, 0).astype(jnp.bfloat16)

    def await_peer(step):
        give_part(step).wait_recv()

    def send_far(step):
        give_out(step).start()
        give_lse(step).start()

    def await_far(step):
        give_out(step).wait_recv()
        give_lse(step).wait_recv()

    def final_stage(step):
        await_far(step)
        merge_final(step)

    def attend(step, with_next):
        slot, next_slot = lax.rem(step, RING), lax.rem(step + 1, RING)
        peaks = jnp.zeros((ROWS, 128), jnp.float32)
        masses = jnp.zeros((ROWS, 128), jnp.float32)
        scores = [None] * pairs
        for i in range(pairs + PV_LAG):
            if i < pairs:
                peaks, masses = weigh_pair(i, peaks, masses)
                if with_next:
                    scores[i] = score_pair(step + 1, next_slot, i)
            if i >= PV_LAG:
                sum_pair(step, slot, i - PV_LAG)
            if with_next and 1 <= i <= pairs:
                mask_pair(step + 1, i - 1, scores[i - 1])
        stat[step, 0] = peaks
        stat[step, 1] = masses
        give[step, 2 * CHUNK] = peaks
        give[step, 2 * CHUNK + 1] = masses

    last = n - 1
    for step in range(AHEAD):
        forward_q(step)
        q_to_far(2 * step + 4).start()
        q_to_far(2 * step + 5).start()
    q_to_sib.wait_recv()
    await_q(0)
    load_k(0, 0).wait()
    for i in range(pairs):
        mask_pair(0, i, score_pair(0, 0, i))
    load_k(RING, 0).start()

    @pl.loop(0, last)
    def _(step):
        @pl.when(2 * step + 2 * AHEAD + 4 < n)
        def _():
            q_to_far(2 * step + 2 * AHEAD + 4).start()
            q_to_far(2 * step + 2 * AHEAD + 5).start()

        @pl.when(step + AHEAD < n)
        def _():
            forward_q(step + AHEAD)

        await_q(step + 1)
        load_k(step + 1, lax.rem(step + 1, RING)).wait()
        load_v(step, lax.rem(step, RING)).wait()

        @pl.when(step >= LAG)
        def _():
            await_peer(step - LAG)

        @pl.when(step >= FINAL_LAG)
        def _():
            await_far(step - FINAL_LAG)

        done = (step + n - FINAL_LAG) // n
        merge_final(done * (step - FINAL_LAG) + (1 - done) * n)
        ready = (step + n - LAG) // n
        merge_chip(ready * (step - LAG) + (1 - ready) * n)
        attend(step, True)
        give_part(step).start()

        @pl.when(step >= LAG)
        def _():
            send_far(step - LAG)

        @pl.when(step + 1 + RING < n)
        def _():
            load_k(step + 1 + RING, lax.rem(step + 1, RING)).start()

        @pl.when(step + RING < n)
        def _():
            load_v(step + RING, lax.rem(step, RING)).start()

    load_v(last, lax.rem(last, RING)).wait()
    await_peer(last - LAG)
    await_far(last - FINAL_LAG)
    merge_final(last - FINAL_LAG)
    merge_chip(last - LAG)
    attend(last, False)
    give_part(last).start()
    send_far(last - LAG)

    @pl.loop(last - LAG + 1, last)
    def _(step):
        await_peer(step)
        merge_chip(step)
        send_far(step)

    @pl.loop(last - FINAL_LAG + 1, last - FINAL_LAG + 1 + EARLY_FINALS)
    def _(step):
        final_stage(step)

    await_peer(last)
    merge_chip(last)
    send_far(last)

    q_to_sib.wait_send()

    @pl.loop(0, n)
    def _(step):
        q_to_far(step).wait_send()
        q_forward(step).wait_send()
        give_part(step).wait_send()

    @pl.loop(0, last - 2)
    def _(step):
        give_out(step).wait_send()
        give_lse(step).wait_send()

    @pl.loop(last - FINAL_LAG + 1 + EARLY_FINALS, n)
    def _(step):
        final_stage(step)

    @pl.loop(last - 2, n)
    def _(step):
        give_out(step).wait_send()
        give_lse(step).wait_send()


def solution(mesh):
    def group_step(q_local, k_span, v_span, len_local):
        num_batch, span, dim = k_span.shape
        n = num_batch // CHUNK
        f32, bf16 = jnp.float32, jnp.bfloat16
        dma = lambda *shape: pltpu.SemaphoreType.DMA(shape)
        hbm = pl.BlockSpec(memory_space=pltpu.HBM)
        out = pl.pallas_call(
            functools.partial(kernel, n, dim**-0.5),
            out_shape=pltpu.VMEM((num_batch * ROWS, dim), bf16),
            in_specs=[pl.BlockSpec(memory_space=pltpu.SMEM), hbm, hbm, hbm],
            out_specs=pl.BlockSpec(memory_space=pltpu.VMEM),
            scratch_shapes=[
                pltpu.VMEM((RING, CHUNK, span, dim), bf16),
                pltpu.VMEM((RING, CHUNK, span, dim), bf16),
                pltpu.VMEM((4, num_batch * ROWS, dim), bf16),
                pltpu.VMEM((CHUNK // 2, 64, span), f32),
                pltpu.VMEM((CHUNK // 2, 64, 128), f32),
                pltpu.VMEM((CHUNK // 2, 64, span), bf16),
                pltpu.VMEM((n + 1, 2 * CHUNK, ROWS, dim), f32),
                pltpu.VMEM((n, 2 * CHUNK + 2, ROWS, dim), f32),
                pltpu.VMEM((n + 1, 2 * CHUNK + 2, ROWS, dim), f32),
                pltpu.VMEM((n + 1, 2, ROWS, dim), f32),
                pltpu.VMEM((n + 1, CHUNK, ROWS, dim), f32),
                pltpu.VMEM((n + 1, CHUNK * ROWS, dim), bf16),
                pltpu.VMEM((n + 1, ROWS, dim), f32),
                pltpu.VMEM((n + 1, CHUNK * ROWS, dim), bf16),
                pltpu.VMEM((n + 1, ROWS, dim), f32),
                pltpu.VMEM((n + 1, ROWS, dim), f32),
                dma(RING),
                dma(RING),
                dma(1),
            ]
            + [dma(n)] * 12,
            compiler_params=pltpu.CompilerParams(
                collective_id=0, has_side_effects=True, vmem_limit_bytes=56 * 1024 * 1024
            ),
        )(len_local, q_local.reshape(num_batch * ROWS, dim), k_span, v_span)
        return out.reshape(num_batch, ROWS, dim)

    return jax.shard_map(
        group_step,
        mesh=mesh,
        in_specs=(P("kv", "dup", None), P("kv", "dup", None), P("kv", "dup", None), P("kv")),
        out_specs=P("kv", "dup", None),
        check_vma=False,
    )
```
